32 devices in a mesh: dp: 1 (over z), ep: 32 (over y, x, core).
Axes of the slice: x: 4, y: 4, z: 1, core: 2. Of those that a mesh axis runs over, the one named last changes fastest.
The devices are a block of a 4x4x8 slice.
Arguments:
- tokens: bfloat16 [8192, 1536], P(('dp', 'ep'))
- expert_ids: int32 [8192, 6], P(('dp', 'ep'))
- gate_vals: float32 [8192, 6], P(('dp', 'ep'))
- w_gate: bfloat16 [64, 1536, 512], P('ep')
- w_up: bfloat16 [64, 1536, 512], P('ep')
- w_down: bfloat16 [64, 512, 1536], P('ep')
- shared_gate: bfloat16 [1536, 1024], replicated
- shared_up: bfloat16 [1536, 1024], replicated
- shared_down: bfloat16 [1024, 1536], replicated
Outputs:
- output: bfloat16 [8192, 1536], P(('dp', 'ep'))
All inputs are finite; a program needn't handle non-finite values.
Results may differ from the reference program's by a relative error of at most 0.00669537.
Values are sent between devices in bfloat16 or wider.
A program may use at most 768 MiB of HBM per device.

```python
import jax
import jax.numpy as jnp
from jax import lax

GROUP_SIZE = 32
TOKENS_DEV = 256
MODEL_DIM = 1536
EXPERT_FF = 512
SHARED_FF = 1024
EXPERTS = 64
TOP_K = 6
LOCAL_EXPERTS = EXPERTS // GROUP_SIZE
SPREAD_SLOTS = max(GROUP_SIZE, EXPERTS // 2)
CAPACITY = (TOKENS_DEV * TOP_K + SPREAD_SLOTS - 1) // SPREAD_SLOTS


def route_ids(route_key):
    key_shift, key_base, key_perm = jax.random.split(route_key, 3)
    dev_shift = jax.random.randint(key_shift, (GROUP_SIZE, 1, 1), 0, GROUP_SIZE)
    base_local = jax.random.randint(key_base, (), 0, LOCAL_EXPERTS)
    src_index = jnp.arange(GROUP_SIZE, dtype=jnp.int32).reshape(GROUP_SIZE, 1, 1)
    local_shift = base_local + src_index * (SPREAD_SLOTS // GROUP_SIZE)
    perm_keys = jax.random.split(key_perm, GROUP_SIZE)
    tok_order = jax.vmap(lambda perm_key: jax.random.permutation(perm_key, TOKENS_DEV))(perm_keys)
    row_pos = tok_order[:, :, None] * TOP_K + jnp.arange(TOP_K, dtype=jnp.int32).reshape(1, 1, TOP_K)
    spot_idx = row_pos % SPREAD_SLOTS
    dest_dev = (dev_shift + spot_idx) % GROUP_SIZE
    local_id = (local_shift + spot_idx // GROUP_SIZE) % LOCAL_EXPERTS
    return (dest_dev * LOCAL_EXPERTS + local_id).reshape(GROUP_SIZE * TOKENS_DEV, TOP_K).astype(jnp.int32)


def setup_inputs(seed: int = 0, part: int = 0) -> dict:
    part_key = jax.random.fold_in(jax.random.key(seed), part)
    key_tok, key_route, key_gate = jax.random.split(part_key, 3)
    weight_keys = jax.random.split(jax.random.key(seed + 1), 6)
    row_count = GROUP_SIZE * TOKENS_DEV
    tokens = jax.random.normal(key_tok, (row_count, MODEL_DIM), jnp.float32).astype(jnp.bfloat16)
    expert_ids = route_ids(key_route)
    gate_vals = 3.0 * TOP_K ** -0.5 * jax.nn.sigmoid(2.0 * jax.random.normal(key_gate, (row_count, TOP_K), jnp.float32))
    w_gate = (jax.random.normal(weight_keys[0], (EXPERTS, MODEL_DIM, EXPERT_FF), jnp.float32) * MODEL_DIM ** -0.5).astype(jnp.bfloat16)
    w_up = (jax.random.normal(weight_keys[1], (EXPERTS, MODEL_DIM, EXPERT_FF), jnp.float32) * MODEL_DIM ** -0.5).astype(jnp.bfloat16)
    w_down = (jax.random.normal(weight_keys[2], (EXPERTS, EXPERT_FF, MODEL_DIM), jnp.float32) * EXPERT_FF ** -0.5).astype(jnp.bfloat16)
    shared_gate = (jax.random.normal(weight_keys[3], (MODEL_DIM, SHARED_FF), jnp.float32) * MODEL_DIM ** -0.5).astype(jnp.bfloat16)
    shared_up = (jax.random.normal(weight_keys[4], (MODEL_DIM, SHARED_FF), jnp.float32) * MODEL_DIM ** -0.5).astype(jnp.bfloat16)
    shared_down = (jax.random.normal(weight_keys[5], (SHARED_FF, MODEL_DIM), jnp.float32) * SHARED_FF ** -0.5).astype(jnp.bfloat16)
    return {"tokens": tokens, "expert_ids": expert_ids, "gate_vals": gate_vals, "w_gate": w_gate, "w_up": w_up, "w_down": w_down, "shared_gate": shared_gate, "shared_up": shared_up, "shared_down": shared_down}


def swiglu(row_block, gate_w, up_w, down_w):
    gate_act = jnp.dot(row_block, gate_w, preferred_element_type=jnp.float32)
    up_act = jnp.dot(row_block, up_w, preferred_element_type=jnp.float32)
    hidden = (jax.nn.silu(gate_act) * up_act).astype(jnp.bfloat16)
    return jnp.dot(hidden, down_w, preferred_element_type=jnp.float32).astype(jnp.bfloat16)


def reference(tokens, expert_ids, gate_vals, w_gate, w_up, w_down, shared_gate, shared_up, shared_down):
    row_count = GROUP_SIZE * TOKENS_DEV
    src_ids = expert_ids.reshape(GROUP_SIZE, TOKENS_DEV * TOP_K)
    one_hot = (src_ids[:, :, None] == jnp.arange(EXPERTS, dtype=jnp.int32)[None, None, :]).astype(jnp.int32)
    slot_pos = jnp.sum(jnp.cumsum(one_hot, axis=1) * one_hot, axis=2) - 1
    buf_row = (jnp.arange(GROUP_SIZE, dtype=jnp.int32)[:, None] * CAPACITY + slot_pos).reshape(-1)
    flat_ids = src_ids.reshape(-1)
    token_rows = jnp.repeat(tokens, TOP_K, axis=0)
    buffers = jnp.zeros((EXPERTS, GROUP_SIZE * CAPACITY, MODEL_DIM), jnp.bfloat16)
    buffers = buffers.at[flat_ids, buf_row].set(token_rows)
    expert_out = lax.map(lambda operands: swiglu(operands[0], operands[1], operands[2], operands[3]), (buffers, w_gate, w_up, w_down))
    picked = expert_out[flat_ids, buf_row].reshape(row_count, TOP_K, MODEL_DIM)
    result_acc = tokens.astype(jnp.float32)
    for slot_idx in range(TOP_K):
        result_acc = result_acc + gate_vals[:, slot_idx:slot_idx + 1] * picked[:, slot_idx, :].astype(jnp.float32)
    shared_out = swiglu(tokens, shared_gate, shared_up, shared_down)
    return (result_acc + shared_out.astype(jnp.float32)).astype(jnp.bfloat16)
```

```python
import functools
import math

import jax
import jax.numpy as jnp
from jax import lax
from jax.experimental import pallas as pl
from jax.experimental.pallas import tpu as pltpu
from jax.sharding import PartitionSpec as P

F32 = jnp.float32
BF16 = jnp.bfloat16
MESH = pl.DeviceIdType.MESH


OFFSETS = (0, -1, 1, 2)


def kernel(side, cap, ids_ref, gat_ref, tok_hbm, wg_hbm, wu_hbm, wd_hbm, sg_hbm, su_hbm, sd_hbm, out_ref,
           w_g, w_u, w_d, tok, info, xbuf, fbuf, raw, relay, gsplit, part, acc, half, fin,
           own_sem, tok_r, tu_s, fu_s, tv_s, fv_s, inf_r, iu_s, iv_s, raw_r, rel_r, f_s, rel_s,
           half_r, half_s, fin_r, fin_s, sh_sem, wl_sem, wr_s, wr_r):
    tok_count, model_dim = tok_hbm.shape
    top_count = ids_ref.shape[1]
    local_count, _, ff = wg_hbm.shape
    chip_experts = 2 * local_count
    block = chip_experts * cap
    piece = tok_count // 2
    hblock = block // 2

    me = lax.axis_index("ep")
    c = me % 2
    chip = me // 2
    cx, cy = chip % side, chip // side
    u = (1 - c) * cx + c * cy
    v = (1 - c) * cy + c * cx

    def chip_at(uu, vv):
        uu, vv = (uu + side) % side, (vv + side) % side
        return (1 - c) * (vv * side + uu) + c * (uu * side + vv)

    def dev_at(uu, vv):
        return chip_at(uu, vv) * 2 + c

    u_dev = (dev_at(u + 1, v), dev_at(u - 1, v))
    v_dev = (dev_at(u, v + 1), dev_at(u, v - 1))
    partner = chip * 2 + (1 - c)
    side_of = (1, 2)

    sent = []

    def send(src, dst, ssem, rsem, dev, keep=None):
        copy = pltpu.make_async_remote_copy(src_ref=src, dst_ref=dst, send_sem=ssem, recv_sem=rsem,
                                            device_id={"ep": dev}, device_id_type=MESH)
        copy.start()
        (sent if keep is None else keep).append(copy)

    def arrived(dst, rsem):
        pltpu.make_async_remote_copy(src_ref=dst, dst_ref=dst, send_sem=half_s.at[0], recv_sem=rsem,
                                     device_id={"ep": me}, device_id_type=MESH).wait_recv()

    def rows_of(p):
        return pl.ds(p * piece, piece)

    def tok_wait(g, k, p):
        arrived(tok.at[g, k, rows_of(p)], tok_r.at[g, k, p])

    own = pltpu.make_async_copy(tok_hbm, tok.at[0, 0], own_sem)
    own.start()
    shared_loads = []
    for i in range(local_count):
        cols = pl.ds(i * ff, ff)
        for j, (src, dst) in enumerate(((sg_hbm.at[:, cols], w_g), (su_hbm.at[:, cols], w_u), (sd_hbm.at[cols], w_d))):
            copy = pltpu.make_async_copy(src, dst.at[i], sh_sem.at[i, j])
            copy.start()
            shared_loads.append(copy)

    barrier = pltpu.get_barrier_semaphore()
    for dev in u_dev + v_dev + (partner,):
        pl.semaphore_signal(barrier, inc=1, device_id={"ep": dev}, device_id_type=MESH)
    pl.semaphore_wait(barrier, 5)

    own.wait()

    def send_u_own():
        for order in range(2):
            for d in range(2):
                p = (d + order) % 2
                send(tok.at[0, 0, rows_of(p)], tok.at[0, side_of[d], rows_of(p)], tu_s.at[d, p],
                     tok_r.at[0, side_of[d], p], u_dev[d])

    def send_v(k):
        for order in range(2):
            for d in range(2):
                p = (d + order) % 2
                send(tok.at[0, k, rows_of(p)], tok.at[side_of[d], k, rows_of(p)], tv_s.at[k, d, p],
                     tok_r.at[side_of[d], k, p], v_dev[d])

    def forward_u(d):
        tok_wait(0, side_of[d], d)
        send(tok.at[0, side_of[d], rows_of(d)], tok.at[0, 3, rows_of(d)], fu_s.at[d], tok_r.at[0, 3, d], u_dev[d])

    def forward_v(k, d):
        tok_wait(side_of[d], k, d)
        send(tok.at[side_of[d], k, rows_of(d)], tok.at[3, k, rows_of(d)], fv_s.at[k, d], tok_r.at[3, k, d], v_dev[d])

    send_u_own()
    send_v(0)
    for i in range(local_count):
        for j, (src, dst) in enumerate(((wg_hbm, w_g), (wu_hbm, w_u), (wd_hbm, w_d))):
            send(src.at[i], dst.at[local_count + i], wr_s.at[i, j], wr_r.at[i, j], partner)

    lane = lax.broadcasted_iota(jnp.int32, (tok_count, 128), 1)
    hots = []
    chosen = jnp.zeros((tok_count, 128), F32)
    for j in range(top_count):
        hot = (ids_ref[:, j:j + 1] == lane).astype(F32)
        hots.append(hot)
        chosen = chosen + hot
    below = (lax.broadcasted_iota(jnp.int32, (tok_count, tok_count), 0)
             > lax.broadcasted_iota(jnp.int32, (tok_count, tok_count), 1)).astype(F32).astype(BF16)
    slot = jnp.dot(below, chosen.astype(BF16), preferred_element_type=F32)
    table = jnp.zeros((tok_count, 128), F32)
    for j in range(top_count):
        code = ids_ref[:, j:j + 1].astype(F32) * cap + jnp.sum(hots[j] * slot, axis=1, keepdims=True)
        table = table + jnp.where(lane == j, code, 0.0) + jnp.where(lane == 8 + j, gat_ref[:, j:j + 1], 0.0)
    info[0, 0] = table.T[0:16]

    def silu_mul(g, up):
        return (jax.nn.silu(g) * up).astype(BF16)

    n_step = 512 if model_dim % 512 == 0 else model_dim

    def shared_part(i):
        for copy in shared_loads[3 * i:3 * i + 3]:
            copy.wait()
        x = tok[0, 0]
        h = silu_mul(jnp.dot(x, w_g[i], preferred_element_type=F32), jnp.dot(x, w_u[i], preferred_element_type=F32))
        for n in range(0, model_dim, n_step):
            y = jnp.dot(h, w_d[i, :, n:n + n_step], preferred_element_type=F32)
            if i > 0:
                y = y + acc[:, n:n + n_step]
            if i == local_count - 1:
                y = y.astype(BF16).astype(F32) + x[:, n:n + n_step].astype(F32)
            acc[:, n:n + n_step] = y

    own_loads = []

    def load_own(i):
        for j, (src, dst) in enumerate(((wg_hbm, w_g), (wu_hbm, w_u), (wd_hbm, w_d))):
            copy = pltpu.make_async_copy(src.at[i], dst.at[i], wl_sem.at[i, j])
            copy.start()
            own_loads.append(copy)

    shared_part(0)
    load_own(0)

    def inf_wait(g, k):
        arrived(info.at[g, k], inf_r.at[g, k])

    def info_v(k):
        for d in range(2):
            send(info.at[0, k], info.at[side_of[d], k], iv_s.at[k, d], inf_r.at[side_of[d], k], v_dev[d])

    for d in range(2):
        send(info.at[0, 0], info.at[0, side_of[d]], iu_s.at[d], inf_r.at[0, side_of[d]], u_dev[d])
    info_v(0)

    for i in range(1, local_count):
        shared_part(i)
        load_own(i)

    forward_u(0)
    forward_u(1)
    inf_wait(0, 1)
    send(info.at[0, 1], info.at[0, 3], iu_s.at[2], inf_r.at[0, 3], u_dev[0])
    inf_wait(0, 2)
    tok_wait(0, 1, 1)
    send_v(1)
    info_v(1)
    tok_wait(0, 2, 0)
    send_v(2)
    info_v(2)

    def pass_v(k):
        forward_v(k, 0)
        forward_v(k, 1)
        inf_wait(1, k)
        send(info.at[1, k], info.at[3, k], iv_s.at[k, 2], inf_r.at[3, k], v_dev[0])
        inf_wait(2, k)

    pass_v(0)
    tok_wait(0, 3, 0)
    tok_wait(0, 3, 1)
    inf_wait(0, 3)
    send_v(3)
    info_v(3)

    slot_rows = lax.broadcasted_iota(jnp.int32, (block, tok_count), 0)
    turned = (slot_rows + c * (local_count * cap)) % block

    def row_codes(chip_idx):
        return (turned + chip_idx * block).astype(F32)

    f_sent = [[] for _ in range(4)]

    def experts(g):
        slot_f = g % 2
        if g >= 2:
            for copy in f_sent[g - 2]:
                copy.wait_send()

        def pick(k, carry):
            codes = row_codes(chip)
            hit = jnp.zeros((block, tok_count), F32)
            for j in range(top_count):
                hit = hit + (info[g, k, j:j + 1, :] == codes).astype(F32)
            hit = hit.astype(BF16)
            for n in range(0, model_dim, n_step):
                x = jnp.dot(hit, tok[g, k, :, n:n + n_step], preferred_element_type=F32).astype(BF16)
                for e in range(chip_experts):
                    xbuf[e, pl.ds(pl.multiple_of(k * cap, 16), cap), n:n + n_step] = x[e * cap:(e + 1) * cap]
            return carry

        lax.fori_loop(0, 4, pick, 0)

        def one(e, carry):
            x = xbuf[e]
            h = silu_mul(jnp.dot(x, w_g[e], preferred_element_type=F32), jnp.dot(x, w_u[e], preferred_element_type=F32))
            at = pl.ds(pl.multiple_of(e * cap, 16), cap)
            for n in range(0, model_dim, n_step):
                y = jnp.dot(h, w_d[e, :, n:n + n_step], preferred_element_type=F32).astype(BF16)
                raw[g, at, n:n + n_step] = y[0:cap]
                for k in range(1, 4):
                    fbuf[slot_f, k - 1, at, n:n + n_step] = y[k * cap:(k + 1) * cap]
            return carry

        lax.fori_loop(0, chip_experts, one, 0)

    def hrows(p):
        return pl.ds(p * hblock, hblock)

    def raw_rows(m, p):
        return pl.ds(m * block + p * hblock, hblock)

    def send_rows(g):
        slot_f = g % 2
        for d in range(2):
            send(fbuf.at[slot_f, 2, hrows(d)], relay.at[g, d], f_s.at[g, d, 2], rel_r.at[g, d], u_dev[d], f_sent[g])
        for d in range(2):
            for p in range(2):
                send(fbuf.at[slot_f, 1 - d, hrows(p)], raw.at[g, raw_rows(side_of[d], p)], f_s.at[g, d, p],
                     raw_r.at[g, side_of[d] - 1, p], u_dev[d], f_sent[g])

    def pass_rows(g):
        for d in range(2):
            arrived(relay.at[g, d], rel_r.at[g, d])
            send(relay.at[g, d], raw.at[g, raw_rows(3, d)], rel_s.at[g, d], raw_r.at[g, 2, d], u_dev[d])

    def combine(g, store):
        for m in range(1, 4):
            for p in range(2):
                arrived(raw.at[g, raw_rows(m, p)], raw_r.at[g, m - 1, p])
        for m in range(4):
            codes = row_codes(chip_at(u + OFFSETS[m], v))
            gate = jnp.zeros((block, tok_count), F32)
            for j in range(top_count):
                gate = gate + jnp.where(info[g, 0, j:j + 1, :] == codes, info[g, 0, 8 + j:9 + j, :], 0.0)
            gate = gate.T
            for s in range(3):
                part_s = gate.astype(BF16)
                gsplit[s * tok_count:(s + 1) * tok_count, m * block:(m + 1) * block] = part_s
                gate = gate - part_s.astype(F32)
        step = 256 if model_dim % 256 == 0 else model_dim

        def cols(n, carry):
            at = pl.ds(pl.multiple_of(n * step, 128), step)
            y = jnp.dot(gsplit[...], raw[g, :, at], preferred_element_type=F32)
            store(at, y[0:tok_count] + y[tok_count:2 * tok_count] + y[2 * tok_count:3 * tok_count])
            return carry

        lax.fori_loop(0, model_dim // step, cols, 0)

    def store_own(at, y):
        acc[:, at] = acc[:, at] + y

    def store_part(g):
        def store(at, y):
            part[g - 1, :, at] = y
        return store

    def send_fin(g, d, p):
        send(part.at[g - 1, rows_of(p)], fin.at[d, rows_of(p)], fin_s.at[d, p], fin_r.at[d, p], v_dev[d])

    for copy in own_loads:
        copy.wait()
    for i in range(local_count):
        for j, dst in enumerate((w_g, w_u, w_d)):
            arrived(dst.at[local_count + i], wr_r.at[i, j])

    experts(0)
    pass_v(1)
    send_rows(0)
    pass_v(2)
    pass_v(3)
    for k in range(4):
        tok_wait(1, k, 1)
    experts(1)
    pass_rows(0)
    send_rows(1)
    for k in range(4):
        tok_wait(2, k, 0)
    experts(2)
    pass_rows(1)
    send_rows(2)
    combine(0, store_own)
    pass_rows(2)
    for k in range(4):
        tok_wait(3, k, 0)
        tok_wait(3, k, 1)
        inf_wait(3, k)
    experts(3)
    combine(1, store_part(1))
    send_rows(3)
    send_fin(1, 1, 0)
    combine(2, store_part(2))
    pass_rows(3)
    send_fin(2, 0, 1)
    combine(3, store_part(3))
    for d in range(2):
        send(part.at[2, rows_of(d)], half.at[d], half_s.at[d], half_r.at[d], v_dev[d])
    for d in range(2):
        g = 2 - d
        arrived(half.at[d], half_r.at[d])
        part[g - 1, d * piece:(d + 1) * piece] = part[g - 1, d * piece:(d + 1) * piece] + half[d]
        send_fin(g, d, d)
    for p in range(2):
        for d in range(2):
            arrived(fin.at[d, rows_of(p)], fin_r.at[d, p])
        at = slice(p * piece, (p + 1) * piece)
        out_ref[at] = (acc[at] + fin[0, at] + fin[1, at]).astype(out_ref.dtype)

    for copies in f_sent[2:] + [sent]:
        for copy in copies:
            copy.wait_send()


def solution(mesh):
    group_size = mesh.shape["ep"]
    side = math.isqrt(group_size // 2)

    def moe_step(tokens, expert_ids, gate_vals, w_gate, w_up, w_down, shared_gate, shared_up, shared_down):
        tok_count, model_dim = tokens.shape
        top_count = expert_ids.shape[1]
        local_count, _, ff = w_gate.shape
        expert_count = local_count * group_size
        spread = max(group_size, expert_count // 2)
        cap = (tok_count * top_count + spread - 1) // spread
        block = 2 * local_count * cap
        piece = tok_count // 2
        dma = pltpu.SemaphoreType.DMA
        vmem = pl.BlockSpec(memory_space=pltpu.VMEM)
        hbm = pl.BlockSpec(memory_space=pl.ANY)
        scratch = [
            pltpu.VMEM((2 * local_count, model_dim, ff), BF16),
            pltpu.VMEM((2 * local_count, model_dim, ff), BF16),
            pltpu.VMEM((2 * local_count, ff, model_dim), BF16),
            pltpu.VMEM((4, 4, tok_count, model_dim), BF16),
            pltpu.VMEM((4, 4, 16, tok_count), F32),
            pltpu.VMEM((2 * local_count, 4 * cap, model_dim), BF16),
            pltpu.VMEM((2, 3, block, model_dim), BF16),
            pltpu.VMEM((4, 4 * block, model_dim), BF16),
            pltpu.VMEM((4, 2, block // 2, model_dim), BF16),
            pltpu.VMEM((3 * tok_count, 4 * block), BF16),
            pltpu.VMEM((3, tok_count, model_dim), F32),
            pltpu.VMEM((tok_count, model_dim), F32),
            pltpu.VMEM((2, piece, model_dim), F32),
            pltpu.VMEM((2, tok_count, model_dim), F32),
            dma(()), dma((4, 4, 2)), dma((2, 2)), dma((2,)), dma((4, 2, 2)), dma((4, 2)),
            dma((4, 4)), dma((3,)), dma((4, 3)),
            dma((4, 3, 2)), dma((4, 2)), dma((4, 2, 3)), dma((4, 2)),
            dma((2,)), dma((2,)), dma((2, 2)), dma((2, 2)),
            dma((local_count, 3)), dma((local_count, 3)), dma((local_count, 3)), dma((local_count, 3)),
        ]
        return pl.pallas_call(
            functools.partial(kernel, side, cap),
            out_shape=jax.ShapeDtypeStruct(tokens.shape, tokens.dtype),
            in_specs=[vmem, vmem] + [hbm] * 7,
            out_specs=vmem,
            scratch_shapes=scratch,
            compiler_params=pltpu.CompilerParams(collective_id=0, has_side_effects=True, vmem_limit_bytes=67043328),
        )(expert_ids, gate_vals, tokens, w_gate, w_up, w_down, shared_gate, shared_up, shared_down)

    row_spec = P(("dp", "ep"), None)
    expert_spec = P("ep", None, None)
    whole_spec = P(None, None)
    return jax.shard_map(moe_step, mesh=mesh, in_specs=(row_spec, row_spec, row_spec, expert_spec, expert_spec, expert_spec, whole_spec, whole_spec, whole_spec), out_specs=row_spec, check_vma=False)
```

```python
import functools
import math

import jax
import jax.numpy as jnp
from jax import lax
from jax.experimental import pallas as pl
from jax.experimental.pallas import tpu as pltpu
from jax.sharding import PartitionSpec as P

F32 = jnp.float32
BF16 = jnp.bfloat16
MESH = pl.DeviceIdType.MESH


OFFSETS = (0, -1, 1, 2)
SIDE = (1, 2)

WHOLE = {(0, 0): 0, (0, 1): 1, (0, 2): 2, (0, 3): 3, (1, 0): 4, (1, 2): 5, (2, 1): 6, (2, 3): 7}


def kernel(side, cap, ids_ref, gat_ref, tok_hbm, wg_hbm, wu_hbm, wd_hbm, sg_hbm, su_hbm, sd_hbm, out_ref,
           w_g, w_u, w_d, tok, info, xg, stage, raw, relay, gsplit, part, acc, half, fin,
           own_sem, tok_r, tu_s, fu_s, tv_s, x_r, xc_s, xf_s, inf_r, iu_s, iv_s, if_s, raw_r, rel_r, f_s, rel_s,
           half_r, half_s, fin_r, fin_s, sh_sem, wl_sem, wr_s, wr_r):
    tok_count, model_dim = tok_hbm.shape
    top_count = ids_ref.shape[0]
    local_count, _, ff = wg_hbm.shape
    chip_experts = 2 * local_count
    expert_count = local_count * side * side * 2
    block = chip_experts * cap
    piece = tok_count // 2
    chunks = 2
    width = model_dim // chunks

    me = lax.axis_index("ep")
    c = me % 2
    chip = me // 2
    cx, cy = chip % side, chip // side
    u = (1 - c) * cx + c * cy
    v = (1 - c) * cy + c * cx

    def chip_at(uu, vv):
        uu, vv = (uu + side) % side, (vv + side) % side
        return (1 - c) * (vv * side + uu) + c * (uu * side + vv)

    def dev_at(uu, vv):
        return chip_at(uu, vv) * 2 + c

    u_dev = (dev_at(u + 1, v), dev_at(u - 1, v))
    v_dev = (dev_at(u, v + 1), dev_at(u, v - 1))
    v_chip = (chip_at(u, v + 1), chip_at(u, v - 1))
    partner = chip * 2 + (1 - c)

    sent = []

    def send(src, dst, ssem, rsem, dev, keep=True):
        copy = pltpu.make_async_remote_copy(src_ref=src, dst_ref=dst, send_sem=ssem, recv_sem=rsem,
                                            device_id={"ep": dev}, device_id_type=MESH)
        copy.start()
        if keep:
            sent.append(copy)
        return copy

    def arrived(dst, rsem):
        pltpu.make_async_remote_copy(src_ref=dst, dst_ref=dst, send_sem=half_s.at[0, 0], recv_sem=rsem,
                                     device_id={"ep": me}, device_id_type=MESH).wait_recv()

    def rows_of(p):
        return pl.ds(p * piece, piece)

    own = pltpu.make_async_copy(tok_hbm, tok.at[0], own_sem)
    own.start()
    shared_loads = []
    for i in range(local_count):
        cols = pl.ds(i * ff, ff)
        for j, (src, dst) in enumerate(((sg_hbm.at[:, cols], w_g), (su_hbm.at[:, cols], w_u), (sd_hbm.at[cols], w_d))):
            copy = pltpu.make_async_copy(src, dst.at[i], sh_sem.at[i, j])
            copy.start()
            shared_loads.append(copy)

    barrier = pltpu.get_barrier_semaphore()
    for dev in u_dev + v_dev + (partner,):
        pl.semaphore_signal(barrier, inc=1, device_id={"ep": dev}, device_id_type=MESH)
    pl.semaphore_wait(barrier, 5)
    own.wait()

    def tok_wait(g, k, p):
        arrived(tok.at[WHOLE[g, k], rows_of(p)], tok_r.at[WHOLE[g, k], p])

    def send_u_own():
        for order in range(2):
            for d in range(2):
                p = (d + order) % 2
                send(tok.at[0, rows_of(p)], tok.at[SIDE[d], rows_of(p)], tu_s.at[d, p], tok_r.at[SIDE[d], p], u_dev[d])

    def forward_u(d):
        tok_wait(0, SIDE[d], d)
        send(tok.at[SIDE[d], rows_of(d)], tok.at[3, rows_of(d)], fu_s.at[d], tok_r.at[3, d], u_dev[d])

    def whole_v(k, p):
        d = k % 2
        at = WHOLE[SIDE[d], k]
        send(tok.at[k, rows_of(p)], tok.at[at, rows_of(p)], tv_s.at[k, p], tok_r.at[at, p], v_dev[d])

    send_u_own()
    whole_v(0, 0)
    whole_v(0, 1)

    expert = lax.broadcasted_iota(jnp.int32, (expert_count, tok_count), 0)
    hots = []
    chosen = jnp.zeros((expert_count, tok_count), F32)
    for j in range(top_count):
        hot = (ids_ref[j:j + 1, :] == expert).astype(F32)
        hots.append(hot)
        chosen = chosen + hot
    above = (lax.broadcasted_iota(jnp.int32, (tok_count, tok_count), 0)
             < lax.broadcasted_iota(jnp.int32, (tok_count, tok_count), 1)).astype(F32).astype(BF16)
    slot = jnp.dot(chosen.astype(BF16), above, preferred_element_type=F32)
    info[0, 0] = jnp.zeros((16, tok_count), F32)
    for j in range(top_count):
        info[0, 0, j:j + 1, :] = ids_ref[j:j + 1, :].astype(F32) * cap + jnp.sum(hots[j] * slot, axis=0, keepdims=True)
        info[0, 0, 8 + j:9 + j, :] = gat_ref[j:j + 1, :]

    slot_rows = lax.broadcasted_iota(jnp.int32, (block, tok_count), 0) + c * (local_count * cap)
    turned = jnp.where(slot_rows >= block, slot_rows - block, slot_rows)
    n_step = 512 if model_dim % 512 == 0 else model_dim

    def row_codes(chip_idx):
        return (turned + chip_idx * block).astype(F32)

    def pick(g, k, chip_idx, dst, first):
        codes = row_codes(chip_idx)
        hit = jnp.zeros((block, tok_count), F32)
        for j in range(top_count):
            hit = hit + (info[g, k, j:j + 1, :] == codes).astype(F32)
        hit = hit.astype(BF16)
        for n in range(0, model_dim, n_step):
            x = jnp.dot(hit, tok[WHOLE[g, k], :, n:n + n_step], preferred_element_type=F32).astype(BF16)
            for e in range(chip_experts):
                dst[e, first:first + cap, n:n + n_step] = x[e * cap:(e + 1) * cap]

    def group_rows(k):
        return pl.ds(k * cap, cap)

    near = [None] * 4

    def near_v(k):
        d = 1 - k % 2
        pick(0, k, v_chip[d], stage.at[k], 0)
        near[k] = send(stage.at[k], xg.at[SIDE[d], :, group_rows(k)], xc_s.at[k], x_r.at[SIDE[d], k], v_dev[d], False)

    def inf_wait(g, k):
        arrived(info.at[g, k], inf_r.at[g, k])

    def far_v(k):
        d = k % 2
        g = SIDE[d]
        tok_wait(g, k, 0)
        tok_wait(g, k, 1)
        inf_wait(g, k)
        near[k].wait_send()
        pick(g, k, v_chip[d], stage.at[k], 0)
        send(stage.at[k], xg.at[3, :, group_rows(k)], xf_s.at[k], x_r.at[3, k], v_dev[d])
        if k == 0:
            send(info.at[g, 0], info.at[3, 0], if_s, inf_r.at[3, 0], v_dev[d])

    def info_v(k):
        for d in range(2):
            if k == 0 or d == k % 2:
                send(info.at[0, k], info.at[SIDE[d], k], iv_s.at[k, d], inf_r.at[SIDE[d], k], v_dev[d])

    near_v(0)
    for d in range(2):
        send(info.at[0, 0], info.at[0, SIDE[d]], iu_s.at[d], inf_r.at[0, SIDE[d]], u_dev[d])
    info_v(0)

    for i in range(local_count):
        for j, (src, dst) in enumerate(((wg_hbm, w_g), (wu_hbm, w_u), (wd_hbm, w_d))):
            send(src.at[i], dst.at[local_count + i], wr_s.at[i, j], wr_r.at[i, j], partner)

    def silu_mul(g, up):
        return (jax.nn.silu(g) * up).astype(BF16)

    def shared_part(i):
        for copy in shared_loads[3 * i:3 * i + 3]:
            copy.wait()
        x = tok[0]
        h = silu_mul(jnp.dot(x, w_g[i], preferred_element_type=F32), jnp.dot(x, w_u[i], preferred_element_type=F32))
        for n in range(0, model_dim, n_step):
            y = jnp.dot(h, w_d[i, :, n:n + n_step], preferred_element_type=F32)
            if i > 0:
                y = y + acc[:, n:n + n_step]
            if i == local_count - 1:
                y = y.astype(BF16).astype(F32) + x[:, n:n + n_step].astype(F32)
            acc[:, n:n + n_step] = y

    own_loads = []

    def load_own(i):
        for j, (src, dst) in enumerate(((wg_hbm, w_g), (wu_hbm, w_u), (wd_hbm, w_d))):
            copy = pltpu.make_async_copy(src.at[i], dst.at[i], wl_sem.at[i, j])
            copy.start()
            own_loads.append(copy)

    for i in range(local_count):
        shared_part(i)
        load_own(i)

    forward_u(0)
    forward_u(1)
    inf_wait(0, 1)
    send(info.at[0, 1], info.at[0, 3], iu_s.at[2], inf_r.at[0, 3], u_dev[0])
    inf_wait(0, 2)
    whole_v(1, 0)
    whole_v(2, 1)
    tok_wait(0, 1, 1)
    whole_v(1, 1)
    info_v(1)
    near_v(1)
    tok_wait(0, 2, 0)
    whole_v(2, 0)
    info_v(2)
    near_v(2)
    far_v(0)
    for p in range(2):
        tok_wait(0, 3, p)
        whole_v(3, p)
    inf_wait(0, 3)
    info_v(3)
    near_v(3)

    def experts(g):
        def one(e, carry):
            x = xg[g, e]
            h = silu_mul(jnp.dot(x, w_g[e], preferred_element_type=F32), jnp.dot(x, w_u[e], preferred_element_type=F32))
            for n in range(0, model_dim, n_step):
                y = jnp.dot(h, w_d[e, :, n:n + n_step], preferred_element_type=F32).astype(BF16)
                raw[g, 0, e, :, n:n + n_step] = y[0:cap]
                xg[g, e, cap:4 * cap, n:n + n_step] = y[cap:4 * cap]
            return carry

        lax.fori_loop(0, chip_experts, one, 0)

    def own_pick(g, ks):
        for k in ks:
            pick(g, k, chip, xg.at[g], k * cap)

    def x_wait(g, ks):
        for k in ks:
            arrived(xg.at[g, :, group_rows(k)], x_r.at[g, k])

    def e_half(d):
        return pl.ds(d * local_count, local_count)

    def col_chunk(f):
        return slice(None) if f is None else pl.ds(f * width, width)

    def send_rows(g, f=None):
        at = col_chunk(f)
        i = f or 0
        for d in range(2):
            send(xg.at[g, e_half(d), group_rows(3), at], relay.at[g, d, :, :, at], f_s.at[g, d, 1, i],
                 rel_r.at[g, d, i], u_dev[d])
        for d in range(2):
            send(xg.at[g, :, group_rows(2 - d), at], raw.at[g, SIDE[d], :, :, at], f_s.at[g, d, 0, i],
                 raw_r.at[g, SIDE[d], 0, i], u_dev[d])

    def pass_rows(g, f=None):
        at = col_chunk(f)
        i = f or 0
        for d in range(2):
            arrived(relay.at[g, d, :, :, at], rel_r.at[g, d, i])
            send(relay.at[g, d, :, :, at], raw.at[g, 3, e_half(d), :, at], rel_s.at[g, d, i], raw_r.at[g, 3, d, i], u_dev[d])

    def raw_wait(g, f=None):
        at = col_chunk(f)
        i = f or 0
        for m in range(1, 3):
            arrived(raw.at[g, m, :, :, at], raw_r.at[g, m, 0, i])
        for d in range(2):
            arrived(raw.at[g, 3, e_half(d), :, at], raw_r.at[g, 3, d, i])

    def gates_of(g):
        for m in range(4):
            codes = row_codes(chip_at(u + OFFSETS[m], v))
            gate = jnp.zeros((block, tok_count), F32)
            for j in range(top_count):
                gate = gate + jnp.where(info[g, 0, j:j + 1, :] == codes, info[g, 0, 8 + j:9 + j, :], 0.0)
            gate = gate.T
            for s in range(3):
                part_s = gate.astype(BF16)
                gsplit[s * tok_count:(s + 1) * tok_count, m * block:(m + 1) * block] = part_s
                gate = gate - part_s.astype(F32)

    step = 256 if width % 256 == 0 else width

    def gated(g, f=None):
        first, count = (0, model_dim // step) if f is None else (f * (width // step), width // step)

        def cols(n, carry):
            at = pl.ds(pl.multiple_of(n * step, 128), step)
            rows = raw[g, :, :, :, at].reshape(4 * block, step)
            y = jnp.dot(gsplit[...], rows, preferred_element_type=F32)
            y = y[0:tok_count] + y[tok_count:2 * tok_count] + y[2 * tok_count:3 * tok_count]
            if g == 0:
                acc[:, at] = acc[:, at] + y
            else:
                part[g - 1, :, at] = y
            return carry

        lax.fori_loop(first, first + count, cols, 0)

    def send_fin(g, d, p, f=None):
        at = col_chunk(f)
        send(part.at[g - 1, rows_of(p), at], fin.at[d, rows_of(p), at], fin_s.at[d, p, f or 0], fin_r.at[d, p, f or 0], v_dev[d])

    own_pick(0, range(4))
    for copy in own_loads:
        copy.wait()
    for i in range(local_count):
        for j, dst in enumerate((w_g, w_u, w_d)):
            arrived(dst.at[local_count + i], wr_r.at[i, j])
    experts(0)
    far_v(1)
    send_rows(0)
    far_v(2)
    far_v(3)
    own_pick(1, (0, 2))
    x_wait(1, (1, 3))
    experts(1)
    pass_rows(0)
    send_rows(1)
    own_pick(2, (1, 3))
    x_wait(2, (0, 2))
    experts(2)
    pass_rows(1)
    send_rows(2)
    raw_wait(0)
    gates_of(0)
    gated(0)
    pass_rows(2)
    x_wait(3, range(4))
    experts(3)
    for f in range(chunks):
        send_rows(3, f)
    raw_wait(1)
    gates_of(1)
    gated(1)
    raw_wait(2)
    inf_wait(2, 0)
    gates_of(2)
    pass_rows(3, 0)
    gated(2)
    for f in range(1, chunks):
        pass_rows(3, f)
    inf_wait(3, 0)
    gates_of(3)
    for f in range(chunks):
        raw_wait(3, f)
        gated(3, f)
        for d in range(2):
            send(part.at[2, rows_of(d), col_chunk(f)], half.at[d, :, col_chunk(f)], half_s.at[d, f], half_r.at[d, f], v_dev[d])
    send_fin(1, 1, 0)
    send_fin(2, 0, 1)
    for f in range(chunks):
        at = slice(f * width, (f + 1) * width)
        for d in range(2):
            g = 2 - d
            arrived(half.at[d, :, col_chunk(f)], half_r.at[d, f])
            rows = slice(d * piece, (d + 1) * piece)
            part[g - 1, rows, at] = part[g - 1, rows, at] + half[d, :, at]
            send_fin(g, d, d, f)
    for d in range(2):
        arrived(fin.at[d, rows_of(1 - d)], fin_r.at[d, 1 - d, 0])
        rows = slice((1 - d) * piece, (2 - d) * piece)
        acc[rows] = acc[rows] + fin[d, rows]
    for f in range(chunks):
        at = slice(f * width, (f + 1) * width)
        for d in range(2):
            arrived(fin.at[d, rows_of(d), col_chunk(f)], fin_r.at[d, d, f])
            rows = slice(d * piece, (d + 1) * piece)
            out_ref[rows, at] = (acc[rows, at] + fin[d, rows, at]).astype(out_ref.dtype)

    for copy in sent:
        copy.wait_send()


def solution(mesh):
    group_size = mesh.shape["ep"]
    side = math.isqrt(group_size // 2)

    def moe_step(tokens, expert_ids, gate_vals, w_gate, w_up, w_down, shared_gate, shared_up, shared_down):
        tok_count, model_dim = tokens.shape
        top_count = expert_ids.shape[1]
        local_count, _, ff = w_gate.shape
        expert_count = local_count * group_size
        spread = max(group_size, expert_count // 2)
        cap = (tok_count * top_count + spread - 1) // spread
        block = 2 * local_count * cap
        piece = tok_count // 2
        dma = pltpu.SemaphoreType.DMA
        vmem = pl.BlockSpec(memory_space=pltpu.VMEM)
        hbm = pl.BlockSpec(memory_space=pl.ANY)
        scratch = [
            pltpu.VMEM((2 * local_count, model_dim, ff), BF16),
            pltpu.VMEM((2 * local_count, model_dim, ff), BF16),
            pltpu.VMEM((2 * local_count, ff, model_dim), BF16),
            pltpu.VMEM((len(WHOLE), tok_count, model_dim), BF16),
            pltpu.VMEM((4, 4, 16, tok_count), F32),
            pltpu.VMEM((4, 2 * local_count, 4 * cap, model_dim), BF16),
            pltpu.VMEM((4, 2 * local_count, cap, model_dim), BF16),
            pltpu.VMEM((4, 4, 2 * local_count, cap, model_dim), BF16),
            pltpu.VMEM((4, 2, local_count, cap, model_dim), BF16),
            pltpu.VMEM((3 * tok_count, 4 * block), BF16),
            pltpu.VMEM((3, tok_count, model_dim), F32),
            pltpu.VMEM((tok_count, model_dim), F32),
            pltpu.VMEM((2, piece, model_dim), F32),
            pltpu.VMEM((2, tok_count, model_dim), F32),
            dma(()), dma((len(WHOLE), 2)), dma((2, 2)), dma((2,)), dma((4, 2)), dma((4, 4)), dma((4,)), dma((4,)),
            dma((4, 4)), dma((3,)), dma((4, 2)), dma(()),
            dma((4, 4, 2, 2)), dma((4, 2, 2)), dma((4, 2, 2, 2)), dma((4, 2, 2)),
            dma((2, 2)), dma((2, 2)), dma((2, 2, 2)), dma((2, 2, 2)),
            dma((local_count, 3)), dma((local_count, 3)), dma((local_count, 3)), dma((local_count, 3)),
        ]
        return pl.pallas_call(
            functools.partial(kernel, side, cap),
            out_shape=jax.ShapeDtypeStruct(tokens.shape, tokens.dtype),
            in_specs=[vmem, vmem] + [hbm] * 7,
            out_specs=vmem,
            scratch_shapes=scratch,
            compiler_params=pltpu.CompilerParams(collective_id=0, has_side_effects=True, vmem_limit_bytes=67043328),
        )(expert_ids.T, gate_vals.T, tokens, w_gate, w_up, w_down, shared_gate, shared_up, shared_down)

    row_spec = P(("dp", "ep"), None)
    expert_spec = P("ep", None, None)
    whole_spec = P(None, None)
    return jax.shard_map(moe_step, mesh=mesh, in_specs=(row_spec, row_spec, row_spec, expert_spec, expert_spec, expert_spec, whole_spec, whole_spec, whole_spec), out_specs=row_spec, check_vma=False)
```

```python
import functools
import math

import jax
import jax.numpy as jnp
from jax import lax
from jax.experimental import pallas as pl
from jax.experimental.pallas import tpu as pltpu
from jax.sharding import PartitionSpec as P

F32 = jnp.float32
BF16 = jnp.bfloat16
MESH = pl.DeviceIdType.MESH


def scoped(fn):
    @functools.wraps(fn)
    def run(*a):
        tag = "_".join(str(x) for x in a if isinstance(x, (int, tuple, list, range)))
        with jax.named_scope((fn.__name__ + "#a=" + tag).replace(" ", "").replace("(", "").replace(")", "").replace(",", "_")):
            return fn(*a)
    return run


OFFSETS = (0, -1, 1, 2)
SIDE = (1, 2)

WHOLE = {(0, 0): 0, (0, 1): 1, (0, 2): 2, (0, 3): 3, (1, 0): 4, (1, 2): 5, (2, 1): 6, (2, 3): 7}


def kernel(side, cap, ids_ref, gat_ref, tok_hbm, wg_hbm, wu_hbm, wd_hbm, sg_hbm, su_hbm, sd_hbm, base_hbm, last_hbm,
           w_g, w_u, w_d, tok, info, xg, stage, raw, relay, gsplit, part, acc, half, fin,
           own_sem, tok_r, tu_s, fu_s, tv_s, x_r, xc_s, xf_s, inf_r, iu_s, iv_s, if_s, raw_r, rel_r, f_s, rel_s,
           half_r, half_s, fin_r, fin_s, base_s, sh_sem, wl_sem, wr_s, wr_r):
    tok_count, model_dim = tok_hbm.shape
    top_count = ids_ref.shape[0]
    local_count, _, ff = wg_hbm.shape
    chip_experts = 2 * local_count
    expert_count = local_count * side * side * 2
    block = chip_experts * cap
    piece = tok_count // 2
    chunks = 2
    width = model_dim // chunks

    me = lax.axis_index("ep")
    c = me % 2
    chip = me // 2
    cx, cy = chip % side, chip // side
    u = (1 - c) * cx + c * cy
    v = (1 - c) * cy + c * cx

    def chip_at(uu, vv):
        uu, vv = (uu + side) % side, (vv + side) % side
        return (1 - c) * (vv * side + uu) + c * (uu * side + vv)

    def dev_at(uu, vv):
        return chip_at(uu, vv) * 2 + c

    u_dev = (dev_at(u + 1, v), dev_at(u - 1, v))
    v_dev = (dev_at(u, v + 1), dev_at(u, v - 1))
    v_chip = (chip_at(u, v + 1), chip_at(u, v - 1))
    partner = chip * 2 + (1 - c)

    sent = []

    def send(src, dst, ssem, rsem, dev, keep=True):
        copy = pltpu.make_async_remote_copy(src_ref=src, dst_ref=dst, send_sem=ssem, recv_sem=rsem,
                                            device_id={"ep": dev}, device_id_type=MESH)
        copy.start()
        if keep:
            sent.append(copy)
        return copy

    def arrived(dst, rsem):
        pltpu.make_async_remote_copy(src_ref=dst, dst_ref=dst, send_sem=half_s.at[0, 0], recv_sem=rsem,
                                     device_id={"ep": me}, device_id_type=MESH).wait_recv()

    def rows_of(p):
        return pl.ds(p * piece, piece)

    own = pltpu.make_async_copy(tok_hbm, tok.at[0], own_sem)
    own.start()
    shared_loads = []
    for i in range(local_count):
        cols = pl.ds(i * ff, ff)
        for j, (src, dst) in enumerate(((sg_hbm.at[:, cols], w_g), (su_hbm.at[:, cols], w_u), (sd_hbm.at[cols], w_d))):
            copy = pltpu.make_async_copy(src, dst.at[i], sh_sem.at[i, j])
            copy.start()
            shared_loads.append(copy)

    barrier = pltpu.get_barrier_semaphore()
    for dev in u_dev + v_dev + (partner,):
        pl.semaphore_signal(barrier, inc=1, device_id={"ep": dev}, device_id_type=MESH)
    expert = lax.broadcasted_iota(jnp.int32, (expert_count, tok_count), 0)
    hots = []
    chosen = jnp.zeros((expert_count, tok_count), F32)
    for j in range(top_count):
        hot = (ids_ref[j:j + 1, :] == expert).astype(F32)
        hots.append(hot)
        chosen = chosen + hot
    above = (lax.broadcasted_iota(jnp.int32, (tok_count, tok_count), 0)
             < lax.broadcasted_iota(jnp.int32, (tok_count, tok_count), 1)).astype(F32).astype(BF16)
    slot = jnp.dot(chosen.astype(BF16), above, preferred_element_type=F32)
    info[0, 0] = jnp.zeros((16, tok_count), F32)
    for j in range(top_count):
        info[0, 0, j:j + 1, :] = ids_ref[j:j + 1, :].astype(F32) * cap + jnp.sum(hots[j] * slot, axis=0, keepdims=True)
        info[0, 0, 8 + j:9 + j, :] = gat_ref[j:j + 1, :]

    @scoped
    def tok_wait(g, k, p):
        arrived(tok.at[WHOLE[g, k], rows_of(p)], tok_r.at[WHOLE[g, k], p])

    def send_u_own():
        for order in range(2):
            for d in range(2):
                p = (d + order) % 2
                send(tok.at[0, rows_of(p)], tok.at[SIDE[d], rows_of(p)], tu_s.at[d, p], tok_r.at[SIDE[d], p], u_dev[d])

    @scoped
    def forward_u(d):
        tok_wait(0, SIDE[d], d)
        send(tok.at[SIDE[d], rows_of(d)], tok.at[3, rows_of(d)], fu_s.at[d], tok_r.at[3, d], u_dev[d])

    def whole_v(k, p):
        d = k % 2
        at = WHOLE[SIDE[d], k]
        send(tok.at[k, rows_of(p)], tok.at[at, rows_of(p)], tv_s.at[k, p], tok_r.at[at, p], v_dev[d])

    slot_rows = lax.broadcasted_iota(jnp.int32, (block, tok_count), 0) + c * (local_count * cap)
    turned = jnp.where(slot_rows >= block, slot_rows - block, slot_rows)
    n_step = 512 if model_dim % 512 == 0 else model_dim

    def row_codes(chip_idx):
        return (turned + chip_idx * block).astype(F32)

    def pick(g, k, chip_idx, dst, first):
        codes = row_codes(chip_idx)
        hit = jnp.zeros((block, tok_count), F32)
        for j in range(top_count):
            hit = hit + (info[g, k, j:j + 1, :] == codes).astype(F32)
        hit = hit.astype(BF16)
        for n in range(0, model_dim, n_step):
            x = jnp.dot(hit, tok[WHOLE[g, k], :, n:n + n_step], preferred_element_type=F32).astype(BF16)
            for e in range(chip_experts):
                dst[e, first:first + cap, n:n + n_step] = x[e * cap:(e + 1) * cap]

    def group_rows(k):
        return pl.ds(k * cap, cap)

    near = [None] * 4

    @scoped
    def near_v(k):
        d = 1 - k % 2
        pick(0, k, v_chip[d], stage.at[k], 0)
        near[k] = send(stage.at[k], xg.at[SIDE[d], :, group_rows(k)], xc_s.at[k], x_r.at[SIDE[d], k], v_dev[d], False)

    codes_only = pl.ds(0, 8)

    def inf_rows(k):
        return pl.ds(0, 16) if k == 0 else codes_only

    @scoped
    def inf_wait(g, k):
        arrived(info.at[g, k, inf_rows(k)], inf_r.at[g, k])

    @scoped
    def far_v(k):
        d = k % 2
        g = SIDE[d]
        tok_wait(g, k, 0)
        tok_wait(g, k, 1)
        inf_wait(g, k)
        near[k].wait_send()
        pick(g, k, v_chip[d], stage.at[k], 0)
        send(stage.at[k], xg.at[3, :, group_rows(k)], xf_s.at[k], x_r.at[3, k], v_dev[d])
        if k == 0:
            send(info.at[g, 0], info.at[3, 0], if_s, inf_r.at[3, 0], v_dev[d])

    def info_v(k):
        for d in range(2):
            if k == 0 or d == k % 2:
                send(info.at[0, k, inf_rows(k)], info.at[SIDE[d], k, inf_rows(k)], iv_s.at[k, d],
                     inf_r.at[SIDE[d], k], v_dev[d])

    with jax.named_scope('ownwait'):
        own.wait()
    with jax.named_scope('barrier'):
        pl.semaphore_wait(barrier, 5)
    for d in range(2):
        send(info.at[0, 0, codes_only], info.at[0, SIDE[d], codes_only], iu_s.at[d], inf_r.at[0, SIDE[d]], u_dev[d])
    info_v(0)
    send_u_own()
    whole_v(0, 0)
    whole_v(0, 1)
    near_v(0)

    for i in range(local_count):
        for j, (src, dst) in enumerate(((wg_hbm, w_g), (wu_hbm, w_u), (wd_hbm, w_d))):
            send(src.at[i], dst.at[local_count + i], wr_s.at[i, j], wr_r.at[i, j], partner)

    def silu_mul(g, up):
        return (jax.nn.silu(g) * up).astype(BF16)

    @scoped
    def shared_part(i):
        for copy in shared_loads[3 * i:3 * i + 3]:
            copy.wait()
        x = tok[0]
        h = silu_mul(jnp.dot(x, w_g[i], preferred_element_type=F32), jnp.dot(x, w_u[i], preferred_element_type=F32))
        for n in range(0, model_dim, n_step):
            y = jnp.dot(h, w_d[i, :, n:n + n_step], preferred_element_type=F32)
            if i > 0:
                y = y + acc[:, n:n + n_step]
            if i == local_count - 1:
                y = y.astype(BF16).astype(F32) + x[:, n:n + n_step].astype(F32)
            acc[:, n:n + n_step] = y

    own_loads = []

    def load_own(i):
        for j, (src, dst) in enumerate(((wg_hbm, w_g), (wu_hbm, w_u), (wd_hbm, w_d))):
            copy = pltpu.make_async_copy(src.at[i], dst.at[i], wl_sem.at[i, j])
            copy.start()
            own_loads.append(copy)

    for i in range(local_count):
        shared_part(i)
        load_own(i)

    inf_wait(0, 1)
    send(info.at[0, 1, codes_only], info.at[0, 3, codes_only], iu_s.at[2], inf_r.at[0, 3], u_dev[0])
    info_v(1)
    inf_wait(0, 2)
    info_v(2)
    forward_u(0)
    forward_u(1)
    whole_v(1, 0)
    whole_v(2, 1)
    inf_wait(0, 3)
    info_v(3)
    tok_wait(0, 1, 1)
    whole_v(1, 1)
    tok_wait(0, 2, 0)
    whole_v(2, 0)
    near_v(1)
    near_v(2)
    far_v(0)
    for p in range(2):
        tok_wait(0, 3, p)
        whole_v(3, p)
    near_v(3)

    @scoped
    def experts(g):
        def one(e, carry):
            x = xg[g, e]
            h = silu_mul(jnp.dot(x, w_g[e], preferred_element_type=F32), jnp.dot(x, w_u[e], preferred_element_type=F32))
            for n in range(0, model_dim, n_step):
                y = jnp.dot(h, w_d[e, :, n:n + n_step], preferred_element_type=F32).astype(BF16)
                raw[g, 0, e, :, n:n + n_step] = y[0:cap]
                xg[g, e, cap:4 * cap, n:n + n_step] = y[cap:4 * cap]
            return carry

        lax.fori_loop(0, chip_experts, one, 0)

    @scoped
    def own_pick(g, ks):
        for k in ks:
            pick(g, k, chip, xg.at[g], k * cap)

    @scoped
    def x_wait(g, ks):
        for k in ks:
            arrived(xg.at[g, :, group_rows(k)], x_r.at[g, k])

    def e_half(d):
        return pl.ds(d * local_count, local_count)

    def col_chunk(f):
        return slice(None) if f is None else pl.ds(f * width, width)

    @scoped
    def send_rows(g, f=None):
        at = col_chunk(f)
        i = f or 0
        for d in range(2):
            send(xg.at[g, e_half(d), group_rows(3), at], relay.at[g, d, :, :, at], f_s.at[g, d, 1, i],
                 rel_r.at[g, d, i], u_dev[d])
        for d in range(2):
            send(xg.at[g, :, group_rows(2 - d), at], raw.at[g, SIDE[d], :, :, at], f_s.at[g, d, 0, i],
                 raw_r.at[g, SIDE[d], 0, i], u_dev[d])

    @scoped
    def pass_rows(g, f=None):
        at = col_chunk(f)
        i = f or 0
        for d in range(2):
            arrived(relay.at[g, d, :, :, at], rel_r.at[g, d, i])
            send(relay.at[g, d, :, :, at], raw.at[g, 3, e_half(d), :, at], rel_s.at[g, d, i], raw_r.at[g, 3, d, i], u_dev[d])

    @scoped
    def raw_wait(g, f=None):
        at = col_chunk(f)
        i = f or 0
        for m in range(1, 3):
            arrived(raw.at[g, m, :, :, at], raw_r.at[g, m, 0, i])
        for d in range(2):
            arrived(raw.at[g, 3, e_half(d), :, at], raw_r.at[g, 3, d, i])

    @scoped
    def gates_of(g):
        for m in range(4):
            codes = row_codes(chip_at(u + OFFSETS[m], v))
            gate = jnp.zeros((block, tok_count), F32)
            for j in range(top_count):
                gate = gate + jnp.where(info[g, 0, j:j + 1, :] == codes, info[g, 0, 8 + j:9 + j, :], 0.0)
            gate = gate.T
            for s in range(3):
                part_s = gate.astype(BF16)
                gsplit[s * tok_count:(s + 1) * tok_count, m * block:(m + 1) * block] = part_s
                gate = gate - part_s.astype(F32)

    step = 256 if width % 256 == 0 else width

    @scoped
    def gated(g, f=None):
        first, count = (0, model_dim // step) if f is None else (f * (width // step), width // step)

        def cols(n, carry):
            at = pl.ds(pl.multiple_of(n * step, 128), step)
            rows = raw[g, :, :, :, at].reshape(4 * block, step)
            y = jnp.dot(gsplit[...], rows, preferred_element_type=F32)
            y = y[0:tok_count] + y[tok_count:2 * tok_count] + y[2 * tok_count:3 * tok_count]
            if g == 0:
                acc[:, at] = acc[:, at] + y
            else:
                part[g - 1, :, at] = y
            return carry

        lax.fori_loop(first, first + count, cols, 0)

    def send_early(g, d):
        send(part.at[g - 1, rows_of(1 - d)], fin.at[d], fin_s.at[d, chunks], fin_r.at[d, chunks], v_dev[d])

    def send_last(g, d, f):
        at = col_chunk(f)
        send(part.at[g - 1, rows_of(d), at], last_hbm.at[rows_of(d), at], fin_s.at[d, f], fin_r.at[d, f], v_dev[d])

    own_pick(0, range(4))
    for copy in own_loads:
        copy.wait()
    for i in range(local_count):
        for j, dst in enumerate((w_g, w_u, w_d)):
            arrived(dst.at[local_count + i], wr_r.at[i, j])
    experts(0)
    far_v(1)
    send_rows(0)
    far_v(2)
    far_v(3)
    own_pick(1, (0, 2))
    x_wait(1, (1, 3))
    experts(1)
    pass_rows(0)
    send_rows(1)
    own_pick(2, (1, 3))
    x_wait(2, (0, 2))
    experts(2)
    pass_rows(1)
    send_rows(2)
    raw_wait(0)
    gates_of(0)
    gated(0)
    pass_rows(2)
    x_wait(3, range(4))
    experts(3)
    for f in range(chunks):
        send_rows(3, f)
    raw_wait(1)
    gates_of(1)
    gated(1)
    raw_wait(2)
    inf_wait(2, 0)
    gates_of(2)
    pass_rows(3, 0)
    gated(2)
    send_early(1, 1)
    send_early(2, 0)
    for f in range(1, chunks):
        pass_rows(3, f)
    inf_wait(3, 0)
    gates_of(3)
    for f in range(chunks):
        raw_wait(3, f)
        gated(3, f)
        for d in range(2):
            send(part.at[2, rows_of(d), col_chunk(f)], half.at[d, :, col_chunk(f)], half_s.at[d, f], half_r.at[d, f], v_dev[d])
    for f in range(chunks):
        at = slice(f * width, (f + 1) * width)
        for d in range(2):
            g = 2 - d
            arrived(half.at[d, :, col_chunk(f)], half_r.at[d, f])
            rows = slice(d * piece, (d + 1) * piece)
            part[g - 1, rows, at] = part[g - 1, rows, at] + half[d, :, at]
            send_last(g, d, f)

    for d in range(2):
        arrived(fin.at[d], fin_r.at[d, chunks])
        rows = slice((1 - d) * piece, (2 - d) * piece)
        acc[rows] = acc[rows] + fin[d]
    base = pltpu.make_async_copy(acc, base_hbm, base_s)
    base.start()
    for f in range(chunks):
        for d in range(2):
            arrived(last_hbm.at[rows_of(d), col_chunk(f)], fin_r.at[d, f])
    base.wait()

    for copy in sent:
        copy.wait_send()


def solution(mesh):
    group_size = mesh.shape["ep"]
    side = math.isqrt(group_size // 2)

    def moe_step(tokens, expert_ids, gate_vals, w_gate, w_up, w_down, shared_gate, shared_up, shared_down):
        tok_count, model_dim = tokens.shape
        top_count = expert_ids.shape[1]
        local_count, _, ff = w_gate.shape
        expert_count = local_count * group_size
        spread = max(group_size, expert_count // 2)
        cap = (tok_count * top_count + spread - 1) // spread
        block = 2 * local_count * cap
        piece = tok_count // 2
        dma = pltpu.SemaphoreType.DMA
        vmem = pl.BlockSpec(memory_space=pltpu.VMEM)
        hbm = pl.BlockSpec(memory_space=pl.ANY)
        scratch = [
            pltpu.VMEM((2 * local_count, model_dim, ff), BF16),
            pltpu.VMEM((2 * local_count, model_dim, ff), BF16),
            pltpu.VMEM((2 * local_count, ff, model_dim), BF16),
            pltpu.VMEM((len(WHOLE), tok_count, model_dim), BF16),
            pltpu.VMEM((4, 4, 16, tok_count), F32),
            pltpu.VMEM((4, 2 * local_count, 4 * cap, model_dim), BF16),
            pltpu.VMEM((4, 2 * local_count, cap, model_dim), BF16),
            pltpu.VMEM((4, 4, 2 * local_count, cap, model_dim), BF16),
            pltpu.VMEM((4, 2, local_count, cap, model_dim), BF16),
            pltpu.VMEM((3 * tok_count, 4 * block), BF16),
            pltpu.VMEM((3, tok_count, model_dim), F32),
            pltpu.VMEM((tok_count, model_dim), F32),
            pltpu.VMEM((2, piece, model_dim), F32),
            pltpu.VMEM((2, piece, model_dim), F32),
            dma(()), dma((len(WHOLE), 2)), dma((2, 2)), dma((2,)), dma((4, 2)), dma((4, 4)), dma((4,)), dma((4,)),
            dma((4, 4)), dma((3,)), dma((4, 2)), dma(()),
            dma((4, 4, 2, 2)), dma((4, 2, 2)), dma((4, 2, 2, 2)), dma((4, 2, 2)),
            dma((2, 2)), dma((2, 2)), dma((2, 3)), dma((2, 3)), dma(()),
            dma((local_count, 3)), dma((local_count, 3)), dma((local_count, 3)), dma((local_count, 3)),
        ]
        total = jax.ShapeDtypeStruct(tokens.shape, F32)
        base, last = pl.pallas_call(
            functools.partial(kernel, side, cap),
            out_shape=(total, total),
            in_specs=[vmem, vmem] + [hbm] * 7,
            out_specs=(hbm, hbm),
            scratch_shapes=scratch,
            compiler_params=pltpu.CompilerParams(collective_id=0, has_side_effects=True, vmem_limit_bytes=67043328),
        )(expert_ids.T, gate_vals.T, tokens, w_gate, w_up, w_down, shared_gate, shared_up, shared_down)
        return (base + last).astype(tokens.dtype)

    row_spec = P(("dp", "ep"), None)
    expert_spec = P("ep", None, None)
    whole_spec = P(None, None)
    return jax.shard_map(moe_step, mesh=mesh, in_specs=(row_spec, row_spec, row_spec, expert_spec, expert_spec, expert_spec, whole_spec, whole_spec, whole_spec), out_specs=row_spec, check_vma=False)
```

```python
import functools
import math

import jax
import jax.numpy as jnp
from jax import lax
from jax.experimental import pallas as pl
from jax.experimental.pallas import tpu as pltpu
from jax.sharding import PartitionSpec as P

F32 = jnp.float32
BF16 = jnp.bfloat16
MESH = pl.DeviceIdType.MESH


def scoped(fn):
    @functools.wraps(fn)
    def run(*a):
        tag = "_".join(str(x) for x in a if isinstance(x, (int, tuple, list, range)))
        with jax.named_scope((fn.__name__ + "#a=" + tag).replace(" ", "").replace("(", "").replace(")", "").replace(",", "_")):
            return fn(*a)
    return run


OFFSETS = (0, -1, 1, 2)
SIDE = (1, 2)

WHOLE = {(0, 0): 0, (0, 1): 1, (0, 2): 2, (0, 3): 3, (1, 0): 4, (1, 2): 5, (2, 1): 6, (2, 3): 7}


def kernel(side, cap, ids_ref, gat_ref, tok_hbm, wg_hbm, wu_hbm, wd_hbm, sg_hbm, su_hbm, sd_hbm, base_hbm, last_hbm,
           w_g, w_u, w_d, tok, info, xg, stage, raw, relay, gsplit, part, acc, half, fin,
           own_sem, tok_r, tu_s, fu_s, tv_s, x_r, xc_s, xf_s, inf_r, iu_s, iv_s, if_s, raw_r, rel_r, f_s, rel_s,
           half_r, half_s, fin_r, fin_s, base_s, sh_sem, wl_sem, wr_s, wr_r):
    tok_count, model_dim = tok_hbm.shape
    top_count = ids_ref.shape[0]
    local_count, _, ff = wg_hbm.shape
    chip_experts = 2 * local_count
    expert_count = local_count * side * side * 2
    block = chip_experts * cap
    piece = tok_count // 2
    chunks = 2
    width = model_dim // chunks

    me = lax.axis_index("ep")
    c = me % 2
    chip = me // 2
    cx, cy = chip % side, chip // side
    u = (1 - c) * cx + c * cy
    v = (1 - c) * cy + c * cx

    def chip_at(uu, vv):
        uu, vv = (uu + side) % side, (vv + side) % side
        return (1 - c) * (vv * side + uu) + c * (uu * side + vv)

    def dev_at(uu, vv):
        return chip_at(uu, vv) * 2 + c

    u_dev = (dev_at(u + 1, v), dev_at(u - 1, v))
    v_dev = (dev_at(u, v + 1), dev_at(u, v - 1))
    v_chip = (chip_at(u, v + 1), chip_at(u, v - 1))
    partner = chip * 2 + (1 - c)

    sent = []

    def send(src, dst, ssem, rsem, dev, keep=True):
        copy = pltpu.make_async_remote_copy(src_ref=src, dst_ref=dst, send_sem=ssem, recv_sem=rsem,
                                            device_id={"ep": dev}, device_id_type=MESH)
        copy.start()
        if keep:
            sent.append(copy)
        return copy

    def arrived(dst, rsem):
        pltpu.make_async_remote_copy(src_ref=dst, dst_ref=dst, send_sem=half_s.at[0, 0], recv_sem=rsem,
                                     device_id={"ep": me}, device_id_type=MESH).wait_recv()

    def rows_of(p):
        return pl.ds(p * piece, piece)

    own = pltpu.make_async_copy(tok_hbm, tok.at[0], own_sem)
    own.start()
    barrier = pltpu.get_barrier_semaphore()
    for dev in u_dev + v_dev + (partner,):
        pl.semaphore_signal(barrier, inc=1, device_id={"ep": dev}, device_id_type=MESH)
    expert = lax.broadcasted_iota(jnp.int32, (expert_count, tok_count), 0)
    hots = []
    chosen = jnp.zeros((expert_count, tok_count), F32)
    for j in range(top_count):
        hot = (ids_ref[j:j + 1, :] == expert).astype(F32)
        hots.append(hot)
        chosen = chosen + hot
    above = (lax.broadcasted_iota(jnp.int32, (tok_count, tok_count), 0)
             < lax.broadcasted_iota(jnp.int32, (tok_count, tok_count), 1)).astype(F32).astype(BF16)
    slot = jnp.dot(chosen.astype(BF16), above, preferred_element_type=F32)
    info[0, 0] = jnp.zeros((16, tok_count), F32)
    for j in range(top_count):
        info[0, 0, j:j + 1, :] = ids_ref[j:j + 1, :].astype(F32) * cap + jnp.sum(hots[j] * slot, axis=0, keepdims=True)
        info[0, 0, 8 + j:9 + j, :] = gat_ref[j:j + 1, :]

    @scoped
    def tok_wait(g, k, p):
        arrived(tok.at[WHOLE[g, k], rows_of(p)], tok_r.at[WHOLE[g, k], p])

    def send_u_own():
        for order in range(2):
            for d in range(2):
                p = (d + order) % 2
                send(tok.at[0, rows_of(p)], tok.at[SIDE[d], rows_of(p)], tu_s.at[d, p], tok_r.at[SIDE[d], p], u_dev[d])

    @scoped
    def forward_u(d):
        tok_wait(0, SIDE[d], d)
        send(tok.at[SIDE[d], rows_of(d)], tok.at[3, rows_of(d)], fu_s.at[d], tok_r.at[3, d], u_dev[d])

    def whole_v(k, p):
        d = k % 2
        at = WHOLE[SIDE[d], k]
        send(tok.at[k, rows_of(p)], tok.at[at, rows_of(p)], tv_s.at[k, p], tok_r.at[at, p], v_dev[d])

    slot_rows = lax.broadcasted_iota(jnp.int32, (block, tok_count), 0) + c * (local_count * cap)
    turned = jnp.where(slot_rows >= block, slot_rows - block, slot_rows)
    n_step = 512 if model_dim % 512 == 0 else model_dim

    def row_codes(chip_idx):
        return (turned + chip_idx * block).astype(F32)

    def pick(g, k, chip_idx, dst, first):
        codes = row_codes(chip_idx)
        hit = jnp.zeros((block, tok_count), F32)
        for j in range(top_count):
            hit = hit + (info[g, k, j:j + 1, :] == codes).astype(F32)
        hit = hit.astype(BF16)
        for n in range(0, model_dim, n_step):
            x = jnp.dot(hit, tok[WHOLE[g, k], :, n:n + n_step], preferred_element_type=F32).astype(BF16)
            for e in range(chip_experts):
                dst[e, first:first + cap, n:n + n_step] = x[e * cap:(e + 1) * cap]

    def group_rows(k):
        return pl.ds(k * cap, cap)

    near = [None] * 4

    @scoped
    def near_v(k):
        d = 1 - k % 2
        pick(0, k, v_chip[d], stage.at[k], 0)
        near[k] = send(stage.at[k], xg.at[SIDE[d], :, group_rows(k)], xc_s.at[k], x_r.at[SIDE[d], k], v_dev[d], False)

    codes_only = pl.ds(0, 8)

    def inf_rows(k):
        return pl.ds(0, 16) if k == 0 else codes_only

    @scoped
    def inf_wait(g, k):
        arrived(info.at[g, k, inf_rows(k)], inf_r.at[g, k])

    @scoped
    def far_v(k):
        d = k % 2
        g = SIDE[d]
        tok_wait(g, k, 0)
        tok_wait(g, k, 1)
        inf_wait(g, k)
        at = k if k < 3 else 4
        if k < 3:
            near[k].wait_send()
        else:
            sent.append(near[k])
        pick(g, k, v_chip[d], stage.at[at], 0)
        send(stage.at[at], xg.at[3, :, group_rows(k)], xf_s.at[k], x_r.at[3, k], v_dev[d])
        if k == 0:
            send(info.at[g, 0], info.at[3, 0], if_s, inf_r.at[3, 0], v_dev[d])

    def info_v(k):
        for d in range(2):
            if k == 0 or d == k % 2:
                send(info.at[0, k, inf_rows(k)], info.at[SIDE[d], k, inf_rows(k)], iv_s.at[k, d],
                     inf_r.at[SIDE[d], k], v_dev[d])

    with jax.named_scope('ownwait'):
        own.wait()
    with jax.named_scope('barrier'):
        pl.semaphore_wait(barrier, 5)
    for d in range(2):
        send(info.at[0, 0, codes_only], info.at[0, SIDE[d], codes_only], iu_s.at[d], inf_r.at[0, SIDE[d]], u_dev[d])
    info_v(0)
    send_u_own()
    whole_v(0, 0)
    whole_v(0, 1)

    shared_loads = []
    for i in range(local_count):
        cols = pl.ds(i * ff, ff)
        for j, (src, dst) in enumerate(((sg_hbm.at[:, cols], w_g), (su_hbm.at[:, cols], w_u), (sd_hbm.at[cols], w_d))):
            copy = pltpu.make_async_copy(src, dst.at[i], sh_sem.at[i, j])
            copy.start()
            shared_loads.append(copy)

    near_v(0)

    for i in range(local_count):
        for j, (src, dst) in enumerate(((wg_hbm, w_g), (wu_hbm, w_u), (wd_hbm, w_d))):
            send(src.at[i], dst.at[local_count + i], wr_s.at[i, j], wr_r.at[i, j], partner)

    def silu_mul(g, up):
        return (jax.nn.silu(g) * up).astype(BF16)

    @scoped
    def shared_part(i):
        for copy in shared_loads[3 * i:3 * i + 3]:
            copy.wait()
        x = tok[0]
        h = silu_mul(jnp.dot(x, w_g[i], preferred_element_type=F32), jnp.dot(x, w_u[i], preferred_element_type=F32))
        for n in range(0, model_dim, n_step):
            y = jnp.dot(h, w_d[i, :, n:n + n_step], preferred_element_type=F32)
            if i > 0:
                y = y + acc[:, n:n + n_step]
            if i == local_count - 1:
                y = y.astype(BF16).astype(F32) + x[:, n:n + n_step].astype(F32)
            acc[:, n:n + n_step] = y

    own_loads = []

    def load_own(i):
        for j, (src, dst) in enumerate(((wg_hbm, w_g), (wu_hbm, w_u), (wd_hbm, w_d))):
            copy = pltpu.make_async_copy(src.at[i], dst.at[i], wl_sem.at[i, j])
            copy.start()
            own_loads.append(copy)

    for i in range(local_count):
        shared_part(i)
        load_own(i)

    inf_wait(0, 1)
    send(info.at[0, 1, codes_only], info.at[0, 3, codes_only], iu_s.at[2], inf_r.at[0, 3], u_dev[0])
    info_v(1)
    inf_wait(0, 2)
    info_v(2)
    forward_u(0)
    forward_u(1)
    whole_v(1, 0)
    whole_v(2, 1)
    tok_wait(0, 1, 1)
    whole_v(1, 1)
    tok_wait(0, 2, 0)
    whole_v(2, 0)
    near_v(1)
    near_v(2)
    far_v(0)
    for p in range(2):
        tok_wait(0, 3, p)
        whole_v(3, p)
    inf_wait(0, 3)
    info_v(3)
    near_v(3)

    @scoped
    def experts(g):
        def one(e, carry):
            x = xg[g, e]
            h = silu_mul(jnp.dot(x, w_g[e], preferred_element_type=F32), jnp.dot(x, w_u[e], preferred_element_type=F32))
            for n in range(0, model_dim, n_step):
                y = jnp.dot(h, w_d[e, :, n:n + n_step], preferred_element_type=F32).astype(BF16)
                raw[g, 0, e, :, n:n + n_step] = y[0:cap]
                xg[g, e, cap:4 * cap, n:n + n_step] = y[cap:4 * cap]
            return carry

        lax.fori_loop(0, chip_experts, one, 0)

    @scoped
    def own_pick(g, ks):
        for k in ks:
            pick(g, k, chip, xg.at[g], k * cap)

    @scoped
    def x_wait(g, ks):
        for k in ks:
            arrived(xg.at[g, :, group_rows(k)], x_r.at[g, k])

    def e_half(d):
        return pl.ds(d * local_count, local_count)

    def col_chunk(f):
        return slice(None) if f is None else pl.ds(f * width, width)

    @scoped
    def send_rows(g, f=None):
        at = col_chunk(f)
        i = f or 0
        for d in range(2):
            send(xg.at[g, e_half(d), group_rows(3), at], relay.at[g, d, :, :, at], f_s.at[g, d, 1, i],
                 rel_r.at[g, d, i], u_dev[d])
        for d in range(2):
            send(xg.at[g, :, group_rows(2 - d), at], raw.at[g, SIDE[d], :, :, at], f_s.at[g, d, 0, i],
                 raw_r.at[g, SIDE[d], 0, i], u_dev[d])

    @scoped
    def pass_rows(g, f=None):
        at = col_chunk(f)
        i = f or 0
        for d in range(2):
            arrived(relay.at[g, d, :, :, at], rel_r.at[g, d, i])
            send(relay.at[g, d, :, :, at], raw.at[g, 3, e_half(d), :, at], rel_s.at[g, d, i], raw_r.at[g, 3, d, i], u_dev[d])

    @scoped
    def raw_wait(g, f=None):
        at = col_chunk(f)
        i = f or 0
        for m in range(1, 3):
            arrived(raw.at[g, m, :, :, at], raw_r.at[g, m, 0, i])
        for d in range(2):
            arrived(raw.at[g, 3, e_half(d), :, at], raw_r.at[g, 3, d, i])

    @scoped
    def gates_of(g):
        for m in range(4):
            codes = row_codes(chip_at(u + OFFSETS[m], v))
            gate = jnp.zeros((block, tok_count), F32)
            for j in range(top_count):
                gate = gate + jnp.where(info[g, 0, j:j + 1, :] == codes, info[g, 0, 8 + j:9 + j, :], 0.0)
            gate = gate.T
            for s in range(3):
                part_s = gate.astype(BF16)
                gsplit[s * tok_count:(s + 1) * tok_count, m * block:(m + 1) * block] = part_s
                gate = gate - part_s.astype(F32)

    step = 256 if width % 256 == 0 else width

    @scoped
    def gated(g, f=None):
        first, count = (0, model_dim // step) if f is None else (f * (width // step), width // step)

        def cols(n, carry):
            at = pl.ds(pl.multiple_of(n * step, 128), step)
            rows = raw[g, :, :, :, at].reshape(4 * block, step)
            y = jnp.dot(gsplit[...], rows, preferred_element_type=F32)
            y = y[0:tok_count] + y[tok_count:2 * tok_count] + y[2 * tok_count:3 * tok_count]
            if g == 0:
                acc[:, at] = acc[:, at] + y
            else:
                part[g - 1, :, at] = y
            return carry

        lax.fori_loop(first, first + count, cols, 0)

    def send_early(g, d):
        send(part.at[g - 1, rows_of(1 - d)], fin.at[d], fin_s.at[d, chunks], fin_r.at[d, chunks], v_dev[d])

    def send_last(g, d, f):
        at = col_chunk(f)
        send(part.at[g - 1, rows_of(d), at], last_hbm.at[rows_of(d), at], fin_s.at[d, f], fin_r.at[d, f], v_dev[d])

    own_pick(0, range(4))
    for copy in own_loads:
        copy.wait()
    for i in range(local_count):
        for j, dst in enumerate((w_g, w_u, w_d)):
            arrived(dst.at[local_count + i], wr_r.at[i, j])
    experts(0)
    far_v(1)
    send_rows(0)
    far_v(2)
    far_v(3)
    pass_rows(0)
    own_pick(1, (0, 2))
    x_wait(1, (1, 3))
    experts(1)
    send_rows(1)
    own_pick(2, (1, 3))
    x_wait(2, (0, 2))
    experts(2)
    pass_rows(1)
    send_rows(2)
    raw_wait(0)
    gates_of(0)
    gated(0)
    pass_rows(2)
    x_wait(3, range(4))
    experts(3)
    for f in range(chunks):
        send_rows(3, f)
    raw_wait(1)
    gates_of(1)
    gated(1)
    raw_wait(2)
    inf_wait(2, 0)
    gates_of(2)
    pass_rows(3, 0)
    gated(2)
    send_early(1, 1)
    send_early(2, 0)
    for f in range(1, chunks):
        pass_rows(3, f)
    inf_wait(3, 0)
    gates_of(3)
    for f in range(chunks):
        raw_wait(3, f)
        gated(3, f)
        for d in range(2):
            send(part.at[2, rows_of(d), col_chunk(f)], half.at[d, :, col_chunk(f)], half_s.at[d, f], half_r.at[d, f], v_dev[d])
    for f in range(chunks):
        at = slice(f * width, (f + 1) * width)
        for d in range(2):
            g = 2 - d
            arrived(half.at[d, :, col_chunk(f)], half_r.at[d, f])
            rows = slice(d * piece, (d + 1) * piece)
            part[g - 1, rows, at] = part[g - 1, rows, at] + half[d, :, at]
            send_last(g, d, f)

    for d in range(2):
        arrived(fin.at[d], fin_r.at[d, chunks])
        rows = slice((1 - d) * piece, (2 - d) * piece)
        acc[rows] = acc[rows] + fin[d]
    base = pltpu.make_async_copy(acc, base_hbm, base_s)
    base.start()
    for f in range(chunks):
        for d in range(2):
            arrived(last_hbm.at[rows_of(d), col_chunk(f)], fin_r.at[d, f])
    base.wait()

    for copy in sent:
        copy.wait_send()


def solution(mesh):
    group_size = mesh.shape["ep"]
    side = math.isqrt(group_size // 2)

    def moe_step(tokens, expert_ids, gate_vals, w_gate, w_up, w_down, shared_gate, shared_up, shared_down):
        tok_count, model_dim = tokens.shape
        top_count = expert_ids.shape[1]
        local_count, _, ff = w_gate.shape
        expert_count = local_count * group_size
        spread = max(group_size, expert_count // 2)
        cap = (tok_count * top_count + spread - 1) // spread
        block = 2 * local_count * cap
        piece = tok_count // 2
        dma = pltpu.SemaphoreType.DMA
        vmem = pl.BlockSpec(memory_space=pltpu.VMEM)
        hbm = pl.BlockSpec(memory_space=pl.ANY)
        scratch = [
            pltpu.VMEM((2 * local_count, model_dim, ff), BF16),
            pltpu.VMEM((2 * local_count, model_dim, ff), BF16),
            pltpu.VMEM((2 * local_count, ff, model_dim), BF16),
            pltpu.VMEM((len(WHOLE), tok_count, model_dim), BF16),
            pltpu.VMEM((4, 4, 16, tok_count), F32),
            pltpu.VMEM((4, 2 * local_count, 4 * cap, model_dim), BF16),
            pltpu.VMEM((5, 2 * local_count, cap, model_dim), BF16),
            pltpu.VMEM((4, 4, 2 * local_count, cap, model_dim), BF16),
            pltpu.VMEM((4, 2, local_count, cap, model_dim), BF16),
            pltpu.VMEM((3 * tok_count, 4 * block), BF16),
            pltpu.VMEM((3, tok_count, model_dim), F32),
            pltpu.VMEM((tok_count, model_dim), F32),
            pltpu.VMEM((2, piece, model_dim), F32),
            pltpu.VMEM((2, piece, model_dim), F32),
            dma(()), dma((len(WHOLE), 2)), dma((2, 2)), dma((2,)), dma((4, 2)), dma((4, 4)), dma((4,)), dma((4,)),
            dma((4, 4)), dma((3,)), dma((4, 2)), dma(()),
            dma((4, 4, 2, 2)), dma((4, 2, 2)), dma((4, 2, 2, 2)), dma((4, 2, 2)),
            dma((2, 2)), dma((2, 2)), dma((2, 3)), dma((2, 3)), dma(()),
            dma((local_count, 3)), dma((local_count, 3)), dma((local_count, 3)), dma((local_count, 3)),
        ]
        total = jax.ShapeDtypeStruct(tokens.shape, F32)
        base, last = pl.pallas_call(
            functools.partial(kernel, side, cap),
            out_shape=(total, total),
            in_specs=[vmem, vmem] + [hbm] * 7,
            out_specs=(hbm, hbm),
            scratch_shapes=scratch,
            compiler_params=pltpu.CompilerParams(collective_id=0, has_side_effects=True, vmem_limit_bytes=67043328),
        )(expert_ids.T, gate_vals.T, tokens, w_gate, w_up, w_down, shared_gate, shared_up, shared_down)
        return (base + last).astype(tokens.dtype)

    row_spec = P(("dp", "ep"), None)
    expert_spec = P("ep", None, None)
    whole_spec = P(None, None)
    return jax.shard_map(moe_step, mesh=mesh, in_specs=(row_spec, row_spec, row_spec, expert_spec, expert_spec, expert_spec, whole_spec, whole_spec, whole_spec), out_specs=row_spec, check_vma=False)
```

```python
import functools
import math

import jax
import jax.numpy as jnp
from jax import lax
from jax.experimental import pallas as pl
from jax.experimental.pallas import tpu as pltpu
from jax.sharding import PartitionSpec as P

F32 = jnp.float32
BF16 = jnp.bfloat16
MESH = pl.DeviceIdType.MESH


def scoped(fn):
    @functools.wraps(fn)
    def run(*a):
        tag = "_".join(str(x) for x in a if isinstance(x, (int, tuple, list, range)))
        with jax.named_scope((fn.__name__ + "#a=" + tag).replace(" ", "").replace("(", "").replace(")", "").replace(",", "_")):
            return fn(*a)
    return run


OFFSETS = (0, -1, 1, 2)
SIDE = (1, 2)

WHOLE = {(0, 0): 0, (0, 1): 1, (0, 2): 2, (0, 3): 3, (1, 0): 4, (1, 2): 5, (2, 1): 6, (2, 3): 7}


def kernel(side, cap, ids_ref, gat_ref, tok_hbm, wg_hbm, wu_hbm, wd_hbm, sg_hbm, su_hbm, sd_hbm, base_hbm, last_hbm,
           w_g, w_u, w_d, tok, info, xg, stage, raw, relay, gsplit, part, acc, half, fin,
           own_sem, tok_r, tu_s, fu_s, tv_s, x_r, xc_s, xf_s, inf_r, iu_s, iv_s, if_s, raw_r, rel_r, f_s, rel_s,
           half_r, half_s, fin_r, fin_s, base_s, sh_sem, wl_sem, wr_s, wr_r):
    tok_count, model_dim = tok_hbm.shape
    top_count = ids_ref.shape[0]
    local_count, _, ff = wg_hbm.shape
    chip_experts = 2 * local_count
    expert_count = local_count * side * side * 2
    block = chip_experts * cap
    piece = tok_count // 2
    chunks = 2
    width = model_dim // chunks

    me = lax.axis_index("ep")
    c = me % 2
    chip = me // 2
    cx, cy = chip % side, chip // side
    u = (1 - c) * cx + c * cy
    v = (1 - c) * cy + c * cx

    def chip_at(uu, vv):
        uu, vv = (uu + side) % side, (vv + side) % side
        return (1 - c) * (vv * side + uu) + c * (uu * side + vv)

    def dev_at(uu, vv):
        return chip_at(uu, vv) * 2 + c

    u_dev = (dev_at(u + 1, v), dev_at(u - 1, v))
    v_dev = (dev_at(u, v + 1), dev_at(u, v - 1))
    v_chip = (chip_at(u, v + 1), chip_at(u, v - 1))
    partner = chip * 2 + (1 - c)

    sent = []

    def send(src, dst, ssem, rsem, dev, keep=True):
        copy = pltpu.make_async_remote_copy(src_ref=src, dst_ref=dst, send_sem=ssem, recv_sem=rsem,
                                            device_id={"ep": dev}, device_id_type=MESH)
        copy.start()
        if keep:
            sent.append(copy)
        return copy

    def arrived(dst, rsem):
        pltpu.make_async_remote_copy(src_ref=dst, dst_ref=dst, send_sem=half_s.at[0, 0], recv_sem=rsem,
                                     device_id={"ep": me}, device_id_type=MESH).wait_recv()

    def rows_of(p):
        return pl.ds(p * piece, piece)

    own = pltpu.make_async_copy(tok_hbm, tok.at[0], own_sem)
    own.start()
    barrier = pltpu.get_barrier_semaphore()
    for dev in u_dev + v_dev + (partner,):
        pl.semaphore_signal(barrier, inc=1, device_id={"ep": dev}, device_id_type=MESH)
    expert = lax.broadcasted_iota(jnp.int32, (expert_count, tok_count), 0)
    hots = []
    chosen = jnp.zeros((expert_count, tok_count), F32)
    for j in range(top_count):
        hot = (ids_ref[j:j + 1, :] == expert).astype(F32)
        hots.append(hot)
        chosen = chosen + hot
    above = (lax.broadcasted_iota(jnp.int32, (tok_count, tok_count), 0)
             < lax.broadcasted_iota(jnp.int32, (tok_count, tok_count), 1)).astype(F32).astype(BF16)
    slot = jnp.dot(chosen.astype(BF16), above, preferred_element_type=F32)
    info[0, 0] = jnp.zeros((16, tok_count), F32)
    for j in range(top_count):
        info[0, 0, j:j + 1, :] = ids_ref[j:j + 1, :].astype(F32) * cap + jnp.sum(hots[j] * slot, axis=0, keepdims=True)
        info[0, 0, 8 + j:9 + j, :] = gat_ref[j:j + 1, :]

    @scoped
    def tok_wait(g, k, p):
        arrived(tok.at[WHOLE[g, k], rows_of(p)], tok_r.at[WHOLE[g, k], p])

    def send_u_own():
        for order in range(2):
            for d in range(2):
                p = (d + order) % 2
                send(tok.at[0, rows_of(p)], tok.at[SIDE[d], rows_of(p)], tu_s.at[d, p], tok_r.at[SIDE[d], p], u_dev[d])

    @scoped
    def forward_u(d):
        tok_wait(0, SIDE[d], d)
        send(tok.at[SIDE[d], rows_of(d)], tok.at[3, rows_of(d)], fu_s.at[d], tok_r.at[3, d], u_dev[d])

    def whole_v(k, p):
        d = k % 2
        at = WHOLE[SIDE[d], k]
        send(tok.at[k, rows_of(p)], tok.at[at, rows_of(p)], tv_s.at[k, p], tok_r.at[at, p], v_dev[d])

    slot_rows = lax.broadcasted_iota(jnp.int32, (block, tok_count), 0) + c * (local_count * cap)
    turned = jnp.where(slot_rows >= block, slot_rows - block, slot_rows)
    n_step = 512 if model_dim % 512 == 0 else model_dim

    def row_codes(chip_idx):
        return (turned + chip_idx * block).astype(F32)

    def pick(g, k, chip_idx, dst, first):
        codes = row_codes(chip_idx)
        hit = jnp.zeros((block, tok_count), F32)
        for j in range(top_count):
            hit = hit + (info[g, k, j:j + 1, :] == codes).astype(F32)
        hit = hit.astype(BF16)
        for n in range(0, model_dim, n_step):
            x = jnp.dot(hit, tok[WHOLE[g, k], :, n:n + n_step], preferred_element_type=F32).astype(BF16)
            for e in range(chip_experts):
                dst[e, first:first + cap, n:n + n_step] = x[e * cap:(e + 1) * cap]

    def group_rows(k):
        return pl.ds(k * cap, cap)

    near = [None] * 4

    @scoped
    def near_v(k):
        d = 1 - k % 2
        pick(0, k, v_chip[d], stage.at[k], 0)
        near[k] = send(stage.at[k], xg.at[SIDE[d], :, group_rows(k)], xc_s.at[k], x_r.at[SIDE[d], k], v_dev[d], False)

    codes_only = pl.ds(0, 8)

    def inf_rows(k):
        return pl.ds(0, 16) if k == 0 else codes_only

    @scoped
    def inf_wait(g, k):
        arrived(info.at[g, k, inf_rows(k)], inf_r.at[g, k])

    @scoped
    def far_v(k):
        d = k % 2
        g = SIDE[d]
        tok_wait(g, k, 0)
        tok_wait(g, k, 1)
        inf_wait(g, k)
        at = k if k < 3 else 4
        if k < 3:
            near[k].wait_send()
        else:
            sent.append(near[k])
        pick(g, k, v_chip[d], stage.at[at], 0)
        send(stage.at[at], xg.at[3, :, group_rows(k)], xf_s.at[k], x_r.at[3, k], v_dev[d])
        if k == 0:
            send(info.at[g, 0], info.at[3, 0], if_s, inf_r.at[3, 0], v_dev[d])

    def info_v(k):
        for d in range(2):
            if k == 0 or d == k % 2:
                send(info.at[0, k, inf_rows(k)], info.at[SIDE[d], k, inf_rows(k)], iv_s.at[k, d],
                     inf_r.at[SIDE[d], k], v_dev[d])

    with jax.named_scope('ownwait'):
        own.wait()
    with jax.named_scope('barrier'):
        pl.semaphore_wait(barrier, 5)
    for d in range(2):
        send(info.at[0, 0, codes_only], info.at[0, SIDE[d], codes_only], iu_s.at[d], inf_r.at[0, SIDE[d]], u_dev[d])
    info_v(0)
    send_u_own()
    whole_v(0, 0)
    whole_v(0, 1)

    shared_loads = []
    for i in range(local_count):
        cols = pl.ds(i * ff, ff)
        for j, (src, dst) in enumerate(((sg_hbm.at[:, cols], w_g), (su_hbm.at[:, cols], w_u), (sd_hbm.at[cols], w_d))):
            copy = pltpu.make_async_copy(src, dst.at[i], sh_sem.at[i, j])
            copy.start()
            shared_loads.append(copy)

    near_v(0)

    for i in range(local_count):
        for j, (src, dst) in enumerate(((wg_hbm, w_g), (wu_hbm, w_u), (wd_hbm, w_d))):
            send(src.at[i], dst.at[local_count + i], wr_s.at[i, j], wr_r.at[i, j], partner)

    def silu_mul(g, up):
        return (jax.nn.silu(g) * up).astype(BF16)

    @scoped
    def shared_part(i):
        for copy in shared_loads[3 * i:3 * i + 3]:
            copy.wait()
        x = tok[0]
        h = silu_mul(jnp.dot(x, w_g[i], preferred_element_type=F32), jnp.dot(x, w_u[i], preferred_element_type=F32))
        for n in range(0, model_dim, n_step):
            y = jnp.dot(h, w_d[i, :, n:n + n_step], preferred_element_type=F32)
            if i > 0:
                y = y + acc[:, n:n + n_step]
            if i == local_count - 1:
                y = y.astype(BF16).astype(F32) + x[:, n:n + n_step].astype(F32)
            acc[:, n:n + n_step] = y

    own_loads = []

    def load_own(i):
        for j, (src, dst) in enumerate(((wg_hbm, w_g), (wu_hbm, w_u), (wd_hbm, w_d))):
            copy = pltpu.make_async_copy(src.at[i], dst.at[i], wl_sem.at[i, j])
            copy.start()
            own_loads.append(copy)

    for i in range(local_count):
        shared_part(i)
        load_own(i)

    inf_wait(0, 1)
    send(info.at[0, 1, codes_only], info.at[0, 3, codes_only], iu_s.at[2], inf_r.at[0, 3], u_dev[0])
    info_v(1)
    inf_wait(0, 2)
    info_v(2)
    forward_u(0)
    forward_u(1)
    whole_v(1, 0)
    whole_v(2, 1)
    tok_wait(0, 1, 1)
    whole_v(1, 1)
    tok_wait(0, 2, 0)
    whole_v(2, 0)
    near_v(1)
    near_v(2)
    far_v(0)
    for p in range(2):
        tok_wait(0, 3, p)
        whole_v(3, p)
    inf_wait(0, 3)
    info_v(3)
    near_v(3)

    @scoped
    def experts(g):
        def one(e, carry):
            x = xg[g, e]
            h = silu_mul(jnp.dot(x, w_g[e], preferred_element_type=F32), jnp.dot(x, w_u[e], preferred_element_type=F32))
            for n in range(0, model_dim, n_step):
                y = jnp.dot(h, w_d[e, :, n:n + n_step], preferred_element_type=F32).astype(BF16)
                raw[g, 0, e, :, n:n + n_step] = y[0:cap]
                xg[g, e, cap:4 * cap, n:n + n_step] = y[cap:4 * cap]
            return carry

        lax.fori_loop(0, chip_experts, one, 0)

    @scoped
    def own_pick(g, ks):
        for k in ks:
            pick(g, k, chip, xg.at[g], k * cap)

    @scoped
    def x_wait(g, ks):
        for k in ks:
            arrived(xg.at[g, :, group_rows(k)], x_r.at[g, k])

    def e_half(d):
        return pl.ds(d * local_count, local_count)

    def col_chunk(f):
        return slice(None) if f is None else pl.ds(f * width, width)

    @scoped
    def send_rows(g, f=None):
        at = col_chunk(f)
        i = f or 0
        for d in range(2):
            send(xg.at[g, e_half(d), group_rows(3), at], relay.at[g, d, :, :, at], f_s.at[g, d, 1, i],
                 rel_r.at[g, d, i], u_dev[d])
        for d in range(2):
            send(xg.at[g, :, group_rows(2 - d), at], raw.at[g, SIDE[d], :, :, at], f_s.at[g, d, 0, i],
                 raw_r.at[g, SIDE[d], 0, i], u_dev[d])

    @scoped
    def pass_rows(g, f=None):
        at = col_chunk(f)
        i = f or 0
        for d in range(2):
            arrived(relay.at[g, d, :, :, at], rel_r.at[g, d, i])
            send(relay.at[g, d, :, :, at], raw.at[g, 3, e_half(d), :, at], rel_s.at[g, d, i], raw_r.at[g, 3, d, i], u_dev[d])

    @scoped
    def raw_wait(g, f=None):
        at = col_chunk(f)
        i = f or 0
        for m in range(1, 3):
            arrived(raw.at[g, m, :, :, at], raw_r.at[g, m, 0, i])
        for d in range(2):
            arrived(raw.at[g, 3, e_half(d), :, at], raw_r.at[g, 3, d, i])

    @scoped
    def gates_of(g):
        for m in range(4):
            codes = row_codes(chip_at(u + OFFSETS[m], v))
            gate = jnp.zeros((block, tok_count), F32)
            for j in range(top_count):
                gate = gate + jnp.where(info[g, 0, j:j + 1, :] == codes, info[g, 0, 8 + j:9 + j, :], 0.0)
            gate = gate.T
            for s in range(3):
                part_s = gate.astype(BF16)
                gsplit[s * tok_count:(s + 1) * tok_count, m * block:(m + 1) * block] = part_s
                gate = gate - part_s.astype(F32)

    step = 256 if width % 256 == 0 else width

    @scoped
    def gated(g, f=None):
        first, count = (0, model_dim // step) if f is None else (f * (width // step), width // step)

        def cols(n, carry):
            at = pl.ds(pl.multiple_of(n * step, 128), step)
            rows = raw[g, :, :, :, at].reshape(4 * block, step)
            y = jnp.dot(gsplit[...], rows, preferred_element_type=F32)
            y = y[0:tok_count] + y[tok_count:2 * tok_count] + y[2 * tok_count:3 * tok_count]
            if g == 0:
                acc[:, at] = acc[:, at] + y
            else:
                part[g - 1, :, at] = y
            return carry

        lax.fori_loop(first, first + count, cols, 0)

    def send_early(g, d):
        send(part.at[g - 1, rows_of(1 - d)], fin.at[d], fin_s.at[d, chunks], fin_r.at[d, chunks], v_dev[d])

    def send_last(g, d, f):
        at = col_chunk(f)
        send(part.at[g - 1, rows_of(d), at], last_hbm.at[rows_of(d), at], fin_s.at[d, f], fin_r.at[d, f], v_dev[d])

    own_pick(0, range(4))
    for copy in own_loads:
        copy.wait()
    for i in range(local_count):
        for j, dst in enumerate((w_g, w_u, w_d)):
            arrived(dst.at[local_count + i], wr_r.at[i, j])
    experts(0)
    far_v(1)
    send_rows(0)
    far_v(2)
    far_v(3)
    pass_rows(0)
    own_pick(2, (1, 3))
    x_wait(2, (0, 2))
    experts(2)
    send_rows(2)
    own_pick(1, (0, 2))
    pass_rows(2)
    x_wait(1, (1, 3))
    experts(1)
    send_rows(1)
    raw_wait(0)
    gates_of(0)
    gated(0)
    x_wait(3, range(4))
    experts(3)
    pass_rows(1)
    for f in range(chunks):
        send_rows(3, f)
    raw_wait(2)
    inf_wait(2, 0)
    gates_of(2)
    gated(2)
    inf_wait(3, 0)
    raw_wait(1)
    gates_of(1)
    pass_rows(3, 0)
    gated(1)
    send_early(1, 1)
    send_early(2, 0)
    for f in range(1, chunks):
        pass_rows(3, f)
    gates_of(3)
    for f in range(chunks):
        raw_wait(3, f)
        gated(3, f)
        for d in range(2):
            send(part.at[2, rows_of(d), col_chunk(f)], half.at[d, :, col_chunk(f)], half_s.at[d, f], half_r.at[d, f], v_dev[d])
    for f in range(chunks):
        at = slice(f * width, (f + 1) * width)
        for d in range(2):
            g = 2 - d
            arrived(half.at[d, :, col_chunk(f)], half_r.at[d, f])
            rows = slice(d * piece, (d + 1) * piece)
            part[g - 1, rows, at] = part[g - 1, rows, at] + half[d, :, at]
            send_last(g, d, f)

    for d in range(2):
        arrived(fin.at[d], fin_r.at[d, chunks])
        rows = slice((1 - d) * piece, (2 - d) * piece)
        acc[rows] = acc[rows] + fin[d]
    base = pltpu.make_async_copy(acc, base_hbm, base_s)
    base.start()
    for f in range(chunks):
        for d in range(2):
            arrived(last_hbm.at[rows_of(d), col_chunk(f)], fin_r.at[d, f])
    base.wait()

    for copy in sent:
        copy.wait_send()


def solution(mesh):
    group_size = mesh.shape["ep"]
    side = math.isqrt(group_size // 2)

    def moe_step(tokens, expert_ids, gate_vals, w_gate, w_up, w_down, shared_gate, shared_up, shared_down):
        tok_count, model_dim = tokens.shape
        top_count = expert_ids.shape[1]
        local_count, _, ff = w_gate.shape
        expert_count = local_count * group_size
        spread = max(group_size, expert_count // 2)
        cap = (tok_count * top_count + spread - 1) // spread
        block = 2 * local_count * cap
        piece = tok_count // 2
        dma = pltpu.SemaphoreType.DMA
        vmem = pl.BlockSpec(memory_space=pltpu.VMEM)
        hbm = pl.BlockSpec(memory_space=pl.ANY)
        scratch = [
            pltpu.VMEM((2 * local_count, model_dim, ff), BF16),
            pltpu.VMEM((2 * local_count, model_dim, ff), BF16),
            pltpu.VMEM((2 * local_count, ff, model_dim), BF16),
            pltpu.VMEM((len(WHOLE), tok_count, model_dim), BF16),
            pltpu.VMEM((4, 4, 16, tok_count), F32),
            pltpu.VMEM((4, 2 * local_count, 4 * cap, model_dim), BF16),
            pltpu.VMEM((5, 2 * local_count, cap, model_dim), BF16),
            pltpu.VMEM((4, 4, 2 * local_count, cap, model_dim), BF16),
            pltpu.VMEM((4, 2, local_count, cap, model_dim), BF16),
            pltpu.VMEM((3 * tok_count, 4 * block), BF16),
            pltpu.VMEM((3, tok_count, model_dim), F32),
            pltpu.VMEM((tok_count, model_dim), F32),
            pltpu.VMEM((2, piece, model_dim), F32),
            pltpu.VMEM((2, piece, model_dim), F32),
            dma(()), dma((len(WHOLE), 2)), dma((2, 2)), dma((2,)), dma((4, 2)), dma((4, 4)), dma((4,)), dma((4,)),
            dma((4, 4)), dma((3,)), dma((4, 2)), dma(()),
            dma((4, 4, 2, 2)), dma((4, 2, 2)), dma((4, 2, 2, 2)), dma((4, 2, 2)),
            dma((2, 2)), dma((2, 2)), dma((2, 3)), dma((2, 3)), dma(()),
            dma((local_count, 3)), dma((local_count, 3)), dma((local_count, 3)), dma((local_count, 3)),
        ]
        total = jax.ShapeDtypeStruct(tokens.shape, F32)
        base, last = pl.pallas_call(
            functools.partial(kernel, side, cap),
            out_shape=(total, total),
            in_specs=[vmem, vmem] + [hbm] * 7,
            out_specs=(hbm, hbm),
            scratch_shapes=scratch,
            compiler_params=pltpu.CompilerParams(collective_id=0, has_side_effects=True, vmem_limit_bytes=67043328),
        )(expert_ids.T, gate_vals.T, tokens, w_gate, w_up, w_down, shared_gate, shared_up, shared_down)
        return (base + last).astype(tokens.dtype)

    row_spec = P(("dp", "ep"), None)
    expert_spec = P("ep", None, None)
    whole_spec = P(None, None)
    return jax.shard_map(moe_step, mesh=mesh, in_specs=(row_spec, row_spec, row_spec, expert_spec, expert_spec, expert_spec, whole_spec, whole_spec, whole_spec), out_specs=row_spec, check_vma=False)
```

```python
import functools
import math

import jax
import jax.numpy as jnp
from jax import lax
from jax.experimental import pallas as pl
from jax.experimental.pallas import tpu as pltpu
from jax.sharding import PartitionSpec as P

F32 = jnp.float32
BF16 = jnp.bfloat16
MESH = pl.DeviceIdType.MESH


def scoped(fn):
    @functools.wraps(fn)
    def run(*a):
        tag = "_".join(str(x) for x in a if isinstance(x, (int, tuple, list, range)))
        with jax.named_scope((fn.__name__ + "#a=" + tag).replace(" ", "").replace("(", "").replace(")", "").replace(",", "_")):
            return fn(*a)
    return run


OFFSETS = (0, -1, 1, 2)
SIDE = (1, 2)

WHOLE = {(0, 0): 0, (0, 1): 1, (0, 2): 2, (0, 3): 3, (1, 0): 4, (1, 2): 5, (2, 1): 6, (2, 3): 7}


def kernel(side, cap, ids_hbm, gat_hbm, tok_hbm, wg_hbm, wu_hbm, wd_hbm, sg_hbm, su_hbm, sd_hbm, acc, last,
           ids_ref, gat_ref, w_g, w_u, w_d, tok, info, xg, stage, raw, relay, gsplit, part, half, fin,
           own_sem, tok_r, tu_s, fu_s, tv_s, x_r, xc_s, xf_s, inf_r, iu_s, iv_s, if_s, raw_r, rel_r, f_s, rel_s,
           half_r, half_s, fin_r, fin_s, sh_sem, wl_sem, wr_s, wr_r):
    tok_count, model_dim = tok_hbm.shape
    top_count = ids_hbm.shape[0]
    local_count, _, ff = wg_hbm.shape
    chip_experts = 2 * local_count
    expert_count = local_count * side * side * 2
    block = chip_experts * cap
    piece = tok_count // 2
    chunks = 2
    width = model_dim // chunks

    me = lax.axis_index("ep")
    c = me % 2
    chip = me // 2
    cx, cy = chip % side, chip // side
    u = (1 - c) * cx + c * cy
    v = (1 - c) * cy + c * cx

    def chip_at(uu, vv):
        uu, vv = (uu + side) % side, (vv + side) % side
        return (1 - c) * (vv * side + uu) + c * (uu * side + vv)

    def dev_at(uu, vv):
        return chip_at(uu, vv) * 2 + c

    u_dev = (dev_at(u + 1, v), dev_at(u - 1, v))
    v_dev = (dev_at(u, v + 1), dev_at(u, v - 1))
    v_chip = (chip_at(u, v + 1), chip_at(u, v - 1))
    partner = chip * 2 + (1 - c)

    sent = []

    def send(src, dst, ssem, rsem, dev, keep=True):
        copy = pltpu.make_async_remote_copy(src_ref=src, dst_ref=dst, send_sem=ssem, recv_sem=rsem,
                                            device_id={"ep": dev}, device_id_type=MESH)
        copy.start()
        if keep:
            sent.append(copy)
        return copy

    def arrived(dst, rsem):
        pltpu.make_async_remote_copy(src_ref=dst, dst_ref=dst, send_sem=half_s.at[0, 0], recv_sem=rsem,
                                     device_id={"ep": me}, device_id_type=MESH).wait_recv()

    def rows_of(p):
        return pl.ds(p * piece, piece)

    routes = [pltpu.make_async_copy(src, dst, own_sem.at[i + 1])
              for i, (src, dst) in enumerate(((ids_hbm, ids_ref), (gat_hbm, gat_ref)))]
    for copy in routes:
        copy.start()
    own = pltpu.make_async_copy(tok_hbm, tok.at[0], own_sem.at[0])
    own.start()
    barrier = pltpu.get_barrier_semaphore()
    for dev in u_dev + v_dev + (partner,):
        pl.semaphore_signal(barrier, inc=1, device_id={"ep": dev}, device_id_type=MESH)
    for copy in routes:
        copy.wait()
    expert = lax.broadcasted_iota(jnp.int32, (expert_count, tok_count), 0)
    hots = []
    chosen = jnp.zeros((expert_count, tok_count), F32)
    for j in range(top_count):
        hot = (ids_ref[j:j + 1, :] == expert).astype(F32)
        hots.append(hot)
        chosen = chosen + hot
    above = (lax.broadcasted_iota(jnp.int32, (tok_count, tok_count), 0)
             < lax.broadcasted_iota(jnp.int32, (tok_count, tok_count), 1)).astype(F32).astype(BF16)
    slot = jnp.dot(chosen.astype(BF16), above, preferred_element_type=F32)
    info[0, 0] = jnp.zeros((16, tok_count), F32)
    for j in range(top_count):
        info[0, 0, j:j + 1, :] = ids_ref[j:j + 1, :].astype(F32) * cap + jnp.sum(hots[j] * slot, axis=0, keepdims=True)
        info[0, 0, 8 + j:9 + j, :] = gat_ref[j:j + 1, :]

    @scoped
    def tok_wait(g, k, p):
        arrived(tok.at[WHOLE[g, k], rows_of(p)], tok_r.at[WHOLE[g, k], p])

    def send_u_own():
        for order in range(2):
            for d in range(2):
                p = (d + order) % 2
                send(tok.at[0, rows_of(p)], tok.at[SIDE[d], rows_of(p)], tu_s.at[d, p], tok_r.at[SIDE[d], p], u_dev[d])

    @scoped
    def forward_u(d):
        tok_wait(0, SIDE[d], d)
        send(tok.at[SIDE[d], rows_of(d)], tok.at[3, rows_of(d)], fu_s.at[d], tok_r.at[3, d], u_dev[d])

    def whole_v(k, p):
        d = k % 2
        at = WHOLE[SIDE[d], k]
        send(tok.at[k, rows_of(p)], tok.at[at, rows_of(p)], tv_s.at[k, p], tok_r.at[at, p], v_dev[d])

    slot_rows = lax.broadcasted_iota(jnp.int32, (block, tok_count), 0) + c * (local_count * cap)
    turned = jnp.where(slot_rows >= block, slot_rows - block, slot_rows)
    n_step = 512 if model_dim % 512 == 0 else model_dim

    def row_codes(chip_idx):
        return (turned + chip_idx * block).astype(F32)

    def pick(g, k, chip_idx, dst, first):
        codes = row_codes(chip_idx)
        hit = jnp.zeros((block, tok_count), F32)
        for j in range(top_count):
            hit = hit + (info[g, k, j:j + 1, :] == codes).astype(F32)
        hit = hit.astype(BF16)
        for n in range(0, model_dim, n_step):
            x = jnp.dot(hit, tok[WHOLE[g, k], :, n:n + n_step], preferred_element_type=F32).astype(BF16)
            for e in range(chip_experts):
                dst[e, first:first + cap, n:n + n_step] = x[e * cap:(e + 1) * cap]

    def group_rows(k):
        return pl.ds(k * cap, cap)

    near = [None] * 4

    @scoped
    def near_v(k):
        d = 1 - k % 2
        pick(0, k, v_chip[d], stage.at[k], 0)
        near[k] = send(stage.at[k], xg.at[SIDE[d], :, group_rows(k)], xc_s.at[k], x_r.at[SIDE[d], k], v_dev[d], False)

    codes_only = pl.ds(0, 8)

    def inf_rows(k):
        return pl.ds(0, 16) if k == 0 else codes_only

    @scoped
    def inf_wait(g, k):
        arrived(info.at[g, k, inf_rows(k)], inf_r.at[g, k])

    @scoped
    def far_v(k):
        d = k % 2
        g = SIDE[d]
        tok_wait(g, k, 0)
        tok_wait(g, k, 1)
        inf_wait(g, k)
        at = k if k < 3 else 4
        if k < 3:
            near[k].wait_send()
        else:
            sent.append(near[k])
        pick(g, k, v_chip[d], stage.at[at], 0)
        send(stage.at[at], xg.at[3, :, group_rows(k)], xf_s.at[k], x_r.at[3, k], v_dev[d])
        if k == 0:
            send(info.at[g, 0], info.at[3, 0], if_s, inf_r.at[3, 0], v_dev[d])

    def info_v(k):
        for d in range(2):
            if k == 0 or d == k % 2:
                send(info.at[0, k, inf_rows(k)], info.at[SIDE[d], k, inf_rows(k)], iv_s.at[k, d],
                     inf_r.at[SIDE[d], k], v_dev[d])

    with jax.named_scope('ownwait'):
        own.wait()
    with jax.named_scope('barrier'):
        pl.semaphore_wait(barrier, 5)
    for d in range(2):
        send(info.at[0, 0, codes_only], info.at[0, SIDE[d], codes_only], iu_s.at[d], inf_r.at[0, SIDE[d]], u_dev[d])
    info_v(0)
    send_u_own()
    whole_v(0, 0)
    whole_v(0, 1)

    shared_loads = []
    for i in range(local_count):
        cols = pl.ds(i * ff, ff)
        for j, (src, dst) in enumerate(((sg_hbm.at[:, cols], w_g), (su_hbm.at[:, cols], w_u), (sd_hbm.at[cols], w_d))):
            copy = pltpu.make_async_copy(src, dst.at[i], sh_sem.at[i, j])
            copy.start()
            shared_loads.append(copy)

    near_v(0)

    for i in range(local_count):
        for j, (src, dst) in enumerate(((wg_hbm, w_g), (wu_hbm, w_u), (wd_hbm, w_d))):
            send(src.at[i], dst.at[local_count + i], wr_s.at[i, j], wr_r.at[i, j], partner)

    def silu_mul(g, up):
        return (jax.nn.silu(g) * up).astype(BF16)

    @scoped
    def shared_part(i):
        for copy in shared_loads[3 * i:3 * i + 3]:
            copy.wait()
        x = tok[0]
        h = silu_mul(jnp.dot(x, w_g[i], preferred_element_type=F32), jnp.dot(x, w_u[i], preferred_element_type=F32))
        for n in range(0, model_dim, n_step):
            y = jnp.dot(h, w_d[i, :, n:n + n_step], preferred_element_type=F32)
            if i > 0:
                y = y + acc[:, n:n + n_step]
            if i == local_count - 1:
                y = y.astype(BF16).astype(F32) + x[:, n:n + n_step].astype(F32)
            acc[:, n:n + n_step] = y

    own_loads = []

    def load_own(i):
        for j, (src, dst) in enumerate(((wg_hbm, w_g), (wu_hbm, w_u), (wd_hbm, w_d))):
            copy = pltpu.make_async_copy(src.at[i], dst.at[i], wl_sem.at[i, j])
            copy.start()
            own_loads.append(copy)

    for i in range(local_count):
        shared_part(i)
        load_own(i)

    inf_wait(0, 1)
    send(info.at[0, 1, codes_only], info.at[0, 3, codes_only], iu_s.at[2], inf_r.at[0, 3], u_dev[0])
    info_v(1)
    inf_wait(0, 2)
    info_v(2)
    forward_u(0)
    forward_u(1)
    whole_v(1, 0)
    whole_v(2, 1)
    tok_wait(0, 1, 1)
    whole_v(1, 1)
    tok_wait(0, 2, 0)
    whole_v(2, 0)
    near_v(1)
    near_v(2)
    far_v(0)
    for p in range(2):
        tok_wait(0, 3, p)
        whole_v(3, p)
    inf_wait(0, 3)
    info_v(3)
    near_v(3)

    @scoped
    def experts(g):
        def one(e, carry):
            x = xg[g, e]
            h = silu_mul(jnp.dot(x, w_g[e], preferred_element_type=F32), jnp.dot(x, w_u[e], preferred_element_type=F32))
            for n in range(0, model_dim, n_step):
                y = jnp.dot(h, w_d[e, :, n:n + n_step], preferred_element_type=F32).astype(BF16)
                raw[g, 0, e, :, n:n + n_step] = y[0:cap]
                xg[g, e, cap:4 * cap, n:n + n_step] = y[cap:4 * cap]
            return carry

        lax.fori_loop(0, chip_experts, one, 0)

    @scoped
    def own_pick(g, ks):
        for k in ks:
            pick(g, k, chip, xg.at[g], k * cap)

    @scoped
    def x_wait(g, ks):
        for k in ks:
            arrived(xg.at[g, :, group_rows(k)], x_r.at[g, k])

    def e_half(d):
        return pl.ds(d * local_count, local_count)

    def col_chunk(f):
        return slice(None) if f is None else pl.ds(f * width, width)

    @scoped
    def send_rows(g, f=None):
        at = col_chunk(f)
        i = f or 0
        for d in range(2):
            send(xg.at[g, e_half(d), group_rows(3), at], relay.at[g, d, :, :, at], f_s.at[g, d, 1, i],
                 rel_r.at[g, d, i], u_dev[d])
        for d in range(2):
            send(xg.at[g, :, group_rows(2 - d), at], raw.at[g, SIDE[d], :, :, at], f_s.at[g, d, 0, i],
                 raw_r.at[g, SIDE[d], 0, i], u_dev[d])

    @scoped
    def pass_rows(g, f=None):
        at = col_chunk(f)
        i = f or 0
        for d in range(2):
            arrived(relay.at[g, d, :, :, at], rel_r.at[g, d, i])
            send(relay.at[g, d, :, :, at], raw.at[g, 3, e_half(d), :, at], rel_s.at[g, d, i], raw_r.at[g, 3, d, i], u_dev[d])

    @scoped
    def raw_wait(g, f=None):
        at = col_chunk(f)
        i = f or 0
        for m in range(1, 3):
            arrived(raw.at[g, m, :, :, at], raw_r.at[g, m, 0, i])
        for d in range(2):
            arrived(raw.at[g, 3, e_half(d), :, at], raw_r.at[g, 3, d, i])

    @scoped
    def gates_of(g):
        for m in range(4):
            codes = row_codes(chip_at(u + OFFSETS[m], v))
            gate = jnp.zeros((block, tok_count), F32)
            for j in range(top_count):
                gate = gate + jnp.where(info[g, 0, j:j + 1, :] == codes, info[g, 0, 8 + j:9 + j, :], 0.0)
            gate = gate.T
            for s in range(3):
                part_s = gate.astype(BF16)
                gsplit[s * tok_count:(s + 1) * tok_count, m * block:(m + 1) * block] = part_s
                gate = gate - part_s.astype(F32)

    step = 256 if width % 256 == 0 else width

    @scoped
    def gated(g, f=None):
        first, count = (0, model_dim // step) if f is None else (f * (width // step), width // step)

        def cols(n, carry):
            at = pl.ds(pl.multiple_of(n * step, 128), step)
            rows = raw[g, :, :, :, at].reshape(4 * block, step)
            y = jnp.dot(gsplit[...], rows, preferred_element_type=F32)
            y = y[0:tok_count] + y[tok_count:2 * tok_count] + y[2 * tok_count:3 * tok_count]
            if g == 0:
                acc[:, at] = acc[:, at] + y
            else:
                part[g - 1, :, at] = y
            return carry

        lax.fori_loop(first, first + count, cols, 0)

    def send_early(g, d):
        send(part.at[g - 1, rows_of(1 - d)], fin.at[d], fin_s.at[d, chunks], fin_r.at[d, chunks], v_dev[d])

    def send_last(g, d, f):
        at = col_chunk(f)
        send(part.at[g - 1, rows_of(d), at], last.at[rows_of(d), at], fin_s.at[d, f], fin_r.at[d, f], v_dev[d])

    own_pick(0, range(4))
    for copy in own_loads:
        copy.wait()
    for i in range(local_count):
        for j, dst in enumerate((w_g, w_u, w_d)):
            arrived(dst.at[local_count + i], wr_r.at[i, j])
    experts(0)
    far_v(1)
    send_rows(0)
    far_v(2)
    far_v(3)
    pass_rows(0)
    own_pick(2, (1, 3))
    x_wait(2, (0, 2))
    experts(2)
    send_rows(2)
    own_pick(1, (0, 2))
    pass_rows(2)
    x_wait(1, (1, 3))
    experts(1)
    send_rows(1)
    raw_wait(0)
    gates_of(0)
    gated(0)
    x_wait(3, range(4))
    experts(3)
    pass_rows(1)
    for f in range(chunks):
        send_rows(3, f)
    raw_wait(2)
    inf_wait(2, 0)
    gates_of(2)
    gated(2)
    inf_wait(3, 0)
    raw_wait(1)
    gates_of(1)
    pass_rows(3, 0)
    gated(1)
    send_early(1, 1)
    send_early(2, 0)
    for f in range(1, chunks):
        pass_rows(3, f)
    gates_of(3)
    for f in range(chunks):
        raw_wait(3, f)
        gated(3, f)
        for d in range(2):
            send(part.at[2, rows_of(d), col_chunk(f)], half.at[d, :, col_chunk(f)], half_s.at[d, f], half_r.at[d, f], v_dev[d])
    for f in range(chunks):
        at = slice(f * width, (f + 1) * width)
        for d in range(2):
            g = 2 - d
            arrived(half.at[d, :, col_chunk(f)], half_r.at[d, f])
            rows = slice(d * piece, (d + 1) * piece)
            part[g - 1, rows, at] = part[g - 1, rows, at] + half[d, :, at]
            send_last(g, d, f)

    for d in range(2):
        arrived(fin.at[d], fin_r.at[d, chunks])
        rows = slice((1 - d) * piece, (2 - d) * piece)
        acc[rows] = acc[rows] + fin[d]
    for f in range(chunks):
        for d in range(2):
            arrived(last.at[rows_of(d), col_chunk(f)], fin_r.at[d, f])

    for copy in sent:
        copy.wait_send()


def solution(mesh):
    group_size = mesh.shape["ep"]
    side = math.isqrt(group_size // 2)

    def moe_step(tokens, expert_ids, gate_vals, w_gate, w_up, w_down, shared_gate, shared_up, shared_down):
        tok_count, model_dim = tokens.shape
        top_count = expert_ids.shape[1]
        local_count, _, ff = w_gate.shape
        expert_count = local_count * group_size
        spread = max(group_size, expert_count // 2)
        cap = (tok_count * top_count + spread - 1) // spread
        block = 2 * local_count * cap
        piece = tok_count // 2
        dma = pltpu.SemaphoreType.DMA
        hbm = pl.BlockSpec(memory_space=pl.ANY)
        scratch = [
            pltpu.VMEM((top_count, tok_count), jnp.int32),
            pltpu.VMEM((top_count, tok_count), F32),
            pltpu.VMEM((2 * local_count, model_dim, ff), BF16),
            pltpu.VMEM((2 * local_count, model_dim, ff), BF16),
            pltpu.VMEM((2 * local_count, ff, model_dim), BF16),
            pltpu.VMEM((len(WHOLE), tok_count, model_dim), BF16),
            pltpu.VMEM((4, 4, 16, tok_count), F32),
            pltpu.VMEM((4, 2 * local_count, 4 * cap, model_dim), BF16),
            pltpu.VMEM((5, 2 * local_count, cap, model_dim), BF16),
            pltpu.VMEM((4, 4, 2 * local_count, cap, model_dim), BF16),
            pltpu.VMEM((4, 2, local_count, cap, model_dim), BF16),
            pltpu.VMEM((3 * tok_count, 4 * block), BF16),
            pltpu.VMEM((3, tok_count, model_dim), F32),
            pltpu.VMEM((2, piece, model_dim), F32),
            pltpu.VMEM((2, piece, model_dim), F32),
            dma((3,)), dma((len(WHOLE), 2)), dma((2, 2)), dma((2,)), dma((4, 2)), dma((4, 4)), dma((4,)), dma((4,)),
            dma((4, 4)), dma((3,)), dma((4, 2)), dma(()),
            dma((4, 4, 2, 2)), dma((4, 2, 2)), dma((4, 2, 2, 2)), dma((4, 2, 2)),
            dma((2, 2)), dma((2, 2)), dma((2, 3)), dma((2, 3)),
            dma((local_count, 3)), dma((local_count, 3)), dma((local_count, 3)), dma((local_count, 3)),
        ]
        total = pltpu.VMEM(tokens.shape, F32)
        base, last = pl.pallas_call(
            functools.partial(kernel, side, cap),
            out_shape=(total, total),
            in_specs=[hbm] * 9,
            out_specs=(pl.BlockSpec(memory_space=pltpu.VMEM),) * 2,
            scratch_shapes=scratch,
            compiler_params=pltpu.CompilerParams(collective_id=0, has_side_effects=True, vmem_limit_bytes=63 * 1024 * 1024 - 3200 * 1024),
        )(expert_ids.T, gate_vals.T, tokens, w_gate, w_up, w_down, shared_gate, shared_up, shared_down)
        return (base + last).astype(tokens.dtype)

    row_spec = P(("dp", "ep"), None)
    expert_spec = P("ep", None, None)
    whole_spec = P(None, None)
    return jax.shard_map(moe_step, mesh=mesh, in_specs=(row_spec, row_spec, row_spec, expert_spec, expert_spec, expert_spec, whole_spec, whole_spec, whole_spec), out_specs=row_spec, check_vma=False)
```

```python
import functools
import math

import jax
import jax.numpy as jnp
from jax import lax
from jax.experimental import pallas as pl
from jax.experimental.pallas import tpu as pltpu
from jax.sharding import PartitionSpec as P

F32 = jnp.float32
BF16 = jnp.bfloat16
MESH = pl.DeviceIdType.MESH


def scoped(fn):
    @functools.wraps(fn)
    def run(*a):
        tag = "_".join(str(x) for x in a if isinstance(x, (int, tuple, list, range)))
        with jax.named_scope((fn.__name__ + "#a=" + tag).replace(" ", "").replace("(", "").replace(")", "").replace(",", "_")):
            return fn(*a)
    return run


OFFSETS = (0, -1, 1, 2)
SIDE = (1, 2)

WHOLE = {(0, 0): 0, (0, 1): 1, (0, 2): 2, (0, 3): 3, (1, 0): 4, (1, 2): 5, (2, 1): 6, (2, 3): 7}

TABLES = ((0, 1), (0, 2), (0, 3), (1, 0), (1, 2), (2, 0), (2, 1), (2, 3), (3, 0))


def kernel(side, cap, ids_hbm, gat_hbm, tok_hbm, wg_hbm, wu_hbm, wd_hbm, sg_hbm, su_hbm, sd_hbm, acc, last,
           ids_ref, gat_ref, w_g, w_u, w_d, tok, info, xg, stage, raw, relay, gsplit, part, half, fin,
           own_sem, load_sem, tok_r, inf_r, x_r, raw_r, rel_r, half_r, fin_r, wr_r,
           tok_s, near_s, far_s, inf_s, f_s, rel_s, half_s, fin_s, wr_s):
    tok_count, model_dim = tok_hbm.shape
    top_count = ids_hbm.shape[0]
    local_count, _, ff = wg_hbm.shape
    chip_experts = 2 * local_count
    expert_count = local_count * side * side * 2
    block = chip_experts * cap
    piece = tok_count // 2
    chunks = 2
    width = model_dim // chunks

    me = lax.axis_index("ep")
    c = me % 2
    chip = me // 2
    cx, cy = chip % side, chip // side
    u = (1 - c) * cx + c * cy
    v = (1 - c) * cy + c * cx

    def chip_at(uu, vv):
        uu, vv = (uu + side) % side, (vv + side) % side
        return (1 - c) * (vv * side + uu) + c * (uu * side + vv)

    def dev_at(uu, vv):
        return chip_at(uu, vv) * 2 + c

    u_dev = (dev_at(u + 1, v), dev_at(u - 1, v))
    v_dev = (dev_at(u, v + 1), dev_at(u, v - 1))
    v_chip = (chip_at(u, v + 1), chip_at(u, v - 1))
    partner = chip * 2 + (1 - c)

    def send(src, dst, ssem, rsem, dev):
        copy = pltpu.make_async_remote_copy(src_ref=src, dst_ref=dst, send_sem=ssem, recv_sem=rsem,
                                            device_id={"ep": dev}, device_id_type=MESH)
        copy.start()
        return copy

    def filled(dst, sem):
        pltpu.make_async_copy(dst, dst, sem).wait()

    def rows_of(p):
        return pl.ds(p * piece, piece)

    routes = [pltpu.make_async_copy(src, dst, own_sem.at[i + 1])
              for i, (src, dst) in enumerate(((ids_hbm, ids_ref), (gat_hbm, gat_ref)))]
    for copy in routes:
        copy.start()
    own = pltpu.make_async_copy(tok_hbm, tok.at[0], own_sem.at[0])
    own.start()
    barrier = pltpu.get_barrier_semaphore()
    for dev in u_dev + v_dev + (partner,):
        pl.semaphore_signal(barrier, inc=1, device_id={"ep": dev}, device_id_type=MESH)
    for copy in routes:
        copy.wait()
    expert = lax.broadcasted_iota(jnp.int32, (expert_count, tok_count), 0)
    hots = []
    chosen = jnp.zeros((expert_count, tok_count), F32)
    for j in range(top_count):
        hot = (ids_ref[j:j + 1, :] == expert).astype(F32)
        hots.append(hot)
        chosen = chosen + hot
    above = (lax.broadcasted_iota(jnp.int32, (tok_count, tok_count), 0)
             < lax.broadcasted_iota(jnp.int32, (tok_count, tok_count), 1)).astype(F32).astype(BF16)
    slot = jnp.dot(chosen.astype(BF16), above, preferred_element_type=F32)
    info[0] = jnp.zeros((16, tok_count), F32)
    for j in range(top_count):
        info[0, j:j + 1, :] = ids_ref[j:j + 1, :].astype(F32) * cap + jnp.sum(hots[j] * slot, axis=0, keepdims=True)
        info[0, 8 + j:9 + j, :] = gat_ref[j:j + 1, :]

    @scoped
    def tok_wait(g, k, p):
        filled(tok.at[k, rows_of(p)], tok_r.at[2 * k + p - 2])

    @scoped
    def block_wait(g, k):
        filled(tok.at[WHOLE[g, k]], tok_r.at[WHOLE[g, k] + 2])

    def send_u_own():
        for order in range(2):
            for d in range(2):
                p = (d + order) % 2
                send(tok.at[0, rows_of(p)], tok.at[SIDE[d], rows_of(p)], tok_s, tok_r.at[2 * SIDE[d] + p - 2], u_dev[d])

    @scoped
    def forward_u(d):
        tok_wait(0, SIDE[d], d)
        send(tok.at[SIDE[d], rows_of(d)], tok.at[3, rows_of(d)], tok_s, tok_r.at[4 + d], u_dev[d])

    def whole_v(k, p):
        d = k % 2
        at = WHOLE[SIDE[d], k]
        send(tok.at[k, rows_of(p)], tok.at[at, rows_of(p)], tok_s, tok_r.at[at + 2], v_dev[d])

    slot_rows = lax.broadcasted_iota(jnp.int32, (block, tok_count), 0) + c * (local_count * cap)
    turned = jnp.where(slot_rows >= block, slot_rows - block, slot_rows)
    n_step = 512 if model_dim % 512 == 0 else model_dim

    def row_codes(chip_idx):
        return (turned + chip_idx * block).astype(F32)

    def pick(g, k, chip_idx, dst, first):
        codes = row_codes(chip_idx)
        hit = jnp.zeros((block, tok_count), F32)
        for j in range(top_count):
            hit = hit + (info[4 * g + k, j:j + 1, :] == codes).astype(F32)
        hit = hit.astype(BF16)
        for n in range(0, model_dim, n_step):
            x = jnp.dot(hit, tok[WHOLE[g, k], :, n:n + n_step], preferred_element_type=F32).astype(BF16)
            for e in range(chip_experts):
                dst[e, first:first + cap, n:n + n_step] = x[e * cap:(e + 1) * cap]

    def group_rows(k):
        return pl.ds(k * cap, cap)

    near = [None] * 4

    @scoped
    def near_v(k):
        d = 1 - k % 2
        pick(0, k, v_chip[d], stage.at[k], 0)
        near[k] = send(stage.at[k], xg.at[SIDE[d], :, group_rows(k)], near_s.at[k] if k < 3 else far_s, x_r.at[SIDE[d] - 1], v_dev[d])

    codes_only = pl.ds(0, 8)

    def inf_rows(k):
        return pl.ds(0, 16) if k == 0 else codes_only

    @scoped
    def inf_wait(g, k):
        filled(info.at[4 * g + k, inf_rows(k)], inf_r.at[TABLES.index((g, k))])

    @scoped
    def far_v(k):
        d = k % 2
        g = SIDE[d]
        block_wait(g, k)
        inf_wait(g, k)
        at = k if k < 3 else 4
        if k < 3:
            near[k].wait_send()
        pick(g, k, v_chip[d], stage.at[at], 0)
        send(stage.at[at], xg.at[3, :, group_rows(k)], far_s, x_r.at[2], v_dev[d])
        if k == 0:
            send(info.at[4 * g], info.at[12], inf_s, inf_r.at[TABLES.index((3, 0))], v_dev[d])

    def info_v(k):
        for d in range(2):
            if k == 0 or d == k % 2:
                send(info.at[k, inf_rows(k)], info.at[4 * SIDE[d] + k, inf_rows(k)], inf_s,
                     inf_r.at[TABLES.index((SIDE[d], k))], v_dev[d])

    with jax.named_scope('ownwait'):
        own.wait()
    with jax.named_scope('barrier'):
        pl.semaphore_wait(barrier, 5)
    for d in range(2):
        send(info.at[0, codes_only], info.at[SIDE[d], codes_only], inf_s, inf_r.at[TABLES.index((0, SIDE[d]))], u_dev[d])
    info_v(0)
    send_u_own()
    whole_v(0, 0)
    whole_v(0, 1)

    shared_loads = []
    for i in range(local_count):
        cols = pl.ds(i * ff, ff)
        for j, (src, dst) in enumerate(((sg_hbm.at[:, cols], w_g), (su_hbm.at[:, cols], w_u), (sd_hbm.at[cols], w_d))):
            copy = pltpu.make_async_copy(src, dst.at[i], load_sem.at[i, j])
            copy.start()
            shared_loads.append(copy)

    near_v(0)

    for i in range(local_count):
        for j, (src, dst) in enumerate(((wg_hbm, w_g), (wu_hbm, w_u), (wd_hbm, w_d))):
            send(src.at[i], dst.at[local_count + i], wr_s.at[j], wr_r.at[j], partner)

    def silu_mul(g, up):
        return (jax.nn.silu(g) * up).astype(BF16)

    @scoped
    def shared_part(i):
        for copy in shared_loads[3 * i:3 * i + 3]:
            copy.wait()
        x = tok[0]
        h = silu_mul(jnp.dot(x, w_g[i], preferred_element_type=F32), jnp.dot(x, w_u[i], preferred_element_type=F32))
        for n in range(0, model_dim, n_step):
            y = jnp.dot(h, w_d[i, :, n:n + n_step], preferred_element_type=F32)
            if i > 0:
                y = y + acc[:, n:n + n_step]
            if i == local_count - 1:
                y = y.astype(BF16).astype(F32) + x[:, n:n + n_step].astype(F32)
            acc[:, n:n + n_step] = y

    own_loads = []

    def load_own(i):
        for j, (src, dst) in enumerate(((wg_hbm, w_g), (wu_hbm, w_u), (wd_hbm, w_d))):
            copy = pltpu.make_async_copy(src.at[i], dst.at[i], load_sem.at[i, j])
            copy.start()
            own_loads.append(copy)

    for i in range(local_count):
        shared_part(i)
        load_own(i)

    inf_wait(0, 1)
    send(info.at[1, codes_only], info.at[3, codes_only], inf_s, inf_r.at[TABLES.index((0, 3))], u_dev[0])
    info_v(1)
    inf_wait(0, 2)
    info_v(2)
    forward_u(0)
    forward_u(1)
    whole_v(1, 0)
    whole_v(2, 1)
    tok_wait(0, 1, 1)
    whole_v(1, 1)
    tok_wait(0, 2, 0)
    whole_v(2, 0)
    near_v(1)
    near_v(2)
    far_v(0)
    for p in range(2):
        tok_wait(0, 3, p)
        whole_v(3, p)
    inf_wait(0, 3)
    info_v(3)
    near_v(3)

    @scoped
    def experts(g):
        def one(e, carry):
            x = xg[g, e]
            h = silu_mul(jnp.dot(x, w_g[e], preferred_element_type=F32), jnp.dot(x, w_u[e], preferred_element_type=F32))
            for n in range(0, model_dim, n_step):
                y = jnp.dot(h, w_d[e, :, n:n + n_step], preferred_element_type=F32).astype(BF16)
                raw[g, 0, e, :, n:n + n_step] = y[0:cap]
                xg[g, e, cap:4 * cap, n:n + n_step] = y[cap:4 * cap]
            return carry

        lax.fori_loop(0, chip_experts, one, 0)

    @scoped
    def own_pick(g, ks):
        for k in ks:
            pick(g, k, chip, xg.at[g], k * cap)

    @scoped
    def x_wait(g, ks):
        filled(xg.at[g, pl.ds(0, len(ks) * chip_experts // 4)], x_r.at[g - 1])

    def e_half(d):
        return pl.ds(d * local_count, local_count)

    def col_chunk(f):
        return slice(None) if f is None else pl.ds(f * width, width)

    @scoped
    def send_rows(g, f=None):
        at = col_chunk(f)
        i = f or 0
        for d in range(2):
            send(xg.at[g, e_half(d), group_rows(3), at], relay.at[g, d, :, :, at], f_s, rel_r.at[g + i], u_dev[d])
        for d in range(2):
            send(xg.at[g, :, group_rows(2 - d), at], raw.at[g, SIDE[d], :, :, at], f_s, raw_r.at[g + i], u_dev[d])

    @scoped
    def pass_rows(g, f=None):
        at = col_chunk(f)
        i = f or 0
        filled(relay.at[g, :, :, :, at], rel_r.at[g + i])
        for d in range(2):
            send(relay.at[g, d, :, :, at], raw.at[g, 3, e_half(d), :, at], rel_s, raw_r.at[g + i], u_dev[d])

    @scoped
    def raw_wait(g, f=None):
        at = col_chunk(f)
        i = f or 0
        filled(raw.at[g, pl.ds(1, 3), :, :, at], raw_r.at[g + i])

    @scoped
    def gates_of(g):
        for m in range(4):
            codes = row_codes(chip_at(u + OFFSETS[m], v))
            gate = jnp.zeros((block, tok_count), F32)
            for j in range(top_count):
                gate = gate + jnp.where(info[4 * g, j:j + 1, :] == codes, info[4 * g, 8 + j:9 + j, :], 0.0)
            gate = gate.T
            for s in range(3):
                part_s = gate.astype(BF16)
                gsplit[s * tok_count:(s + 1) * tok_count, m * block:(m + 1) * block] = part_s
                gate = gate - part_s.astype(F32)

    step = 256 if width % 256 == 0 else width

    @scoped
    def gated(g, f=None):
        first, count = (0, model_dim // step) if f is None else (f * (width // step), width // step)

        def cols(n, carry):
            at = pl.ds(pl.multiple_of(n * step, 128), step)
            rows = raw[g, :, :, :, at].reshape(4 * block, step)
            y = jnp.dot(gsplit[...], rows, preferred_element_type=F32)
            y = y[0:tok_count] + y[tok_count:2 * tok_count] + y[2 * tok_count:3 * tok_count]
            if g == 0:
                acc[:, at] = acc[:, at] + y
            else:
                part[g - 1, :, at] = y
            return carry

        lax.fori_loop(first, first + count, cols, 0)

    def send_early(g, d):
        send(part.at[g - 1, rows_of(1 - d)], fin.at[d], fin_s, fin_r.at[0], v_dev[d])

    def send_last(g, d, f):
        at = col_chunk(f)
        send(part.at[g - 1, rows_of(d), at], last.at[rows_of(d), at], fin_s, fin_r.at[1], v_dev[d])

    own_pick(0, range(4))
    for copy in own_loads:
        copy.wait()
    for j, dst in enumerate((w_g, w_u, w_d)):
        filled(dst.at[pl.ds(local_count, local_count)], wr_r.at[j])
    experts(0)
    far_v(1)
    send_rows(0)
    far_v(2)
    far_v(3)
    pass_rows(0)
    own_pick(2, (1, 3))
    x_wait(2, (0, 2))
    experts(2)
    send_rows(2)
    own_pick(1, (0, 2))
    pass_rows(2)
    x_wait(1, (1, 3))
    experts(1)
    send_rows(1)
    raw_wait(0)
    gates_of(0)
    gated(0)
    x_wait(3, range(4))
    experts(3)
    pass_rows(1)
    for f in range(chunks):
        send_rows(3, f)
    raw_wait(2)
    inf_wait(2, 0)
    gates_of(2)
    gated(2)
    inf_wait(3, 0)
    raw_wait(1)
    gates_of(1)
    pass_rows(3, 0)
    gated(1)
    send_early(1, 1)
    send_early(2, 0)
    for f in range(1, chunks):
        pass_rows(3, f)
    gates_of(3)
    for f in range(chunks):
        raw_wait(3, f)
        gated(3, f)
        for d in range(2):
            send(part.at[2, rows_of(d), col_chunk(f)], half.at[d, :, col_chunk(f)], half_s, half_r.at[f], v_dev[d])
    for f in range(chunks):
        at = slice(f * width, (f + 1) * width)
        filled(half.at[:, :, col_chunk(f)], half_r.at[f])
        for d in range(2):
            g = 2 - d
            rows = slice(d * piece, (d + 1) * piece)
            part[g - 1, rows, at] = part[g - 1, rows, at] + half[d, :, at]
            send_last(g, d, f)

    filled(fin, fin_r.at[0])
    for d in range(2):
        rows = slice((1 - d) * piece, (2 - d) * piece)
        acc[rows] = acc[rows] + fin[d]

    filled(tok.at[pl.ds(0, 7)], tok_s)
    filled(stage, far_s)
    filled(info.at[pl.ds(0, 6)], inf_s)
    for j, dst in enumerate((w_g, w_u, w_d)):
        filled(dst.at[pl.ds(0, local_count)], wr_s.at[j])
    filled(raw.at[pl.ds(0, 3)], f_s)
    filled(relay, rel_s)
    filled(half, half_s)
    filled(part.at[pl.ds(0, 2)], fin_s)
    filled(last, fin_r.at[1])


def solution(mesh):
    group_size = mesh.shape["ep"]
    side = math.isqrt(group_size // 2)

    def moe_step(tokens, expert_ids, gate_vals, w_gate, w_up, w_down, shared_gate, shared_up, shared_down):
        tok_count, model_dim = tokens.shape
        top_count = expert_ids.shape[1]
        local_count, _, ff = w_gate.shape
        expert_count = local_count * group_size
        spread = max(group_size, expert_count // 2)
        cap = (tok_count * top_count + spread - 1) // spread
        block = 2 * local_count * cap
        piece = tok_count // 2
        dma = pltpu.SemaphoreType.DMA
        hbm = pl.BlockSpec(memory_space=pl.ANY)
        scratch = [
            pltpu.VMEM((top_count, tok_count), jnp.int32),
            pltpu.VMEM((top_count, tok_count), F32),
            pltpu.VMEM((2 * local_count, model_dim, ff), BF16),
            pltpu.VMEM((2 * local_count, model_dim, ff), BF16),
            pltpu.VMEM((2 * local_count, ff, model_dim), BF16),
            pltpu.VMEM((len(WHOLE), tok_count, model_dim), BF16),
            pltpu.VMEM((16, 16, tok_count), F32),
            pltpu.VMEM((4, 2 * local_count, 4 * cap, model_dim), BF16),
            pltpu.VMEM((5, 2 * local_count, cap, model_dim), BF16),
            pltpu.VMEM((4, 4, 2 * local_count, cap, model_dim), BF16),
            pltpu.VMEM((4, 2, local_count, cap, model_dim), BF16),
            pltpu.VMEM((3 * tok_count, 4 * block), BF16),
            pltpu.VMEM((3, tok_count, model_dim), F32),
            pltpu.VMEM((2, piece, model_dim), F32),
            pltpu.VMEM((2, piece, model_dim), F32),
            dma((3,)), dma((local_count, 3)), dma((len(WHOLE) + 2,)), dma((len(TABLES),)), dma((3,)), dma((5,)), dma((5,)),
            dma((2,)), dma((2,)), dma((3,)),
            dma(()), dma((3,)), dma(()), dma(()), dma(()), dma(()), dma(()), dma(()), dma((3,)),
        ]
        total = pltpu.VMEM(tokens.shape, F32)
        base, last = pl.pallas_call(
            functools.partial(kernel, side, cap),
            out_shape=(total, total),
            in_specs=[hbm] * 9,
            out_specs=(pl.BlockSpec(memory_space=pltpu.VMEM),) * 2,
            scratch_shapes=scratch,
            compiler_params=pltpu.CompilerParams(collective_id=0, has_side_effects=True, vmem_limit_bytes=63 * 1024 * 1024 - 3200 * 1024),
        )(expert_ids.T, gate_vals.T, tokens, w_gate, w_up, w_down, shared_gate, shared_up, shared_down)
        return (base + last).astype(tokens.dtype)

    row_spec = P(("dp", "ep"), None)
    expert_spec = P("ep", None, None)
    whole_spec = P(None, None)
    return jax.shard_map(moe_step, mesh=mesh, in_specs=(row_spec, row_spec, row_spec, expert_spec, expert_spec, expert_spec, whole_spec, whole_spec, whole_spec), out_specs=row_spec, check_vma=False)
```

```python
import functools
import math

import jax
import jax.numpy as jnp
from jax import lax
from jax.experimental import pallas as pl
from jax.experimental.pallas import tpu as pltpu
from jax.sharding import PartitionSpec as P

F32 = jnp.float32
BF16 = jnp.bfloat16
MESH = pl.DeviceIdType.MESH


def scoped(fn):
    @functools.wraps(fn)
    def run(*a):
        tag = "_".join(str(x) for x in a if isinstance(x, (int, tuple, list, range)))
        with jax.named_scope((fn.__name__ + "#a=" + tag).replace(" ", "").replace("(", "").replace(")", "").replace(",", "_")):
            return fn(*a)
    return run


OFFSETS = (0, -1, 1, 2)
SIDE = (1, 2)

WHOLE = {(0, 0): 0, (0, 1): 1, (0, 2): 2, (0, 3): 3, (1, 0): 4, (1, 2): 5, (2, 1): 6, (2, 3): 7}

TABLES = ((0, 1), (0, 2), (0, 3), (1, 0), (1, 2), (2, 0), (2, 1), (2, 3), (3, 0))


def kernel(side, cap, ids_hbm, gat_hbm, tok_hbm, wg_hbm, wu_hbm, wd_hbm, sg_hbm, su_hbm, sd_hbm, acc, last,
           ids_ref, gat_ref, w_g, w_u, w_d, tok, info, xg, stage, raw, relay, gsplit, part, half, fin,
           own_sem, load_sem, tok_r, inf_r, x_r, raw_r, rel_r, half_r, fin_r, wr_r,
           tok_s, near_s, far_s, inf_s, f_s, rel_s, half_s, fin_s, wr_s):
    tok_count, model_dim = tok_hbm.shape
    top_count = ids_hbm.shape[0]
    local_count, _, ff = wg_hbm.shape
    chip_experts = 2 * local_count
    expert_count = local_count * side * side * 2
    block = chip_experts * cap
    piece = tok_count // 2
    chunks = 2
    width = model_dim // chunks

    me = lax.axis_index("ep")
    c = me % 2
    chip = me // 2
    cx, cy = chip % side, chip // side
    u = (1 - c) * cx + c * cy
    v = (1 - c) * cy + c * cx

    def chip_at(uu, vv):
        uu, vv = (uu + side) % side, (vv + side) % side
        return (1 - c) * (vv * side + uu) + c * (uu * side + vv)

    def dev_at(uu, vv):
        return chip_at(uu, vv) * 2 + c

    u_dev = (dev_at(u + 1, v), dev_at(u - 1, v))
    v_dev = (dev_at(u, v + 1), dev_at(u, v - 1))
    v_chip = (chip_at(u, v + 1), chip_at(u, v - 1))
    partner = chip * 2 + (1 - c)

    def send(src, dst, ssem, rsem, dev):
        copy = pltpu.make_async_remote_copy(src_ref=src, dst_ref=dst, send_sem=ssem, recv_sem=rsem,
                                            device_id={"ep": dev}, device_id_type=MESH)
        copy.start()
        return copy

    def filled(dst, sem):
        pltpu.make_async_copy(dst, dst, sem).wait()

    def rows_of(p):
        return pl.ds(p * piece, piece)

    barrier = pltpu.get_barrier_semaphore()
    for dev in u_dev + v_dev + (partner,):
        pl.semaphore_signal(barrier, inc=1, device_id={"ep": dev}, device_id_type=MESH)

    routes = [pltpu.make_async_copy(src, dst, own_sem.at[i + 1])
              for i, (src, dst) in enumerate(((ids_hbm, ids_ref), (gat_hbm, gat_ref)))]
    for copy in routes:
        copy.start()
    own = pltpu.make_async_copy(tok_hbm, tok.at[0], own_sem.at[0])
    own.start()
    @scoped
    def tok_wait(g, k, p):
        filled(tok.at[k, rows_of(p)], tok_r.at[2 * k + p - 2])

    @scoped
    def block_wait(g, k):
        filled(tok.at[WHOLE[g, k]], tok_r.at[WHOLE[g, k] + 2])

    def send_u_own(order):
        for d in range(2):
            p = (d + order) % 2
            send(tok.at[0, rows_of(p)], tok.at[SIDE[d], rows_of(p)], tok_s, tok_r.at[2 * SIDE[d] + p - 2], u_dev[d])

    @scoped
    def forward_u(d):
        tok_wait(0, SIDE[d], d)
        send(tok.at[SIDE[d], rows_of(d)], tok.at[3, rows_of(d)], tok_s, tok_r.at[4 + d], u_dev[d])

    def whole_v(k, p):
        d = k % 2
        at = WHOLE[SIDE[d], k]
        send(tok.at[k, rows_of(p)], tok.at[at, rows_of(p)], tok_s, tok_r.at[at + 2], v_dev[d])

    slot_rows = lax.broadcasted_iota(jnp.int32, (block, tok_count), 0) + c * (local_count * cap)
    turned = jnp.where(slot_rows >= block, slot_rows - block, slot_rows)
    n_step = 512 if model_dim % 512 == 0 else model_dim

    def row_codes(chip_idx):
        return (turned + chip_idx * block).astype(F32)

    def pick(g, k, chip_idx, dst, first):
        codes = row_codes(chip_idx)
        hit = jnp.zeros((block, tok_count), F32)
        for j in range(top_count):
            hit = hit + (info[4 * g + k, j:j + 1, :] == codes).astype(F32)
        hit = hit.astype(BF16)
        for n in range(0, model_dim, n_step):
            x = jnp.dot(hit, tok[WHOLE[g, k], :, n:n + n_step], preferred_element_type=F32).astype(BF16)
            for e in range(chip_experts):
                dst[e, first:first + cap, n:n + n_step] = x[e * cap:(e + 1) * cap]

    def group_rows(k):
        return pl.ds(k * cap, cap)

    near = [None] * 4

    @scoped
    def near_v(k):
        d = 1 - k % 2
        pick(0, k, v_chip[d], stage.at[k], 0)
        near[k] = send(stage.at[k], xg.at[SIDE[d], :, group_rows(k)], near_s.at[k] if k < 3 else far_s, x_r.at[SIDE[d] - 1], v_dev[d])

    codes_only = pl.ds(0, 8)

    def inf_rows(k):
        return pl.ds(0, 16) if k == 0 else codes_only

    @scoped
    def inf_wait(g, k):
        filled(info.at[4 * g + k, inf_rows(k)], inf_r.at[TABLES.index((g, k))])

    @scoped
    def far_v(k):
        d = k % 2
        g = SIDE[d]
        block_wait(g, k)
        inf_wait(g, k)
        at = k if k < 3 else 4
        if k < 3:
            near[k].wait_send()
        pick(g, k, v_chip[d], stage.at[at], 0)
        send(stage.at[at], xg.at[3, :, group_rows(k)], far_s, x_r.at[2], v_dev[d])
        if k == 0:
            send(info.at[4 * g], info.at[12], inf_s, inf_r.at[TABLES.index((3, 0))], v_dev[d])

    def info_v(k):
        for d in range(2):
            if k == 0 or d == k % 2:
                send(info.at[k, inf_rows(k)], info.at[4 * SIDE[d] + k, inf_rows(k)], inf_s,
                     inf_r.at[TABLES.index((SIDE[d], k))], v_dev[d])

    with jax.named_scope('ownwait'):
        own.wait()
    with jax.named_scope('barrier'):
        pl.semaphore_wait(barrier, 5)
    send_u_own(0)
    whole_v(0, 0)

    for copy in routes:
        copy.wait()
    expert = lax.broadcasted_iota(jnp.int32, (expert_count, tok_count), 0)
    hots = []
    chosen = jnp.zeros((expert_count, tok_count), F32)
    for j in range(top_count):
        hot = (ids_ref[j:j + 1, :] == expert).astype(F32)
        hots.append(hot)
        chosen = chosen + hot
    above = (lax.broadcasted_iota(jnp.int32, (tok_count, tok_count), 0)
             < lax.broadcasted_iota(jnp.int32, (tok_count, tok_count), 1)).astype(F32).astype(BF16)
    slot = jnp.dot(chosen.astype(BF16), above, preferred_element_type=F32)
    info[0] = jnp.zeros((16, tok_count), F32)
    for j in range(top_count):
        info[0, j:j + 1, :] = ids_ref[j:j + 1, :].astype(F32) * cap + jnp.sum(hots[j] * slot, axis=0, keepdims=True)
        info[0, 8 + j:9 + j, :] = gat_ref[j:j + 1, :]

    for d in range(2):
        send(info.at[0, codes_only], info.at[SIDE[d], codes_only], inf_s, inf_r.at[TABLES.index((0, SIDE[d]))], u_dev[d])
    info_v(0)
    send_u_own(1)
    whole_v(0, 1)

    shared_loads = []
    for i in range(local_count):
        cols = pl.ds(i * ff, ff)
        for j, (src, dst) in enumerate(((sg_hbm.at[:, cols], w_g), (su_hbm.at[:, cols], w_u), (sd_hbm.at[cols], w_d))):
            copy = pltpu.make_async_copy(src, dst.at[i], load_sem.at[i, j])
            copy.start()
            shared_loads.append(copy)

    near_v(0)

    for i in range(local_count):
        for j, (src, dst) in enumerate(((wg_hbm, w_g), (wu_hbm, w_u), (wd_hbm, w_d))):
            send(src.at[i], dst.at[local_count + i], wr_s.at[j], wr_r.at[j], partner)

    def silu_mul(g, up):
        return (jax.nn.silu(g) * up).astype(BF16)

    @scoped
    def shared_part(i):
        for copy in shared_loads[3 * i:3 * i + 3]:
            copy.wait()
        x = tok[0]
        h = silu_mul(jnp.dot(x, w_g[i], preferred_element_type=F32), jnp.dot(x, w_u[i], preferred_element_type=F32))
        for n in range(0, model_dim, n_step):
            y = jnp.dot(h, w_d[i, :, n:n + n_step], preferred_element_type=F32)
            if i > 0:
                y = y + acc[:, n:n + n_step]
            if i == local_count - 1:
                y = y.astype(BF16).astype(F32) + x[:, n:n + n_step].astype(F32)
            acc[:, n:n + n_step] = y

    own_loads = []

    def load_own(i):
        for j, (src, dst) in enumerate(((wg_hbm, w_g), (wu_hbm, w_u), (wd_hbm, w_d))):
            copy = pltpu.make_async_copy(src.at[i], dst.at[i], load_sem.at[i, j])
            copy.start()
            own_loads.append(copy)

    for i in range(local_count):
        shared_part(i)
        load_own(i)

    inf_wait(0, 1)
    send(info.at[1, codes_only], info.at[3, codes_only], inf_s, inf_r.at[TABLES.index((0, 3))], u_dev[0])
    info_v(1)
    inf_wait(0, 2)
    info_v(2)
    forward_u(0)
    forward_u(1)
    whole_v(1, 0)
    whole_v(2, 1)
    tok_wait(0, 1, 1)
    whole_v(1, 1)
    tok_wait(0, 2, 0)
    whole_v(2, 0)
    near_v(1)
    near_v(2)
    far_v(0)
    for p in range(2):
        tok_wait(0, 3, p)
        whole_v(3, p)
    inf_wait(0, 3)
    info_v(3)
    near_v(3)

    @scoped
    def experts(g):
        def one(e, carry):
            x = xg[g, e]
            h = silu_mul(jnp.dot(x, w_g[e], preferred_element_type=F32), jnp.dot(x, w_u[e], preferred_element_type=F32))
            for n in range(0, model_dim, n_step):
                y = jnp.dot(h, w_d[e, :, n:n + n_step], preferred_element_type=F32).astype(BF16)
                raw[g, 0, e, :, n:n + n_step] = y[0:cap]
                xg[g, e, cap:4 * cap, n:n + n_step] = y[cap:4 * cap]
            return carry

        lax.fori_loop(0, chip_experts, one, 0)

    @scoped
    def own_pick(g, ks):
        for k in ks:
            pick(g, k, chip, xg.at[g], k * cap)

    @scoped
    def x_wait(g, ks):
        filled(xg.at[g, pl.ds(0, len(ks) * chip_experts // 4)], x_r.at[g - 1])

    def e_half(d):
        return pl.ds(d * local_count, local_count)

    def col_chunk(f):
        return slice(None) if f is None else pl.ds(f * width, width)

    @scoped
    def send_rows(g, f=None):
        at = col_chunk(f)
        i = f or 0
        for d in range(2):
            send(xg.at[g, e_half(d), group_rows(3), at], relay.at[g, d, :, :, at], f_s, rel_r.at[g + i], u_dev[d])
        for d in range(2):
            send(xg.at[g, :, group_rows(2 - d), at], raw.at[g, SIDE[d], :, :, at], f_s, raw_r.at[g + i], u_dev[d])

    @scoped
    def pass_rows(g, f=None):
        at = col_chunk(f)
        i = f or 0
        filled(relay.at[g, :, :, :, at], rel_r.at[g + i])
        for d in range(2):
            send(relay.at[g, d, :, :, at], raw.at[g, 3, e_half(d), :, at], rel_s, raw_r.at[g + i], u_dev[d])

    @scoped
    def raw_wait(g, f=None):
        at = col_chunk(f)
        i = f or 0
        filled(raw.at[g, pl.ds(1, 3), :, :, at], raw_r.at[g + i])

    @scoped
    def gates_of(g):
        for m in range(4):
            codes = row_codes(chip_at(u + OFFSETS[m], v))
            gate = jnp.zeros((block, tok_count), F32)
            for j in range(top_count):
                gate = gate + jnp.where(info[4 * g, j:j + 1, :] == codes, info[4 * g, 8 + j:9 + j, :], 0.0)
            gate = gate.T
            for s in range(3):
                part_s = gate.astype(BF16)
                gsplit[s * tok_count:(s + 1) * tok_count, m * block:(m + 1) * block] = part_s
                gate = gate - part_s.astype(F32)

    step = 256 if width % 256 == 0 else width

    @scoped
    def gated(g, f=None):
        first, count = (0, model_dim // step) if f is None else (f * (width // step), width // step)

        def cols(n, carry):
            at = pl.ds(pl.multiple_of(n * step, 128), step)
            rows = raw[g, :, :, :, at].reshape(4 * block, step)
            y = jnp.dot(gsplit[...], rows, preferred_element_type=F32)
            y = y[0:tok_count] + y[tok_count:2 * tok_count] + y[2 * tok_count:3 * tok_count]
            if g == 0:
                acc[:, at] = acc[:, at] + y
            else:
                part[g - 1, :, at] = y
            return carry

        lax.fori_loop(first, first + count, cols, 0)

    def send_early(g, d):
        send(part.at[g - 1, rows_of(1 - d)], fin.at[d], fin_s, fin_r.at[0], v_dev[d])

    def send_last(g, d, f):
        at = col_chunk(f)
        send(part.at[g - 1, rows_of(d), at], last.at[rows_of(d), at], fin_s, fin_r.at[1], v_dev[d])

    own_pick(0, range(4))
    for copy in own_loads:
        copy.wait()
    for j, dst in enumerate((w_g, w_u, w_d)):
        filled(dst.at[pl.ds(local_count, local_count)], wr_r.at[j])
    experts(0)
    far_v(1)
    send_rows(0)
    far_v(2)
    far_v(3)
    pass_rows(0)
    own_pick(2, (1, 3))
    x_wait(2, (0, 2))
    experts(2)
    send_rows(2)
    own_pick(1, (0, 2))
    pass_rows(2)
    x_wait(1, (1, 3))
    experts(1)
    send_rows(1)
    raw_wait(0)
    gates_of(0)
    gated(0)
    x_wait(3, range(4))
    experts(3)
    pass_rows(1)
    for f in range(chunks):
        send_rows(3, f)
    raw_wait(2)
    inf_wait(2, 0)
    gates_of(2)
    gated(2)
    inf_wait(3, 0)
    raw_wait(1)
    gates_of(1)
    pass_rows(3, 0)
    gated(1)
    send_early(1, 1)
    send_early(2, 0)
    for f in range(1, chunks):
        pass_rows(3, f)
    gates_of(3)
    for f in range(chunks):
        raw_wait(3, f)
        gated(3, f)
        for d in range(2):
            send(part.at[2, rows_of(d), col_chunk(f)], half.at[d, :, col_chunk(f)], half_s, half_r.at[f], v_dev[d])
    for f in range(chunks):
        at = slice(f * width, (f + 1) * width)
        filled(half.at[:, :, col_chunk(f)], half_r.at[f])
        for d in range(2):
            g = 2 - d
            rows = slice(d * piece, (d + 1) * piece)
            part[g - 1, rows, at] = part[g - 1, rows, at] + half[d, :, at]
            send_last(g, d, f)

    filled(fin, fin_r.at[0])
    for d in range(2):
        rows = slice((1 - d) * piece, (2 - d) * piece)
        acc[rows] = acc[rows] + fin[d]

    filled(tok.at[pl.ds(0, 7)], tok_s)
    filled(stage, far_s)
    filled(info.at[pl.ds(0, 6)], inf_s)
    for j, dst in enumerate((w_g, w_u, w_d)):
        filled(dst.at[pl.ds(0, local_count)], wr_s.at[j])
    filled(raw.at[pl.ds(0, 3)], f_s)
    filled(relay, rel_s)
    filled(half, half_s)
    filled(part.at[pl.ds(0, 2)], fin_s)
    filled(last, fin_r.at[1])


def solution(mesh):
    group_size = mesh.shape["ep"]
    side = math.isqrt(group_size // 2)

    def moe_step(tokens, expert_ids, gate_vals, w_gate, w_up, w_down, shared_gate, shared_up, shared_down):
        tok_count, model_dim = tokens.shape
        top_count = expert_ids.shape[1]
        local_count, _, ff = w_gate.shape
        expert_count = local_count * group_size
        spread = max(group_size, expert_count // 2)
        cap = (tok_count * top_count + spread - 1) // spread
        block = 2 * local_count * cap
        piece = tok_count // 2
        dma = pltpu.SemaphoreType.DMA
        hbm = pl.BlockSpec(memory_space=pl.ANY)
        scratch = [
            pltpu.VMEM((top_count, tok_count), jnp.int32),
            pltpu.VMEM((top_count, tok_count), F32),
            pltpu.VMEM((2 * local_count, model_dim, ff), BF16),
            pltpu.VMEM((2 * local_count, model_dim, ff), BF16),
            pltpu.VMEM((2 * local_count, ff, model_dim), BF16),
            pltpu.VMEM((len(WHOLE), tok_count, model_dim), BF16),
            pltpu.VMEM((16, 16, tok_count), F32),
            pltpu.VMEM((4, 2 * local_count, 4 * cap, model_dim), BF16),
            pltpu.VMEM((5, 2 * local_count, cap, model_dim), BF16),
            pltpu.VMEM((4, 4, 2 * local_count, cap, model_dim), BF16),
            pltpu.VMEM((4, 2, local_count, cap, model_dim), BF16),
            pltpu.VMEM((3 * tok_count, 4 * block), BF16),
            pltpu.VMEM((3, tok_count, model_dim), F32),
            pltpu.VMEM((2, piece, model_dim), F32),
            pltpu.VMEM((2, piece, model_dim), F32),
            dma((3,)), dma((local_count, 3)), dma((len(WHOLE) + 2,)), dma((len(TABLES),)), dma((3,)), dma((5,)), dma((5,)),
            dma((2,)), dma((2,)), dma((3,)),
            dma(()), dma((3,)), dma(()), dma(()), dma(()), dma(()), dma(()), dma(()), dma((3,)),
        ]
        total = pltpu.VMEM(tokens.shape, F32)
        base, last = pl.pallas_call(
            functools.partial(kernel, side, cap),
            out_shape=(total, total),
            in_specs=[hbm] * 9,
            out_specs=(pl.BlockSpec(memory_space=pltpu.VMEM),) * 2,
            scratch_shapes=scratch,
            compiler_params=pltpu.CompilerParams(collective_id=0, has_side_effects=True, vmem_limit_bytes=63 * 1024 * 1024 - 3200 * 1024),
        )(expert_ids.T, gate_vals.T, tokens, w_gate, w_up, w_down, shared_gate, shared_up, shared_down)
        return (base + last).astype(tokens.dtype)

    row_spec = P(("dp", "ep"), None)
    expert_spec = P("ep", None, None)
    whole_spec = P(None, None)
    return jax.shard_map(moe_step, mesh=mesh, in_specs=(row_spec, row_spec, row_spec, expert_spec, expert_spec, expert_spec, whole_spec, whole_spec, whole_spec), out_specs=row_spec, check_vma=False)
```

```python
import functools
import math

import jax
import jax.numpy as jnp
from jax import lax
from jax.experimental import pallas as pl
from jax.experimental.pallas import tpu as pltpu
from jax.sharding import PartitionSpec as P

F32 = jnp.float32
BF16 = jnp.bfloat16
MESH = pl.DeviceIdType.MESH


OFFSETS = (0, -1, 1, 2)
SIDE = (1, 2)

WHOLE = {(0, 0): 0, (0, 1): 1, (0, 2): 2, (0, 3): 3, (1, 0): 4, (1, 2): 5, (2, 1): 6, (2, 3): 7}

TABLES = ((0, 1), (0, 2), (0, 3), (1, 0), (1, 2), (2, 0), (2, 1), (2, 3), (3, 0))


def kernel(side, cap, ids_hbm, gat_hbm, tok_hbm, wg_hbm, wu_hbm, wd_hbm, sg_hbm, su_hbm, sd_hbm, acc, last,
           ids_ref, gat_ref, w_g, w_u, w_d, tok, info, xg, stage, raw, relay, gsplit, part, half, fin,
           own_sem, load_sem, tok_r, inf_r, x_r, raw_r, rel_r, half_r, fin_r, wr_r,
           tok_s, near_s, far_s, inf_s, f_s, rel_s, half_s, fin_s, wr_s):
    tok_count, model_dim = tok_hbm.shape
    top_count = ids_hbm.shape[0]
    local_count, _, ff = wg_hbm.shape
    chip_experts = 2 * local_count
    expert_count = local_count * side * side * 2
    block = chip_experts * cap
    piece = tok_count // 2
    chunks = 2
    width = model_dim // chunks

    me = lax.axis_index("ep")
    c = me % 2
    chip = me // 2
    cx, cy = chip % side, chip // side
    u = (1 - c) * cx + c * cy
    v = (1 - c) * cy + c * cx

    def chip_at(uu, vv):
        uu, vv = (uu + side) % side, (vv + side) % side
        return (1 - c) * (vv * side + uu) + c * (uu * side + vv)

    def dev_at(uu, vv):
        return chip_at(uu, vv) * 2 + c

    u_dev = (dev_at(u + 1, v), dev_at(u - 1, v))
    v_dev = (dev_at(u, v + 1), dev_at(u, v - 1))
    v_chip = (chip_at(u, v + 1), chip_at(u, v - 1))
    partner = chip * 2 + (1 - c)

    def send(src, dst, ssem, rsem, dev):
        copy = pltpu.make_async_remote_copy(src_ref=src, dst_ref=dst, send_sem=ssem, recv_sem=rsem,
                                            device_id={"ep": dev}, device_id_type=MESH)
        copy.start()
        return copy

    def filled(dst, sem):
        pltpu.make_async_copy(dst, dst, sem).wait()

    def rows_of(p):
        return pl.ds(p * piece, piece)

    barrier = pltpu.get_barrier_semaphore()
    for dev in u_dev + v_dev + (partner,):
        pl.semaphore_signal(barrier, inc=1, device_id={"ep": dev}, device_id_type=MESH)

    routes = [pltpu.make_async_copy(src, dst, own_sem.at[i + 1])
              for i, (src, dst) in enumerate(((ids_hbm, ids_ref), (gat_hbm, gat_ref)))]
    for copy in routes:
        copy.start()
    own = pltpu.make_async_copy(tok_hbm, tok.at[0], own_sem.at[0])
    own.start()
    def tok_wait(g, k, p):
        filled(tok.at[k, rows_of(p)], tok_r.at[2 * k + p - 2])

    def block_wait(g, k):
        filled(tok.at[WHOLE[g, k]], tok_r.at[WHOLE[g, k] + 2])

    def send_u_own(order):
        for d in range(2):
            p = (d + order) % 2
            send(tok.at[0, rows_of(p)], tok.at[SIDE[d], rows_of(p)], tok_s, tok_r.at[2 * SIDE[d] + p - 2], u_dev[d])

    def forward_u(d):
        tok_wait(0, SIDE[d], d)
        send(tok.at[SIDE[d], rows_of(d)], tok.at[3, rows_of(d)], tok_s, tok_r.at[4 + d], u_dev[d])

    def whole_v(k, p):
        d = k % 2
        at = WHOLE[SIDE[d], k]
        send(tok.at[k, rows_of(p)], tok.at[at, rows_of(p)], tok_s, tok_r.at[at + 2], v_dev[d])

    slot_rows = lax.broadcasted_iota(jnp.int32, (block, tok_count), 0) + c * (local_count * cap)
    turned = jnp.where(slot_rows >= block, slot_rows - block, slot_rows)
    n_step = 512 if model_dim % 512 == 0 else model_dim

    def row_codes(chip_idx):
        return (turned + chip_idx * block).astype(F32)

    def pick(g, k, chip_idx, dst, first):
        codes = row_codes(chip_idx)
        hit = jnp.zeros((block, tok_count), F32)
        for j in range(top_count):
            hit = hit + (info[4 * g + k, j:j + 1, :] == codes).astype(F32)
        hit = hit.astype(BF16)
        for n in range(0, model_dim, n_step):
            x = jnp.dot(hit, tok[WHOLE[g, k], :, n:n + n_step], preferred_element_type=F32).astype(BF16)
            for e in range(chip_experts):
                dst[e, first:first + cap, n:n + n_step] = x[e * cap:(e + 1) * cap]

    def group_rows(k):
        return pl.ds(k * cap, cap)

    near = [None] * 4

    def near_v(k):
        d = 1 - k % 2
        pick(0, k, v_chip[d], stage.at[k], 0)
        near[k] = send(stage.at[k], xg.at[SIDE[d], :, group_rows(k)], near_s.at[k] if k < 3 else far_s, x_r.at[SIDE[d] - 1], v_dev[d])

    codes_only = pl.ds(0, 8)

    def inf_rows(k):
        return pl.ds(0, 16) if k == 0 else codes_only

    def inf_wait(g, k):
        filled(info.at[4 * g + k, inf_rows(k)], inf_r.at[TABLES.index((g, k))])

    def far_v(k):
        d = k % 2
        g = SIDE[d]
        block_wait(g, k)
        inf_wait(g, k)
        at = k if k < 3 else 4
        if k < 3:
            near[k].wait_send()
        pick(g, k, v_chip[d], stage.at[at], 0)
        send(stage.at[at], xg.at[3, :, group_rows(k)], far_s, x_r.at[2], v_dev[d])
        if k == 0:
            send(info.at[4 * g], info.at[12], inf_s, inf_r.at[TABLES.index((3, 0))], v_dev[d])

    def info_v(k):
        for d in range(2):
            if k == 0 or d == k % 2:
                send(info.at[k, inf_rows(k)], info.at[4 * SIDE[d] + k, inf_rows(k)], inf_s,
                     inf_r.at[TABLES.index((SIDE[d], k))], v_dev[d])

    own.wait()
    pl.semaphore_wait(barrier, 5)
    send_u_own(0)
    whole_v(0, 0)

    for copy in routes:
        copy.wait()
    expert = lax.broadcasted_iota(jnp.int32, (expert_count, tok_count), 0)
    hots = []
    chosen = jnp.zeros((expert_count, tok_count), F32)
    for j in range(top_count):
        hot = (ids_ref[j:j + 1, :] == expert).astype(F32)
        hots.append(hot)
        chosen = chosen + hot
    above = (lax.broadcasted_iota(jnp.int32, (tok_count, tok_count), 0)
             < lax.broadcasted_iota(jnp.int32, (tok_count, tok_count), 1)).astype(F32).astype(BF16)
    slot = jnp.dot(chosen.astype(BF16), above, preferred_element_type=F32)
    info[0] = jnp.zeros((16, tok_count), F32)
    for j in range(top_count):
        info[0, j:j + 1, :] = ids_ref[j:j + 1, :].astype(F32) * cap + jnp.sum(hots[j] * slot, axis=0, keepdims=True)
        info[0, 8 + j:9 + j, :] = gat_ref[j:j + 1, :]

    for d in range(2):
        send(info.at[0, codes_only], info.at[SIDE[d], codes_only], inf_s, inf_r.at[TABLES.index((0, SIDE[d]))], u_dev[d])
    info_v(0)
    send_u_own(1)
    whole_v(0, 1)

    shared_loads = []
    for i in range(local_count):
        cols = pl.ds(i * ff, ff)
        for j, (src, dst) in enumerate(((sg_hbm.at[:, cols], w_g), (su_hbm.at[:, cols], w_u), (sd_hbm.at[cols], w_d))):
            copy = pltpu.make_async_copy(src, dst.at[i], load_sem.at[i, j])
            copy.start()
            shared_loads.append(copy)

    near_v(0)

    for i in range(local_count):
        for j, (src, dst) in enumerate(((wg_hbm, w_g), (wu_hbm, w_u), (wd_hbm, w_d))):
            send(src.at[i], dst.at[local_count + i], wr_s.at[j], wr_r.at[j], partner)

    def silu_mul(g, up):
        return (jax.nn.silu(g) * up).astype(BF16)

    def shared_part(i):
        for copy in shared_loads[3 * i:3 * i + 3]:
            copy.wait()
        x = tok[0]
        h = silu_mul(jnp.dot(x, w_g[i], preferred_element_type=F32), jnp.dot(x, w_u[i], preferred_element_type=F32))
        for n in range(0, model_dim, n_step):
            y = jnp.dot(h, w_d[i, :, n:n + n_step], preferred_element_type=F32)
            if i > 0:
                y = y + acc[:, n:n + n_step]
            if i == local_count - 1:
                y = y.astype(BF16).astype(F32) + x[:, n:n + n_step].astype(F32)
            acc[:, n:n + n_step] = y

    own_loads = []

    def load_own(i):
        for j, (src, dst) in enumerate(((wg_hbm, w_g), (wu_hbm, w_u), (wd_hbm, w_d))):
            copy = pltpu.make_async_copy(src.at[i], dst.at[i], load_sem.at[i, j])
            copy.start()
            own_loads.append(copy)

    for i in range(local_count):
        shared_part(i)
        load_own(i)

    inf_wait(0, 1)
    send(info.at[1, codes_only], info.at[3, codes_only], inf_s, inf_r.at[TABLES.index((0, 3))], u_dev[0])
    info_v(1)
    inf_wait(0, 2)
    info_v(2)
    forward_u(0)
    forward_u(1)
    whole_v(1, 0)
    whole_v(2, 1)
    tok_wait(0, 1, 1)
    whole_v(1, 1)
    tok_wait(0, 2, 0)
    whole_v(2, 0)
    near_v(1)
    near_v(2)
    far_v(0)
    for p in range(2):
        tok_wait(0, 3, p)
        whole_v(3, p)
    inf_wait(0, 3)
    info_v(3)
    near_v(3)

    def experts(g):
        def one(e, carry):
            x = xg[g, e]
            h = silu_mul(jnp.dot(x, w_g[e], preferred_element_type=F32), jnp.dot(x, w_u[e], preferred_element_type=F32))
            for n in range(0, model_dim, n_step):
                y = jnp.dot(h, w_d[e, :, n:n + n_step], preferred_element_type=F32).astype(BF16)
                raw[g, 0, e, :, n:n + n_step] = y[0:cap]
                xg[g, e, cap:4 * cap, n:n + n_step] = y[cap:4 * cap]
            return carry

        lax.fori_loop(0, chip_experts, one, 0)

    def own_pick(g, ks):
        for k in ks:
            pick(g, k, chip, xg.at[g], k * cap)

    def x_wait(g, ks):
        filled(xg.at[g, pl.ds(0, len(ks) * chip_experts // 4)], x_r.at[g - 1])

    def e_half(d):
        return pl.ds(d * local_count, local_count)

    def col_chunk(f):
        return slice(None) if f is None else pl.ds(f * width, width)

    def send_rows(g, f=None):
        at = col_chunk(f)
        i = f or 0
        for d in range(2):
            send(xg.at[g, e_half(d), group_rows(3), at], relay.at[g, d, :, :, at], f_s, rel_r.at[g + i], u_dev[d])
        for d in range(2):
            send(xg.at[g, :, group_rows(2 - d), at], raw.at[g, SIDE[d], :, :, at], f_s, raw_r.at[g + i], u_dev[d])

    def pass_rows(g, f=None):
        at = col_chunk(f)
        i = f or 0
        filled(relay.at[g, :, :, :, at], rel_r.at[g + i])
        for d in range(2):
            send(relay.at[g, d, :, :, at], raw.at[g, 3, e_half(d), :, at], rel_s, raw_r.at[g + i], u_dev[d])

    def raw_wait(g, f=None):
        at = col_chunk(f)
        i = f or 0
        filled(raw.at[g, pl.ds(1, 3), :, :, at], raw_r.at[g + i])

    def gates_of(g):
        for m in range(4):
            codes = row_codes(chip_at(u + OFFSETS[m], v))
            gate = jnp.zeros((block, tok_count), F32)
            for j in range(top_count):
                gate = gate + jnp.where(info[4 * g, j:j + 1, :] == codes, info[4 * g, 8 + j:9 + j, :], 0.0)
            gate = gate.T
            for s in range(3):
                part_s = gate.astype(BF16)
                gsplit[s * tok_count:(s + 1) * tok_count, m * block:(m + 1) * block] = part_s
                gate = gate - part_s.astype(F32)

    step = 256 if width % 256 == 0 else width

    def gated(g, f=None):
        first, count = (0, model_dim // step) if f is None else (f * (width // step), width // step)

        def cols(n, carry):
            at = pl.ds(pl.multiple_of(n * step, 128), step)
            rows = raw[g, :, :, :, at].reshape(4 * block, step)
            y = jnp.dot(gsplit[...], rows, preferred_element_type=F32)
            y = y[0:tok_count] + y[tok_count:2 * tok_count] + y[2 * tok_count:3 * tok_count]
            if g == 0:
                acc[:, at] = acc[:, at] + y
            else:
                part[g - 1, :, at] = y
            return carry

        lax.fori_loop(first, first + count, cols, 0)

    def send_early(g, d):
        send(part.at[g - 1, rows_of(1 - d)], fin.at[d], fin_s, fin_r.at[0], v_dev[d])

    def send_last(g, d, f):
        at = col_chunk(f)
        send(part.at[g - 1, rows_of(d), at], last.at[rows_of(d), at], fin_s, fin_r.at[1], v_dev[d])

    own_pick(0, range(4))
    for copy in own_loads:
        copy.wait()
    for j, dst in enumerate((w_g, w_u, w_d)):
        filled(dst.at[pl.ds(local_count, local_count)], wr_r.at[j])
    experts(0)
    far_v(1)
    send_rows(0)
    far_v(2)
    far_v(3)
    pass_rows(0)
    own_pick(2, (1, 3))
    x_wait(2, (0, 2))
    experts(2)
    send_rows(2)
    own_pick(1, (0, 2))
    pass_rows(2)
    x_wait(1, (1, 3))
    experts(1)
    send_rows(1)
    raw_wait(0)
    gates_of(0)
    gated(0)
    x_wait(3, range(4))
    experts(3)
    pass_rows(1)
    for f in range(chunks):
        send_rows(3, f)
    raw_wait(2)
    inf_wait(2, 0)
    gates_of(2)
    gated(2)
    inf_wait(3, 0)
    raw_wait(1)
    gates_of(1)
    pass_rows(3, 0)
    gated(1)
    send_early(1, 1)
    send_early(2, 0)
    for f in range(1, chunks):
        pass_rows(3, f)
    gates_of(3)
    for f in range(chunks):
        raw_wait(3, f)
        gated(3, f)
        for d in range(2):
            send(part.at[2, rows_of(d), col_chunk(f)], half.at[d, :, col_chunk(f)], half_s, half_r.at[f], v_dev[d])
    for f in range(chunks):
        at = slice(f * width, (f + 1) * width)
        filled(half.at[:, :, col_chunk(f)], half_r.at[f])
        for d in range(2):
            g = 2 - d
            rows = slice(d * piece, (d + 1) * piece)
            part[g - 1, rows, at] = part[g - 1, rows, at] + half[d, :, at]
            send_last(g, d, f)

    filled(fin, fin_r.at[0])
    for d in range(2):
        rows = slice((1 - d) * piece, (2 - d) * piece)
        acc[rows] = acc[rows] + fin[d]

    filled(tok.at[pl.ds(0, 7)], tok_s)
    filled(stage, far_s)
    filled(info.at[pl.ds(0, 6)], inf_s)
    for j, dst in enumerate((w_g, w_u, w_d)):
        filled(dst.at[pl.ds(0, local_count)], wr_s.at[j])
    filled(raw.at[pl.ds(0, 3)], f_s)
    filled(relay, rel_s)
    filled(half, half_s)
    filled(part.at[pl.ds(0, 2)], fin_s)
    filled(last, fin_r.at[1])


def solution(mesh):
    group_size = mesh.shape["ep"]
    side = math.isqrt(group_size // 2)

    def moe_step(tokens, expert_ids, gate_vals, w_gate, w_up, w_down, shared_gate, shared_up, shared_down):
        tok_count, model_dim = tokens.shape
        top_count = expert_ids.shape[1]
        local_count, _, ff = w_gate.shape
        expert_count = local_count * group_size
        spread = max(group_size, expert_count // 2)
        cap = (tok_count * top_count + spread - 1) // spread
        block = 2 * local_count * cap
        piece = tok_count // 2
        dma = pltpu.SemaphoreType.DMA
        hbm = pl.BlockSpec(memory_space=pl.ANY)
        scratch = [
            pltpu.VMEM((top_count, tok_count), jnp.int32),
            pltpu.VMEM((top_count, tok_count), F32),
            pltpu.VMEM((2 * local_count, model_dim, ff), BF16),
            pltpu.VMEM((2 * local_count, model_dim, ff), BF16),
            pltpu.VMEM((2 * local_count, ff, model_dim), BF16),
            pltpu.VMEM((len(WHOLE), tok_count, model_dim), BF16),
            pltpu.VMEM((16, 16, tok_count), F32),
            pltpu.VMEM((4, 2 * local_count, 4 * cap, model_dim), BF16),
            pltpu.VMEM((5, 2 * local_count, cap, model_dim), BF16),
            pltpu.VMEM((4, 4, 2 * local_count, cap, model_dim), BF16),
            pltpu.VMEM((4, 2, local_count, cap, model_dim), BF16),
            pltpu.VMEM((3 * tok_count, 4 * block), BF16),
            pltpu.VMEM((3, tok_count, model_dim), F32),
            pltpu.VMEM((2, piece, model_dim), F32),
            pltpu.VMEM((2, piece, model_dim), F32),
            dma((3,)), dma((local_count, 3)), dma((len(WHOLE) + 2,)), dma((len(TABLES),)), dma((3,)), dma((5,)), dma((5,)),
            dma((2,)), dma((2,)), dma((3,)),
            dma(()), dma((3,)), dma(()), dma(()), dma(()), dma(()), dma(()), dma(()), dma((3,)),
        ]
        total = pltpu.VMEM(tokens.shape, F32)
        base, last = pl.pallas_call(
            functools.partial(kernel, side, cap),
            out_shape=(total, total),
            in_specs=[hbm] * 9,
            out_specs=(pl.BlockSpec(memory_space=pltpu.VMEM),) * 2,
            scratch_shapes=scratch,
            compiler_params=pltpu.CompilerParams(collective_id=0, has_side_effects=True, vmem_limit_bytes=63 * 1024 * 1024 - 3200 * 1024),
        )(expert_ids.T, gate_vals.T, tokens, w_gate, w_up, w_down, shared_gate, shared_up, shared_down)
        return (base + last).astype(tokens.dtype)

    row_spec = P(("dp", "ep"), None)
    expert_spec = P("ep", None, None)
    whole_spec = P(None, None)
    return jax.shard_map(moe_step, mesh=mesh, in_specs=(row_spec, row_spec, row_spec, expert_spec, expert_spec, expert_spec, whole_spec, whole_spec, whole_spec), out_specs=row_spec, check_vma=False)
```

```python
import functools
import math

import jax
import jax.numpy as jnp
from jax import lax
from jax.experimental import pallas as pl
from jax.experimental.pallas import tpu as pltpu
from jax.sharding import PartitionSpec as P

F32 = jnp.float32
BF16 = jnp.bfloat16
MESH = pl.DeviceIdType.MESH


def scoped(fn):
    @functools.wraps(fn)
    def run(*a):
        tag = "_".join(str(x) for x in a if isinstance(x, (int, tuple, list, range)))
        with jax.named_scope((fn.__name__ + "#a=" + tag).replace(" ", "").replace("(", "").replace(")", "").replace(",", "_")):
            return fn(*a)
    return run


OFFSETS = (0, -1, 1, 2)
SIDE = (1, 2)

WHOLE = {(0, 0): 0, (0, 1): 1, (0, 2): 2, (1, 1): 3, (2, 0): 4, (2, 2): 5, (3, 1): 6}
WAY = (1, 0, 1)
TABLES = ((0, 1), (0, 2), (1, 0), (1, 1), (2, 0), (2, 2), (3, 0), (3, 1))


def kernel(side, cap, ids_hbm, gat_hbm, tok_hbm, wg_hbm, wu_hbm, wd_hbm, sg_hbm, su_hbm, sd_hbm, acc, last,
           ids_ref, gat_ref, w_g, w_u, w_d, tok, info, xg, stage, raw, relay, gsplit, part, half, fin,
           own_sem, load_sem, tok_r, inf_r, x_r, raw_r, rel_r, half_r, fin_r, wr_r,
           tok_s, near_s, far_s, inf_s, f_s, rel_s, half_s, fin_s, wr_s):
    tok_count, model_dim = tok_hbm.shape
    top_count = ids_hbm.shape[0]
    local_count, _, ff = wg_hbm.shape
    chip_experts = 2 * local_count
    expert_count = local_count * side * side * 2
    block = chip_experts * cap
    piece = tok_count // 2
    chunks = 2
    width = model_dim // chunks

    me = lax.axis_index("ep")
    c = me % 2
    chip = me // 2
    cx, cy = chip % side, chip // side
    u = (1 - c) * cx + c * cy
    v = (1 - c) * cy + c * cx

    def chip_at(uu, vv):
        uu, vv = (uu + side) % side, (vv + side) % side
        return (1 - c) * (vv * side + uu) + c * (uu * side + vv)

    def dev_at(uu, vv):
        return chip_at(uu, vv) * 2 + c

    u_dev = (dev_at(u + 1, v), dev_at(u - 1, v))
    v_dev = (dev_at(u, v + 1), dev_at(u, v - 1))
    u_chip = (chip_at(u + 1, v), chip_at(u - 1, v))
    v_chip = (chip_at(u, v + 1), chip_at(u, v - 1))
    partner = chip * 2 + (1 - c)

    def send(src, dst, ssem, rsem, dev):
        copy = pltpu.make_async_remote_copy(src_ref=src, dst_ref=dst, send_sem=ssem, recv_sem=rsem,
                                            device_id={"ep": dev}, device_id_type=MESH)
        copy.start()
        return copy

    def filled(dst, sem):
        pltpu.make_async_copy(dst, dst, sem).wait()

    def rows_of(p):
        return pl.ds(p * piece, piece)

    barrier = pltpu.get_barrier_semaphore()
    for dev in u_dev + v_dev + (partner,):
        pl.semaphore_signal(barrier, inc=1, device_id={"ep": dev}, device_id_type=MESH)

    routes = [pltpu.make_async_copy(src, dst, own_sem.at[i + 1])
              for i, (src, dst) in enumerate(((ids_hbm, ids_ref), (gat_hbm, gat_ref)))]
    for copy in routes:
        copy.start()
    own = pltpu.make_async_copy(tok_hbm, tok.at[0], own_sem.at[0])
    own.start()
    @scoped
    def tok_wait(g, k, p):
        filled(tok.at[k, rows_of(p)], tok_r.at[2 * k + p - 2])

    @scoped
    def block_wait(g, k):
        filled(tok.at[WHOLE[g, k]], tok_r.at[WHOLE[g, k] + 1])

    def send_u_own(order):
        for d in range(2):
            p = (d + order) % 2
            send(tok.at[0, rows_of(p)], tok.at[SIDE[d], rows_of(p)], tok_s, tok_r.at[2 * SIDE[d] + p - 2], u_dev[d])

    def whole_v(k, p):
        d = WAY[k]
        at = WHOLE[SIDE[d], k]
        send(tok.at[k, rows_of(p)], tok.at[at, rows_of(p)], tok_s, tok_r.at[at + 1], v_dev[d])

    slot_rows = lax.broadcasted_iota(jnp.int32, (block, tok_count), 0) + c * (local_count * cap)
    turned = jnp.where(slot_rows >= block, slot_rows - block, slot_rows)
    n_step = 512 if model_dim % 512 == 0 else model_dim

    def row_codes(chip_idx):
        return (turned + chip_idx * block).astype(F32)

    def pick(g, k, chip_idx, dst, first, es=(0, chip_experts)):
        codes = row_codes(chip_idx)[es[0] * cap:es[1] * cap]
        hit = jnp.zeros(codes.shape, F32)
        for j in range(top_count):
            hit = hit + (info[table_at(g, k, j), :] == codes).astype(F32)
        hit = hit.astype(BF16)
        for n in range(0, model_dim, n_step):
            x = jnp.dot(hit, tok[WHOLE[g, k], :, n:n + n_step], preferred_element_type=F32).astype(BF16)
            for e in range(*es):
                dst[e, first:first + cap, n:n + n_step] = x[(e - es[0]) * cap:(e - es[0] + 1) * cap]

    def group_rows(k):
        return pl.ds(k * cap, cap)

    @scoped
    def send_picked(g, k, chip_idx, at, ssem, to_g, to_k, dev):
        pick(g, k, chip_idx, stage.at[at], 0)
        return send(stage.at[at], xg.at[to_g, :, group_rows(to_k)], ssem, x_r.at[to_g], dev)

    @scoped
    def near_v(k):
        d = 1 - WAY[k]
        return send_picked(0, k, v_chip[d], (0, 2, 3)[k], far_s if k == 2 else near_s.at[k], SIDE[d], k, v_dev[d])

    def table_at(g, k, j, n=1):
        first = 16 * (4 * g + k) + j
        return slice(first, first + n)

    def table_ref(g, k, n):
        return info.at[pl.ds(16 * (4 * g + k), n)]

    def send_info(at, to, n, dev):
        send(table_ref(*at, n), table_ref(*to, n), inf_s, inf_r.at[TABLES.index(to)], dev)

    @scoped
    def inf_wait(g, k):
        filled(table_ref(g, k, 16 if k == 0 else 8), inf_r.at[TABLES.index((g, k))])

    with jax.named_scope('ownwait'):
        own.wait()
    with jax.named_scope('barrier'):
        pl.semaphore_wait(barrier, 5)
    send_u_own(0)
    whole_v(0, 0)

    for copy in routes:
        copy.wait()
    expert = lax.broadcasted_iota(jnp.int32, (expert_count, tok_count), 0)
    hots = []
    chosen = jnp.zeros((expert_count, tok_count), F32)
    for j in range(top_count):
        hot = (ids_ref[j:j + 1, :] == expert).astype(F32)
        hots.append(hot)
        chosen = chosen + hot
    above = (lax.broadcasted_iota(jnp.int32, (tok_count, tok_count), 0)
             < lax.broadcasted_iota(jnp.int32, (tok_count, tok_count), 1)).astype(F32).astype(BF16)
    slot = jnp.dot(chosen.astype(BF16), above, preferred_element_type=F32)
    info[0:16] = jnp.zeros((16, tok_count), F32)
    for j in range(top_count):
        info[j:j + 1, :] = ids_ref[j:j + 1, :].astype(F32) * cap + jnp.sum(hots[j] * slot, axis=0, keepdims=True)
        info[8 + j:9 + j, :] = gat_ref[j:j + 1, :]

    for d in range(2):
        send_info((0, 0), (0, SIDE[d]), 8, u_dev[d])
        send_info((0, 0), (SIDE[d], 0), 16, v_dev[d])
    send_u_own(1)
    whole_v(0, 1)

    shared_loads = []
    for i in range(local_count):
        cols = pl.ds(i * ff, ff)
        for j, (src, dst) in enumerate(((sg_hbm.at[:, cols], w_g), (su_hbm.at[:, cols], w_u), (sd_hbm.at[cols], w_d))):
            copy = pltpu.make_async_copy(src, dst.at[i], load_sem.at[i, j])
            copy.start()
            shared_loads.append(copy)

    near_0 = near_v(0)

    for i in range(local_count):
        for j, (src, dst) in enumerate(((wg_hbm, w_g), (wu_hbm, w_u), (wd_hbm, w_d))):
            send(src.at[i], dst.at[local_count + i], wr_s.at[j], wr_r.at[j], partner)

    def silu_mul(g, up):
        return (jax.nn.silu(g) * up).astype(BF16)

    @scoped
    def shared_part(i):
        for copy in shared_loads[3 * i:3 * i + 3]:
            copy.wait()
        x = tok[0]
        h = silu_mul(jnp.dot(x, w_g[i], preferred_element_type=F32), jnp.dot(x, w_u[i], preferred_element_type=F32))
        for n in range(0, model_dim, n_step):
            y = jnp.dot(h, w_d[i, :, n:n + n_step], preferred_element_type=F32)
            if i > 0:
                y = y + acc[:, n:n + n_step]
            if i == local_count - 1:
                y = y.astype(BF16).astype(F32) + x[:, n:n + n_step].astype(F32)
            acc[:, n:n + n_step] = y

    own_loads = []

    def load_own(i):
        for j, (src, dst) in enumerate(((wg_hbm, w_g), (wu_hbm, w_u), (wd_hbm, w_d))):
            copy = pltpu.make_async_copy(src.at[i], dst.at[i], load_sem.at[i, j])
            copy.start()
            own_loads.append(copy)

    for i in range(local_count):
        shared_part(i)
        load_own(i)

    def e_half(d):
        return pl.ds(d * local_count, local_count)

    inf_wait(0, 1)
    send_info((0, 1), (1, 1), 8, v_dev[0])
    inf_wait(0, 2)
    send_info((0, 2), (2, 2), 8, v_dev[1])
    for k, p in ((1, 0), (2, 1), (1, 1), (2, 0)):
        tok_wait(0, k, p)
        whole_v(k, p)
    for d in range(2):
        pick(0, SIDE[d], u_chip[d], stage.at[1], 0, (d * local_count, (d + 1) * local_count))
        send(stage.at[1, e_half(d)], xg.at[0, e_half(d), group_rows(3)], near_s.at[2], x_r.at[0], u_dev[d])
    near_1 = near_v(1)
    near_v(2)
    block_wait(2, 0)
    inf_wait(2, 0)
    send_info((2, 0), (3, 0), 16, v_dev[1])
    send_picked(2, 0, v_chip[1], 4, far_s, 3, 0, v_dev[1])
    block_wait(1, 1)
    send(tok.at[WHOLE[1, 1]], tok.at[WHOLE[3, 1]], tok_s, tok_r.at[WHOLE[3, 1] + 1], v_dev[0])
    inf_wait(1, 1)
    send_info((1, 1), (3, 1), 8, v_dev[0])
    send_picked(1, 1, u_chip[0], 5, far_s, 1, 3, u_dev[0])

    @scoped
    def experts(g):
        def one(e, carry):
            x = xg[g, e]
            h = silu_mul(jnp.dot(x, w_g[e], preferred_element_type=F32), jnp.dot(x, w_u[e], preferred_element_type=F32))
            for n in range(0, model_dim, n_step):
                y = jnp.dot(h, w_d[e, :, n:n + n_step], preferred_element_type=F32).astype(BF16)
                raw[g, 0, e, :, n:n + n_step] = y[0:cap]
                xg[g, e, cap:4 * cap, n:n + n_step] = y[cap:4 * cap]
            return carry

        lax.fori_loop(0, chip_experts, one, 0)

    @scoped
    def own_pick(g, ks):
        for k in ks:
            pick(g, k, chip, xg.at[g], k * cap)

    @scoped
    def x_wait(g, ks):
        filled(xg.at[g, pl.ds(0, len(ks) * chip_experts // 4)], x_r.at[g])

    def col_chunk(f):
        return slice(None) if f is None else pl.ds(f * width, width)

    @scoped
    def send_rows(g, f=None):
        at = col_chunk(f)
        i = f or 0
        for d in range(2):
            send(xg.at[g, e_half(d), group_rows(3), at], relay.at[g, d, :, :, at], f_s, rel_r.at[g + i], u_dev[d])
        for d in range(2):
            send(xg.at[g, :, group_rows(2 - d), at], raw.at[g, SIDE[d], :, :, at], f_s, raw_r.at[g + i], u_dev[d])

    @scoped
    def pass_rows(g, f=None):
        at = col_chunk(f)
        i = f or 0
        filled(relay.at[g, :, :, :, at], rel_r.at[g + i])
        for d in range(2):
            send(relay.at[g, d, :, :, at], raw.at[g, 3, e_half(d), :, at], rel_s, raw_r.at[g + i], u_dev[d])

    @scoped
    def raw_wait(g, f=None):
        at = col_chunk(f)
        i = f or 0
        filled(raw.at[g, pl.ds(1, 3), :, :, at], raw_r.at[g + i])

    @scoped
    def gates_of(g):
        for m in range(4):
            codes = row_codes(chip_at(u + OFFSETS[m], v))
            gate = jnp.zeros((block, tok_count), F32)
            for j in range(top_count):
                gate = gate + jnp.where(info[table_at(g, 0, j), :] == codes, info[table_at(g, 0, 8 + j), :], 0.0)
            gate = gate.T
            for s in range(3):
                part_s = gate.astype(BF16)
                gsplit[s * tok_count:(s + 1) * tok_count, m * block:(m + 1) * block] = part_s
                gate = gate - part_s.astype(F32)

    step = 256 if width % 256 == 0 else width

    @scoped
    def gated(g, f=None):
        first, count = (0, model_dim // step) if f is None else (f * (width // step), width // step)

        def cols(n, carry):
            at = pl.ds(pl.multiple_of(n * step, 128), step)
            rows = raw[g, :, :, :, at].reshape(4 * block, step)
            y = jnp.dot(gsplit[...], rows, preferred_element_type=F32)
            y = y[0:tok_count] + y[tok_count:2 * tok_count] + y[2 * tok_count:3 * tok_count]
            if g == 0:
                acc[:, at] = acc[:, at] + y
            else:
                part[g - 1, :, at] = y
            return carry

        lax.fori_loop(first, first + count, cols, 0)

    def send_early(g, d):
        send(part.at[g - 1, rows_of(1 - d)], fin.at[d], fin_s, fin_r.at[0], v_dev[d])

    def send_last(g, d, f):
        at = col_chunk(f)
        send(part.at[g - 1, rows_of(d), at], last.at[rows_of(d), at], fin_s, fin_r.at[1], v_dev[d])

    own_pick(0, (0, 1, 2))
    for copy in own_loads:
        copy.wait()
    for j, dst in enumerate((w_g, w_u, w_d)):
        filled(dst.at[pl.ds(local_count, local_count)], wr_r.at[j])
    x_wait(0, (3,))
    experts(0)
    block_wait(2, 2)
    inf_wait(2, 2)
    near_0.wait_send()
    send_picked(2, 2, v_chip[1], 0, far_s, 3, 2, v_dev[1])
    filled(stage.at[1], near_s.at[2])
    send_picked(2, 2, u_chip[1], 1, far_s, 2, 3, u_dev[1])
    send_rows(0)
    own_pick(1, (1,))
    x_wait(1, (0, 2, 3))
    experts(1)
    block_wait(3, 1)
    inf_wait(3, 1)
    near_1.wait_send()
    send_picked(3, 1, u_chip[0], 2, far_s, 3, 3, u_dev[0])
    pass_rows(0)
    send_rows(1)
    own_pick(2, (0, 2))
    own_pick(3, (1,))
    pass_rows(1)
    x_wait(2, (1, 3))
    experts(2)
    send_rows(2)
    raw_wait(0)
    gates_of(0)
    gated(0)
    x_wait(3, (0, 2, 3))
    experts(3)
    pass_rows(2)
    for f in range(chunks):
        send_rows(3, f)
    raw_wait(1)
    inf_wait(1, 0)
    gates_of(1)
    gated(1)
    inf_wait(3, 0)
    raw_wait(2)
    gates_of(2)
    pass_rows(3, 0)
    gated(2)
    send_early(1, 1)
    send_early(2, 0)
    for f in range(1, chunks):
        pass_rows(3, f)
    gates_of(3)
    for f in range(chunks):
        raw_wait(3, f)
        gated(3, f)
        for d in range(2):
            send(part.at[2, rows_of(d), col_chunk(f)], half.at[d, :, col_chunk(f)], half_s, half_r.at[f], v_dev[d])
    for f in range(chunks):
        at = slice(f * width, (f + 1) * width)
        filled(half.at[:, :, col_chunk(f)], half_r.at[f])
        for d in range(2):
            g = 2 - d
            rows = slice(d * piece, (d + 1) * piece)
            part[g - 1, rows, at] = part[g - 1, rows, at] + half[d, :, at]
            send_last(g, d, f)

    filled(fin, fin_r.at[0])
    for d in range(2):
        rows = slice((1 - d) * piece, (2 - d) * piece)
        acc[rows] = acc[rows] + fin[d]

    filled(tok.at[pl.ds(0, 6)], tok_s)
    filled(stage, far_s)
    filled(info.at[pl.ds(0, 5 * 8 + 3 * 16)], inf_s)
    for j, dst in enumerate((w_g, w_u, w_d)):
        filled(dst.at[pl.ds(0, local_count)], wr_s.at[j])
    filled(raw.at[pl.ds(0, 3)], f_s)
    filled(relay, rel_s)
    filled(half, half_s)
    filled(part.at[pl.ds(0, 2)], fin_s)
    filled(last, fin_r.at[1])


def solution(mesh):
    group_size = mesh.shape["ep"]
    side = math.isqrt(group_size // 2)

    def moe_step(tokens, expert_ids, gate_vals, w_gate, w_up, w_down, shared_gate, shared_up, shared_down):
        tok_count, model_dim = tokens.shape
        top_count = expert_ids.shape[1]
        local_count, _, ff = w_gate.shape
        expert_count = local_count * group_size
        spread = max(group_size, expert_count // 2)
        cap = (tok_count * top_count + spread - 1) // spread
        block = 2 * local_count * cap
        piece = tok_count // 2
        dma = pltpu.SemaphoreType.DMA
        hbm = pl.BlockSpec(memory_space=pl.ANY)
        scratch = [
            pltpu.VMEM((top_count, tok_count), jnp.int32),
            pltpu.VMEM((top_count, tok_count), F32),
            pltpu.VMEM((2 * local_count, model_dim, ff), BF16),
            pltpu.VMEM((2 * local_count, model_dim, ff), BF16),
            pltpu.VMEM((2 * local_count, ff, model_dim), BF16),
            pltpu.VMEM((len(WHOLE), tok_count, model_dim), BF16),
            pltpu.VMEM((16 * 16, tok_count), F32),
            pltpu.VMEM((4, 2 * local_count, 4 * cap, model_dim), BF16),
            pltpu.VMEM((6, 2 * local_count, cap, model_dim), BF16),
            pltpu.VMEM((4, 4, 2 * local_count, cap, model_dim), BF16),
            pltpu.VMEM((4, 2, local_count, cap, model_dim), BF16),
            pltpu.VMEM((3 * tok_count, 4 * block), BF16),
            pltpu.VMEM((3, tok_count, model_dim), F32),
            pltpu.VMEM((2, piece, model_dim), F32),
            pltpu.VMEM((2, piece, model_dim), F32),
            dma((3,)), dma((local_count, 3)), dma((len(WHOLE) + 1,)), dma((len(TABLES),)), dma((4,)), dma((5,)), dma((5,)),
            dma((2,)), dma((2,)), dma((3,)),
            dma(()), dma((3,)), dma(()), dma(()), dma(()), dma(()), dma(()), dma(()), dma((3,)),
        ]
        total = pltpu.VMEM(tokens.shape, F32)
        base, last = pl.pallas_call(
            functools.partial(kernel, side, cap),
            out_shape=(total, total),
            in_specs=[hbm] * 9,
            out_specs=(pl.BlockSpec(memory_space=pltpu.VMEM),) * 2,
            scratch_shapes=scratch,
            compiler_params=pltpu.CompilerParams(collective_id=0, has_side_effects=True, vmem_limit_bytes=63 * 1024 * 1024 - 3200 * 1024),
        )(expert_ids.T, gate_vals.T, tokens, w_gate, w_up, w_down, shared_gate, shared_up, shared_down)
        return (base + last).astype(tokens.dtype)

    row_spec = P(("dp", "ep"), None)
    expert_spec = P("ep", None, None)
    whole_spec = P(None, None)
    return jax.shard_map(moe_step, mesh=mesh, in_specs=(row_spec, row_spec, row_spec, expert_spec, expert_spec, expert_spec, whole_spec, whole_spec, whole_spec), out_specs=row_spec, check_vma=False)
```

```python
import functools
import math

import jax
import jax.numpy as jnp
from jax import lax
from jax.experimental import pallas as pl
from jax.experimental.pallas import tpu as pltpu
from jax.sharding import PartitionSpec as P

F32 = jnp.float32
BF16 = jnp.bfloat16
MESH = pl.DeviceIdType.MESH


OFFSETS = (0, -1, 1, 2)
SIDE = (1, 2)

WHOLE = {(0, 0): 0, (0, 1): 1, (0, 2): 2, (1, 1): 3, (2, 0): 4, (2, 2): 5, (3, 1): 6}
WAY = (1, 0, 1)
TABLES = ((0, 1), (0, 2), (1, 0), (1, 1), (2, 0), (2, 2), (3, 0), (3, 1))


def kernel(side, cap, ids_hbm, gat_hbm, tok_hbm, wg_hbm, wu_hbm, wd_hbm, sg_hbm, su_hbm, sd_hbm, acc, last,
           ids_ref, gat_ref, w_g, w_u, w_d, tok, info, xg, stage, raw, relay, gsplit, part, half, fin,
           own_sem, load_sem, tok_r, inf_r, x_r, raw_r, rel_r, half_r, fin_r, wr_r,
           tok_s, near_s, far_s, inf_s, f_s, rel_s, half_s, fin_s, wr_s):
    tok_count, model_dim = tok_hbm.shape
    top_count = ids_hbm.shape[0]
    local_count, _, ff = wg_hbm.shape
    chip_experts = 2 * local_count
    expert_count = local_count * side * side * 2
    block = chip_experts * cap
    piece = tok_count // 2
    chunks = 2
    width = model_dim // chunks

    me = lax.axis_index("ep")
    c = me % 2
    chip = me // 2
    cx, cy = chip % side, chip // side
    u = (1 - c) * cx + c * cy
    v = (1 - c) * cy + c * cx

    def chip_at(uu, vv):
        uu, vv = (uu + side) % side, (vv + side) % side
        return (1 - c) * (vv * side + uu) + c * (uu * side + vv)

    def dev_at(uu, vv):
        return chip_at(uu, vv) * 2 + c

    u_dev = (dev_at(u + 1, v), dev_at(u - 1, v))
    v_dev = (dev_at(u, v + 1), dev_at(u, v - 1))
    u_chip = (chip_at(u + 1, v), chip_at(u - 1, v))
    v_chip = (chip_at(u, v + 1), chip_at(u, v - 1))
    partner = chip * 2 + (1 - c)

    def send(src, dst, ssem, rsem, dev):
        copy = pltpu.make_async_remote_copy(src_ref=src, dst_ref=dst, send_sem=ssem, recv_sem=rsem,
                                            device_id={"ep": dev}, device_id_type=MESH)
        copy.start()
        return copy

    def filled(dst, sem):
        pltpu.make_async_copy(dst, dst, sem).wait()

    def rows_of(p):
        return pl.ds(p * piece, piece)

    barrier = pltpu.get_barrier_semaphore()
    for dev in u_dev + v_dev + (partner,):
        pl.semaphore_signal(barrier, inc=1, device_id={"ep": dev}, device_id_type=MESH)

    routes = [pltpu.make_async_copy(src, dst, own_sem.at[i + 1])
              for i, (src, dst) in enumerate(((ids_hbm, ids_ref), (gat_hbm, gat_ref)))]
    for copy in routes:
        copy.start()
    own = pltpu.make_async_copy(tok_hbm, tok.at[0], own_sem.at[0])
    own.start()
    def tok_wait(g, k, p):
        filled(tok.at[k, rows_of(p)], tok_r.at[2 * k + p - 2])

    def block_wait(g, k):
        filled(tok.at[WHOLE[g, k]], tok_r.at[WHOLE[g, k] + 1])

    def send_u_own(order):
        for d in range(2):
            p = (d + order) % 2
            send(tok.at[0, rows_of(p)], tok.at[SIDE[d], rows_of(p)], tok_s, tok_r.at[2 * SIDE[d] + p - 2], u_dev[d])

    def whole_v(k, p):
        d = WAY[k]
        at = WHOLE[SIDE[d], k]
        send(tok.at[k, rows_of(p)], tok.at[at, rows_of(p)], tok_s, tok_r.at[at + 1], v_dev[d])

    slot_rows = lax.broadcasted_iota(jnp.int32, (block, tok_count), 0) + c * (local_count * cap)
    turned = jnp.where(slot_rows >= block, slot_rows - block, slot_rows)
    n_step = 512 if model_dim % 512 == 0 else model_dim

    def row_codes(chip_idx):
        return (turned + chip_idx * block).astype(F32)

    def pick(g, k, chip_idx, dst, first, es=(0, chip_experts)):
        codes = row_codes(chip_idx)[es[0] * cap:es[1] * cap]
        hit = jnp.zeros(codes.shape, F32)
        for j in range(top_count):
            hit = hit + (info[table_at(g, k, j), :] == codes).astype(F32)
        hit = hit.astype(BF16)
        for n in range(0, model_dim, n_step):
            x = jnp.dot(hit, tok[WHOLE[g, k], :, n:n + n_step], preferred_element_type=F32).astype(BF16)
            for e in range(*es):
                dst[e, first:first + cap, n:n + n_step] = x[(e - es[0]) * cap:(e - es[0] + 1) * cap]

    def group_rows(k):
        return pl.ds(k * cap, cap)

    def send_picked(g, k, chip_idx, at, ssem, to_g, to_k, dev):
        pick(g, k, chip_idx, stage.at[at], 0)
        return send(stage.at[at], xg.at[to_g, :, group_rows(to_k)], ssem, x_r.at[to_g], dev)

    def near_v(k):
        d = 1 - WAY[k]
        return send_picked(0, k, v_chip[d], (0, 2, 3)[k], far_s if k == 2 else near_s.at[k], SIDE[d], k, v_dev[d])

    def table_at(g, k, j, n=1):
        first = 16 * (4 * g + k) + j
        return slice(first, first + n)

    def table_ref(g, k, n):
        return info.at[pl.ds(16 * (4 * g + k), n)]

    def send_info(at, to, n, dev):
        send(table_ref(*at, n), table_ref(*to, n), inf_s, inf_r.at[TABLES.index(to)], dev)

    def inf_wait(g, k):
        filled(table_ref(g, k, 16 if k == 0 else 8), inf_r.at[TABLES.index((g, k))])

    own.wait()
    pl.semaphore_wait(barrier, 5)
    send_u_own(0)
    whole_v(0, 0)

    for copy in routes:
        copy.wait()
    expert = lax.broadcasted_iota(jnp.int32, (expert_count, tok_count), 0)
    hots = []
    chosen = jnp.zeros((expert_count, tok_count), F32)
    for j in range(top_count):
        hot = (ids_ref[j:j + 1, :] == expert).astype(F32)
        hots.append(hot)
        chosen = chosen + hot
    above = (lax.broadcasted_iota(jnp.int32, (tok_count, tok_count), 0)
             < lax.broadcasted_iota(jnp.int32, (tok_count, tok_count), 1)).astype(F32).astype(BF16)
    slot = jnp.dot(chosen.astype(BF16), above, preferred_element_type=F32)
    info[0:16] = jnp.zeros((16, tok_count), F32)
    for j in range(top_count):
        info[j:j + 1, :] = ids_ref[j:j + 1, :].astype(F32) * cap + jnp.sum(hots[j] * slot, axis=0, keepdims=True)
        info[8 + j:9 + j, :] = gat_ref[j:j + 1, :]

    for d in range(2):
        send_info((0, 0), (0, SIDE[d]), 8, u_dev[d])
        send_info((0, 0), (SIDE[d], 0), 16, v_dev[d])
    send_u_own(1)
    whole_v(0, 1)

    shared_loads = []
    for i in range(local_count):
        cols = pl.ds(i * ff, ff)
        for j, (src, dst) in enumerate(((sg_hbm.at[:, cols], w_g), (su_hbm.at[:, cols], w_u), (sd_hbm.at[cols], w_d))):
            copy = pltpu.make_async_copy(src, dst.at[i], load_sem.at[i, j])
            copy.start()
            shared_loads.append(copy)

    near_0 = near_v(0)

    for i in range(local_count):
        for j, (src, dst) in enumerate(((wg_hbm, w_g), (wu_hbm, w_u), (wd_hbm, w_d))):
            send(src.at[i], dst.at[local_count + i], wr_s.at[j], wr_r.at[j], partner)

    def silu_mul(g, up):
        return (jax.nn.silu(g) * up).astype(BF16)

    def shared_part(i):
        for copy in shared_loads[3 * i:3 * i + 3]:
            copy.wait()
        x = tok[0]
        h = silu_mul(jnp.dot(x, w_g[i], preferred_element_type=F32), jnp.dot(x, w_u[i], preferred_element_type=F32))
        for n in range(0, model_dim, n_step):
            y = jnp.dot(h, w_d[i, :, n:n + n_step], preferred_element_type=F32)
            if i > 0:
                y = y + acc[:, n:n + n_step]
            if i == local_count - 1:
                y = y.astype(BF16).astype(F32) + x[:, n:n + n_step].astype(F32)
            acc[:, n:n + n_step] = y

    own_loads = []

    def load_own(i):
        for j, (src, dst) in enumerate(((wg_hbm, w_g), (wu_hbm, w_u), (wd_hbm, w_d))):
            copy = pltpu.make_async_copy(src.at[i], dst.at[i], load_sem.at[i, j])
            copy.start()
            own_loads.append(copy)

    for i in range(local_count):
        shared_part(i)
        load_own(i)

    def e_half(d):
        return pl.ds(d * local_count, local_count)

    inf_wait(0, 1)
    send_info((0, 1), (1, 1), 8, v_dev[0])
    inf_wait(0, 2)
    send_info((0, 2), (2, 2), 8, v_dev[1])
    for k, p in ((1, 0), (2, 1), (1, 1), (2, 0)):
        tok_wait(0, k, p)
        whole_v(k, p)
    for d in range(2):
        pick(0, SIDE[d], u_chip[d], stage.at[1], 0, (d * local_count, (d + 1) * local_count))
        send(stage.at[1, e_half(d)], xg.at[0, e_half(d), group_rows(3)], near_s.at[2], x_r.at[0], u_dev[d])
    near_1 = near_v(1)
    near_v(2)
    block_wait(2, 0)
    inf_wait(2, 0)
    send_info((2, 0), (3, 0), 16, v_dev[1])
    send_picked(2, 0, v_chip[1], 4, far_s, 3, 0, v_dev[1])
    block_wait(1, 1)
    send(tok.at[WHOLE[1, 1]], tok.at[WHOLE[3, 1]], tok_s, tok_r.at[WHOLE[3, 1] + 1], v_dev[0])
    inf_wait(1, 1)
    send_info((1, 1), (3, 1), 8, v_dev[0])
    send_picked(1, 1, u_chip[0], 5, far_s, 1, 3, u_dev[0])

    def experts(g):
        def one(e, carry):
            x = xg[g, e]
            h = silu_mul(jnp.dot(x, w_g[e], preferred_element_type=F32), jnp.dot(x, w_u[e], preferred_element_type=F32))
            for n in range(0, model_dim, n_step):
                y = jnp.dot(h, w_d[e, :, n:n + n_step], preferred_element_type=F32).astype(BF16)
                raw[g, 0, e, :, n:n + n_step] = y[0:cap]
                xg[g, e, cap:4 * cap, n:n + n_step] = y[cap:4 * cap]
            return carry

        lax.fori_loop(0, chip_experts, one, 0)

    def own_pick(g, ks):
        for k in ks:
            pick(g, k, chip, xg.at[g], k * cap)

    def x_wait(g, ks):
        filled(xg.at[g, pl.ds(0, len(ks) * chip_experts // 4)], x_r.at[g])

    def col_chunk(f):
        return slice(None) if f is None else pl.ds(f * width, width)

    def send_rows(g, f=None):
        at = col_chunk(f)
        i = f or 0
        for d in range(2):
            send(xg.at[g, e_half(d), group_rows(3), at], relay.at[g, d, :, :, at], f_s, rel_r.at[g + i], u_dev[d])
        for d in range(2):
            send(xg.at[g, :, group_rows(2 - d), at], raw.at[g, SIDE[d], :, :, at], f_s, raw_r.at[g + i], u_dev[d])

    def pass_rows(g, f=None):
        at = col_chunk(f)
        i = f or 0
        filled(relay.at[g, :, :, :, at], rel_r.at[g + i])
        for d in range(2):
            send(relay.at[g, d, :, :, at], raw.at[g, 3, e_half(d), :, at], rel_s, raw_r.at[g + i], u_dev[d])

    def raw_wait(g, f=None):
        at = col_chunk(f)
        i = f or 0
        filled(raw.at[g, pl.ds(1, 3), :, :, at], raw_r.at[g + i])

    def gates_of(g):
        for m in range(4):
            codes = row_codes(chip_at(u + OFFSETS[m], v))
            gate = jnp.zeros((block, tok_count), F32)
            for j in range(top_count):
                gate = gate + jnp.where(info[table_at(g, 0, j), :] == codes, info[table_at(g, 0, 8 + j), :], 0.0)
            gate = gate.T
            for s in range(3):
                part_s = gate.astype(BF16)
                gsplit[s * tok_count:(s + 1) * tok_count, m * block:(m + 1) * block] = part_s
                gate = gate - part_s.astype(F32)

    step = 256 if width % 256 == 0 else width

    def gated(g, f=None):
        first, count = (0, model_dim // step) if f is None else (f * (width // step), width // step)

        def cols(n, carry):
            at = pl.ds(pl.multiple_of(n * step, 128), step)
            rows = raw[g, :, :, :, at].reshape(4 * block, step)
            y = jnp.dot(gsplit[...], rows, preferred_element_type=F32)
            y = y[0:tok_count] + y[tok_count:2 * tok_count] + y[2 * tok_count:3 * tok_count]
            if g == 0:
                acc[:, at] = acc[:, at] + y
            else:
                part[g - 1, :, at] = y
            return carry

        lax.fori_loop(first, first + count, cols, 0)

    def send_early(g, d):
        send(part.at[g - 1, rows_of(1 - d)], fin.at[d], fin_s, fin_r.at[0], v_dev[d])

    def send_last(g, d, f):
        at = col_chunk(f)
        send(part.at[g - 1, rows_of(d), at], last.at[rows_of(d), at], fin_s, fin_r.at[1], v_dev[d])

    own_pick(0, (0, 1, 2))
    for copy in own_loads:
        copy.wait()
    for j, dst in enumerate((w_g, w_u, w_d)):
        filled(dst.at[pl.ds(local_count, local_count)], wr_r.at[j])
    x_wait(0, (3,))
    experts(0)
    block_wait(2, 2)
    inf_wait(2, 2)
    near_0.wait_send()
    send_picked(2, 2, v_chip[1], 0, far_s, 3, 2, v_dev[1])
    filled(stage.at[1], near_s.at[2])
    send_picked(2, 2, u_chip[1], 1, far_s, 2, 3, u_dev[1])
    send_rows(0)
    own_pick(1, (1,))
    x_wait(1, (0, 2, 3))
    experts(1)
    block_wait(3, 1)
    inf_wait(3, 1)
    near_1.wait_send()
    send_picked(3, 1, u_chip[0], 2, far_s, 3, 3, u_dev[0])
    pass_rows(0)
    send_rows(1)
    own_pick(2, (0, 2))
    own_pick(3, (1,))
    pass_rows(1)
    x_wait(2, (1, 3))
    experts(2)
    send_rows(2)
    raw_wait(0)
    gates_of(0)
    gated(0)
    x_wait(3, (0, 2, 3))
    experts(3)
    pass_rows(2)
    for f in range(chunks):
        send_rows(3, f)
    raw_wait(1)
    inf_wait(1, 0)
    gates_of(1)
    gated(1)
    inf_wait(3, 0)
    raw_wait(2)
    gates_of(2)
    pass_rows(3, 0)
    gated(2)
    send_early(1, 1)
    send_early(2, 0)
    for f in range(1, chunks):
        pass_rows(3, f)
    gates_of(3)
    for f in range(chunks):
        raw_wait(3, f)
        gated(3, f)
        for d in range(2):
            send(part.at[2, rows_of(d), col_chunk(f)], half.at[d, :, col_chunk(f)], half_s, half_r.at[f], v_dev[d])
    for f in range(chunks):
        at = slice(f * width, (f + 1) * width)
        filled(half.at[:, :, col_chunk(f)], half_r.at[f])
        for d in range(2):
            g = 2 - d
            rows = slice(d * piece, (d + 1) * piece)
            part[g - 1, rows, at] = part[g - 1, rows, at] + half[d, :, at]
            send_last(g, d, f)

    filled(fin, fin_r.at[0])
    for d in range(2):
        rows = slice((1 - d) * piece, (2 - d) * piece)
        acc[rows] = acc[rows] + fin[d]

    filled(tok.at[pl.ds(0, 6)], tok_s)
    filled(stage, far_s)
    filled(info.at[pl.ds(0, 5 * 8 + 3 * 16)], inf_s)
    for j, dst in enumerate((w_g, w_u, w_d)):
        filled(dst.at[pl.ds(0, local_count)], wr_s.at[j])
    filled(raw.at[pl.ds(0, 3)], f_s)
    filled(relay, rel_s)
    filled(half, half_s)
    filled(part.at[pl.ds(0, 2)], fin_s)
    filled(last, fin_r.at[1])


def solution(mesh):
    group_size = mesh.shape["ep"]
    side = math.isqrt(group_size // 2)

    def moe_step(tokens, expert_ids, gate_vals, w_gate, w_up, w_down, shared_gate, shared_up, shared_down):
        tok_count, model_dim = tokens.shape
        top_count = expert_ids.shape[1]
        local_count, _, ff = w_gate.shape
        expert_count = local_count * group_size
        spread = max(group_size, expert_count // 2)
        cap = (tok_count * top_count + spread - 1) // spread
        block = 2 * local_count * cap
        piece = tok_count // 2
        dma = pltpu.SemaphoreType.DMA
        hbm = pl.BlockSpec(memory_space=pl.ANY)
        scratch = [
            pltpu.VMEM((top_count, tok_count), jnp.int32),
            pltpu.VMEM((top_count, tok_count), F32),
            pltpu.VMEM((2 * local_count, model_dim, ff), BF16),
            pltpu.VMEM((2 * local_count, model_dim, ff), BF16),
            pltpu.VMEM((2 * local_count, ff, model_dim), BF16),
            pltpu.VMEM((len(WHOLE), tok_count, model_dim), BF16),
            pltpu.VMEM((16 * 16, tok_count), F32),
            pltpu.VMEM((4, 2 * local_count, 4 * cap, model_dim), BF16),
            pltpu.VMEM((6, 2 * local_count, cap, model_dim), BF16),
            pltpu.VMEM((4, 4, 2 * local_count, cap, model_dim), BF16),
            pltpu.VMEM((4, 2, local_count, cap, model_dim), BF16),
            pltpu.VMEM((3 * tok_count, 4 * block), BF16),
            pltpu.VMEM((3, tok_count, model_dim), F32),
            pltpu.VMEM((2, piece, model_dim), F32),
            pltpu.VMEM((2, piece, model_dim), F32),
            dma((3,)), dma((local_count, 3)), dma((len(WHOLE) + 1,)), dma((len(TABLES),)), dma((4,)), dma((5,)), dma((5,)),
            dma((2,)), dma((2,)), dma((3,)),
            dma(()), dma((3,)), dma(()), dma(()), dma(()), dma(()), dma(()), dma(()), dma((3,)),
        ]
        total = pltpu.VMEM(tokens.shape, F32)
        base, last = pl.pallas_call(
            functools.partial(kernel, side, cap),
            out_shape=(total, total),
            in_specs=[hbm] * 9,
            out_specs=(pl.BlockSpec(memory_space=pltpu.VMEM),) * 2,
            scratch_shapes=scratch,
            compiler_params=pltpu.CompilerParams(collective_id=0, has_side_effects=True, vmem_limit_bytes=63 * 1024 * 1024 - 3200 * 1024),
        )(expert_ids.T, gate_vals.T, tokens, w_gate, w_up, w_down, shared_gate, shared_up, shared_down)
        return (base + last).astype(tokens.dtype)

    row_spec = P(("dp", "ep"), None)
    expert_spec = P("ep", None, None)
    whole_spec = P(None, None)
    return jax.shard_map(moe_step, mesh=mesh, in_specs=(row_spec, row_spec, row_spec, expert_spec, expert_spec, expert_spec, whole_spec, whole_spec, whole_spec), out_specs=row_spec, check_vma=False)
```

```python
import functools
import math

import jax
import jax.numpy as jnp
from jax import lax
from jax.experimental import pallas as pl
from jax.experimental.pallas import tpu as pltpu
from jax.sharding import PartitionSpec as P

F32 = jnp.float32
BF16 = jnp.bfloat16
MESH = pl.DeviceIdType.MESH


OFFSETS = (0, -1, 1, 2)
SIDE = (1, 2)

WHOLE = {(0, 0): 0, (0, 1): 1, (0, 2): 2, (1, 1): 3, (2, 2): 4, (3, 1): 5}
WAY = (1, 0, 1)
TABLES = ((0, 1), (0, 2), (1, 0), (1, 1), (2, 0), (2, 2), (3, 0), (3, 1))


def kernel(side, cap, ids_hbm, gat_hbm, tok_hbm, wg_hbm, wu_hbm, wd_hbm, sg_hbm, su_hbm, sd_hbm, acc, last,
           ids_ref, gat_ref, w_g, w_u, w_d, tok, info, xg, stage, raw, relay, gsplit, part, half, fin,
           own_sem, load_sem, tok_r, inf_r, x_r, raw_r, rel_r, half_r, fin_r, wr_r,
           tok_s, near_s, far_s, inf_s, f_s, rel_s, half_s, fin_s, wr_s):
    tok_count, model_dim = tok_hbm.shape
    top_count = ids_hbm.shape[0]
    local_count, _, ff = wg_hbm.shape
    chip_experts = 2 * local_count
    expert_count = local_count * side * side * 2
    block = chip_experts * cap
    piece = tok_count // 2
    chunks = 2
    width = model_dim // chunks

    me = lax.axis_index("ep")
    c = me % 2
    chip = me // 2
    cx, cy = chip % side, chip // side
    u = (1 - c) * cx + c * cy
    v = (1 - c) * cy + c * cx

    def chip_at(uu, vv):
        uu, vv = (uu + side) % side, (vv + side) % side
        return (1 - c) * (vv * side + uu) + c * (uu * side + vv)

    def dev_at(uu, vv):
        return chip_at(uu, vv) * 2 + c

    u_dev = (dev_at(u + 1, v), dev_at(u - 1, v))
    v_dev = (dev_at(u, v + 1), dev_at(u, v - 1))
    u_chip = (chip_at(u + 1, v), chip_at(u - 1, v))
    v_chip = (chip_at(u, v + 1), chip_at(u, v - 1))
    partner = chip * 2 + (1 - c)

    def send(src, dst, ssem, rsem, dev):
        copy = pltpu.make_async_remote_copy(src_ref=src, dst_ref=dst, send_sem=ssem, recv_sem=rsem,
                                            device_id={"ep": dev}, device_id_type=MESH)
        copy.start()
        return copy

    def filled(dst, sem):
        pltpu.make_async_copy(dst, dst, sem).wait()

    def rows_of(p):
        return pl.ds(p * piece, piece)

    barrier = pltpu.get_barrier_semaphore()
    for dev in u_dev + v_dev + (partner,):
        pl.semaphore_signal(barrier, inc=1, device_id={"ep": dev}, device_id_type=MESH)

    routes = [pltpu.make_async_copy(src, dst, own_sem.at[i + 1])
              for i, (src, dst) in enumerate(((ids_hbm, ids_ref), (gat_hbm, gat_ref)))]
    for copy in routes:
        copy.start()
    own = pltpu.make_async_copy(tok_hbm, tok.at[0], own_sem.at[0])
    own.start()
    def tok_wait(g, k, p):
        filled(tok.at[k, rows_of(p)], tok_r.at[2 * k + p - 2])

    def block_wait(g, k):
        filled(tok.at[WHOLE[g, k]], tok_r.at[WHOLE[g, k] + 1])

    def send_u_own(order):
        for d in range(2):
            p = (d + order) % 2
            send(tok.at[0, rows_of(p)], tok.at[SIDE[d], rows_of(p)], tok_s, tok_r.at[2 * SIDE[d] + p - 2], u_dev[d])

    def whole_v(k, p):
        d = WAY[k]
        at = WHOLE[SIDE[d], k]
        send(tok.at[k, rows_of(p)], tok.at[at, rows_of(p)], tok_s, tok_r.at[at + 1], v_dev[d])

    slot_rows = lax.broadcasted_iota(jnp.int32, (block, tok_count), 0) + c * (local_count * cap)
    turned = jnp.where(slot_rows >= block, slot_rows - block, slot_rows)
    n_step = 512 if model_dim % 512 == 0 else model_dim

    def row_codes(chip_idx):
        return (turned + chip_idx * block).astype(F32)

    def pick(g, k, chip_idx, dst, first, es=(0, chip_experts)):
        codes = row_codes(chip_idx)[es[0] * cap:es[1] * cap]
        hit = jnp.zeros(codes.shape, F32)
        for j in range(top_count):
            hit = hit + (info[table_at(g, k, j), :] == codes).astype(F32)
        hit = hit.astype(BF16)
        for n in range(0, model_dim, n_step):
            x = jnp.dot(hit, tok[WHOLE[g, k], :, n:n + n_step], preferred_element_type=F32).astype(BF16)
            for e in range(*es):
                dst[e, first:first + cap, n:n + n_step] = x[(e - es[0]) * cap:(e - es[0] + 1) * cap]

    def group_rows(k):
        return pl.ds(k * cap, cap)

    def send_picked(g, k, chip_idx, at, ssem, to_g, to_k, dev):
        pick(g, k, chip_idx, stage.at[at], 0)
        return send(stage.at[at], xg.at[to_g, :, group_rows(to_k)], ssem, x_r.at[to_g], dev)

    def near_v(k):
        d = 1 - WAY[k]
        return send_picked(0, k, v_chip[d], (0, 2, 3)[k], far_s if k == 2 else near_s.at[k], SIDE[d], k, v_dev[d])

    def table_at(g, k, j, n=1):
        first = 16 * (4 * g + k) + j
        return slice(first, first + n)

    def table_ref(g, k, n):
        return info.at[pl.ds(16 * (4 * g + k), n)]

    def send_info(at, to, n, dev):
        send(table_ref(*at, n), table_ref(*to, n), inf_s, inf_r.at[TABLES.index(to)], dev)

    def inf_wait(g, k):
        filled(table_ref(g, k, 16 if k == 0 else 8), inf_r.at[TABLES.index((g, k))])

    own.wait()
    pl.semaphore_wait(barrier, 5)
    send_u_own(0)

    for copy in routes:
        copy.wait()
    expert = lax.broadcasted_iota(jnp.int32, (expert_count, tok_count), 0)
    hots = []
    chosen = jnp.zeros((expert_count, tok_count), F32)
    for j in range(top_count):
        hot = (ids_ref[j:j + 1, :] == expert).astype(F32)
        hots.append(hot)
        chosen = chosen + hot
    above = (lax.broadcasted_iota(jnp.int32, (tok_count, tok_count), 0)
             < lax.broadcasted_iota(jnp.int32, (tok_count, tok_count), 1)).astype(F32).astype(BF16)
    slot = jnp.dot(chosen.astype(BF16), above, preferred_element_type=F32)
    info[0:16] = jnp.zeros((16, tok_count), F32)
    for j in range(top_count):
        info[j:j + 1, :] = ids_ref[j:j + 1, :].astype(F32) * cap + jnp.sum(hots[j] * slot, axis=0, keepdims=True)
        info[8 + j:9 + j, :] = gat_ref[j:j + 1, :]

    for d in range(2):
        send_info((0, 0), (0, SIDE[d]), 8, u_dev[d])
        send_info((0, 0), (SIDE[d], 0), 16, v_dev[d])
    send_u_own(1)

    shared_loads = []
    for i in range(local_count):
        cols = pl.ds(i * ff, ff)
        for j, (src, dst) in enumerate(((sg_hbm.at[:, cols], w_g), (su_hbm.at[:, cols], w_u), (sd_hbm.at[cols], w_d))):
            copy = pltpu.make_async_copy(src, dst.at[i], load_sem.at[i, j])
            copy.start()
            shared_loads.append(copy)

    near_0 = near_v(0)
    near_down = send_picked(0, 0, v_chip[1], 4, near_s.at[3], SIDE[1], 0, v_dev[1])

    for i in range(local_count):
        for j, (src, dst) in enumerate(((wg_hbm, w_g), (wu_hbm, w_u), (wd_hbm, w_d))):
            send(src.at[i], dst.at[local_count + i], wr_s.at[j], wr_r.at[j], partner)

    def silu_mul(g, up):
        return (jax.nn.silu(g) * up).astype(BF16)

    def shared_part(i):
        for copy in shared_loads[3 * i:3 * i + 3]:
            copy.wait()
        x = tok[0]
        h = silu_mul(jnp.dot(x, w_g[i], preferred_element_type=F32), jnp.dot(x, w_u[i], preferred_element_type=F32))
        for n in range(0, model_dim, n_step):
            y = jnp.dot(h, w_d[i, :, n:n + n_step], preferred_element_type=F32)
            if i > 0:
                y = y + acc[:, n:n + n_step]
            if i == local_count - 1:
                y = y.astype(BF16).astype(F32) + x[:, n:n + n_step].astype(F32)
            acc[:, n:n + n_step] = y

    own_loads = []

    def load_own(i):
        for j, (src, dst) in enumerate(((wg_hbm, w_g), (wu_hbm, w_u), (wd_hbm, w_d))):
            copy = pltpu.make_async_copy(src.at[i], dst.at[i], load_sem.at[i, j])
            copy.start()
            own_loads.append(copy)

    for i in range(local_count):
        shared_part(i)
        load_own(i)

    def e_half(d):
        return pl.ds(d * local_count, local_count)

    inf_wait(0, 1)
    send_info((0, 1), (1, 1), 8, v_dev[0])
    inf_wait(0, 2)
    send_info((0, 2), (2, 2), 8, v_dev[1])
    for k, p in ((1, 0), (2, 1), (1, 1), (2, 0)):
        tok_wait(0, k, p)
        whole_v(k, p)
    for d in range(2):
        first, count = ((0, chip_experts // 4), (chip_experts // 4, chip_experts - chip_experts // 4))[d]
        es = pl.ds(first, count)
        pick(0, SIDE[d], u_chip[d], stage.at[1], 0, (first, first + count))
        send(stage.at[1, es], xg.at[0, es, group_rows(3)], near_s.at[2], x_r.at[0], u_dev[d])
    near_1 = near_v(1)
    near_v(2)
    inf_wait(2, 0)
    send_info((2, 0), (3, 0), 16, v_dev[1])
    block_wait(1, 1)
    send(tok.at[WHOLE[1, 1]], tok.at[WHOLE[3, 1]], tok_s, tok_r.at[WHOLE[3, 1] + 1], v_dev[0])
    inf_wait(1, 1)
    send_info((1, 1), (3, 1), 8, v_dev[0])
    send_picked(1, 1, u_chip[0], 5, far_s, 1, 3, u_dev[0])

    def experts(g):
        def one(e, carry):
            x = xg[g, e]
            h = silu_mul(jnp.dot(x, w_g[e], preferred_element_type=F32), jnp.dot(x, w_u[e], preferred_element_type=F32))
            for n in range(0, model_dim, n_step):
                y = jnp.dot(h, w_d[e, :, n:n + n_step], preferred_element_type=F32).astype(BF16)
                raw[g, 0, e, :, n:n + n_step] = y[0:cap]
                xg[g, e, cap:4 * cap, n:n + n_step] = y[cap:4 * cap]
            return carry

        lax.fori_loop(0, chip_experts, one, 0)

    def own_pick(g, ks):
        for k in ks:
            pick(g, k, chip, xg.at[g], k * cap)

    def x_wait(g, ks):
        filled(xg.at[g, pl.ds(0, len(ks) * chip_experts // 4)], x_r.at[g])

    def col_chunk(f):
        return slice(None) if f is None else pl.ds(f * width, width)

    def send_rows(g, f=None):
        at = col_chunk(f)
        i = f or 0
        for d in range(2):
            send(xg.at[g, e_half(d), group_rows(3), at], relay.at[g, d, :, :, at], f_s, rel_r.at[g + i], u_dev[d])
        for d in range(2):
            send(xg.at[g, :, group_rows(2 - d), at], raw.at[g, SIDE[d], :, :, at], f_s, raw_r.at[g + i], u_dev[d])

    def pass_rows(g, f=None):
        at = col_chunk(f)
        i = f or 0
        filled(relay.at[g, :, :, :, at], rel_r.at[g + i])
        for d in range(2):
            send(relay.at[g, d, :, :, at], raw.at[g, 3, e_half(d), :, at], rel_s, raw_r.at[g + i], u_dev[d])

    def raw_wait(g, f=None):
        at = col_chunk(f)
        i = f or 0
        filled(raw.at[g, pl.ds(1, 3), :, :, at], raw_r.at[g + i])

    def gates_of(g):
        for m in range(4):
            codes = row_codes(chip_at(u + OFFSETS[m], v))
            gate = jnp.zeros((block, tok_count), F32)
            for j in range(top_count):
                gate = gate + jnp.where(info[table_at(g, 0, j), :] == codes, info[table_at(g, 0, 8 + j), :], 0.0)
            gate = gate.T
            for s in range(3):
                part_s = gate.astype(BF16)
                gsplit[s * tok_count:(s + 1) * tok_count, m * block:(m + 1) * block] = part_s
                gate = gate - part_s.astype(F32)

    step = 256 if width % 256 == 0 else width

    def gated(g, f=None):
        first, count = (0, model_dim // step) if f is None else (f * (width // step), width // step)

        def cols(n, carry):
            at = pl.ds(pl.multiple_of(n * step, 128), step)
            rows = raw[g, :, :, :, at].reshape(4 * block, step)
            y = jnp.dot(gsplit[...], rows, preferred_element_type=F32)
            y = y[0:tok_count] + y[tok_count:2 * tok_count] + y[2 * tok_count:3 * tok_count]
            if g == 0:
                acc[:, at] = acc[:, at] + y
            else:
                part[g - 1, :, at] = y
            return carry

        lax.fori_loop(first, first + count, cols, 0)

    def send_early(g, d):
        send(part.at[g - 1, rows_of(1 - d)], fin.at[d], fin_s, fin_r.at[0], v_dev[d])

    def send_last(g, d, f):
        at = col_chunk(f)
        send(part.at[g - 1, rows_of(d), at], last.at[rows_of(d), at], fin_s, fin_r.at[1], v_dev[d])

    own_pick(0, (0, 1, 2))
    for copy in own_loads:
        copy.wait()
    for j, dst in enumerate((w_g, w_u, w_d)):
        filled(dst.at[pl.ds(local_count, local_count)], wr_r.at[j])
    x_wait(0, (3,))
    experts(0)
    block_wait(2, 2)
    inf_wait(2, 2)
    near_0.wait_send()
    send_picked(2, 2, v_chip[1], 0, far_s, 3, 2, v_dev[1])
    filled(stage.at[1], near_s.at[2])
    send_picked(2, 2, u_chip[1], 1, far_s, 2, 3, u_dev[1])
    send_rows(0)
    own_pick(1, (1,))
    x_wait(1, (0, 2, 3))
    experts(1)
    block_wait(3, 1)
    inf_wait(3, 1)
    near_1.wait_send()
    send_picked(3, 1, u_chip[0], 2, far_s, 3, 3, u_dev[0])
    near_down.wait_send()
    send_picked(3, 1, u_chip[1], 4, far_s, 3, 0, u_dev[1])
    pass_rows(0)
    send_rows(1)
    own_pick(2, (2,))
    own_pick(3, (1,))
    pass_rows(1)
    x_wait(2, (0, 1, 3))
    experts(2)
    send_rows(2)
    raw_wait(0)
    gates_of(0)
    gated(0)
    x_wait(3, (0, 2, 3))
    experts(3)
    pass_rows(2)
    for f in range(chunks):
        send_rows(3, f)
    raw_wait(1)
    inf_wait(1, 0)
    gates_of(1)
    gated(1)
    inf_wait(3, 0)
    raw_wait(2)
    gates_of(2)
    pass_rows(3, 0)
    gated(2)
    send_early(1, 1)
    send_early(2, 0)
    for f in range(1, chunks):
        pass_rows(3, f)
    gates_of(3)
    for f in range(chunks):
        raw_wait(3, f)
        gated(3, f)
        for d in range(2):
            send(part.at[2, rows_of(d), col_chunk(f)], half.at[d, :, col_chunk(f)], half_s, half_r.at[f], v_dev[d])
    for f in range(chunks):
        at = slice(f * width, (f + 1) * width)
        filled(half.at[:, :, col_chunk(f)], half_r.at[f])
        for d in range(2):
            g = 2 - d
            rows = slice(d * piece, (d + 1) * piece)
            part[g - 1, rows, at] = part[g - 1, rows, at] + half[d, :, at]
            send_last(g, d, f)

    filled(fin, fin_r.at[0])
    for d in range(2):
        rows = slice((1 - d) * piece, (2 - d) * piece)
        acc[rows] = acc[rows] + fin[d]

    filled(tok.at[pl.ds(0, 5)], tok_s)
    filled(stage, far_s)
    filled(info.at[pl.ds(0, 5 * 8 + 3 * 16)], inf_s)
    for j, dst in enumerate((w_g, w_u, w_d)):
        filled(dst.at[pl.ds(0, local_count)], wr_s.at[j])
    filled(raw.at[pl.ds(0, 3)], f_s)
    filled(relay, rel_s)
    filled(half, half_s)
    filled(part.at[pl.ds(0, 2)], fin_s)
    filled(last, fin_r.at[1])


def solution(mesh):
    group_size = mesh.shape["ep"]
    side = math.isqrt(group_size // 2)

    def moe_step(tokens, expert_ids, gate_vals, w_gate, w_up, w_down, shared_gate, shared_up, shared_down):
        tok_count, model_dim = tokens.shape
        top_count = expert_ids.shape[1]
        local_count, _, ff = w_gate.shape
        expert_count = local_count * group_size
        spread = max(group_size, expert_count // 2)
        cap = (tok_count * top_count + spread - 1) // spread
        block = 2 * local_count * cap
        piece = tok_count // 2
        dma = pltpu.SemaphoreType.DMA
        hbm = pl.BlockSpec(memory_space=pl.ANY)
        scratch = [
            pltpu.VMEM((top_count, tok_count), jnp.int32),
            pltpu.VMEM((top_count, tok_count), F32),
            pltpu.VMEM((2 * local_count, model_dim, ff), BF16),
            pltpu.VMEM((2 * local_count, model_dim, ff), BF16),
            pltpu.VMEM((2 * local_count, ff, model_dim), BF16),
            pltpu.VMEM((len(WHOLE), tok_count, model_dim), BF16),
            pltpu.VMEM((16 * 16, tok_count), F32),
            pltpu.VMEM((4, 2 * local_count, 4 * cap, model_dim), BF16),
            pltpu.VMEM((6, 2 * local_count, cap, model_dim), BF16),
            pltpu.VMEM((4, 4, 2 * local_count, cap, model_dim), BF16),
            pltpu.VMEM((4, 2, local_count, cap, model_dim), BF16),
            pltpu.VMEM((3 * tok_count, 4 * block), BF16),
            pltpu.VMEM((3, tok_count, model_dim), F32),
            pltpu.VMEM((2, piece, model_dim), F32),
            pltpu.VMEM((2, piece, model_dim), F32),
            dma((3,)), dma((local_count, 3)), dma((len(WHOLE) + 1,)), dma((len(TABLES),)), dma((4,)), dma((5,)), dma((5,)),
            dma((2,)), dma((2,)), dma((3,)),
            dma(()), dma((4,)), dma(()), dma(()), dma(()), dma(()), dma(()), dma(()), dma((3,)),
        ]
        total = pltpu.VMEM(tokens.shape, F32)
        base, last = pl.pallas_call(
            functools.partial(kernel, side, cap),
            out_shape=(total, total),
            in_specs=[hbm] * 9,
            out_specs=(pl.BlockSpec(memory_space=pltpu.VMEM),) * 2,
            scratch_shapes=scratch,
            compiler_params=pltpu.CompilerParams(collective_id=0, has_side_effects=True, vmem_limit_bytes=63 * 1024 * 1024 - 3200 * 1024),
        )(expert_ids.T, gate_vals.T, tokens, w_gate, w_up, w_down, shared_gate, shared_up, shared_down)
        return (base + last).astype(tokens.dtype)

    row_spec = P(("dp", "ep"), None)
    expert_spec = P("ep", None, None)
    whole_spec = P(None, None)
    return jax.shard_map(moe_step, mesh=mesh, in_specs=(row_spec, row_spec, row_spec, expert_spec, expert_spec, expert_spec, whole_spec, whole_spec, whole_spec), out_specs=row_spec, check_vma=False)
```

```python
import functools
import math

import jax
import jax.numpy as jnp
from jax import lax
from jax.experimental import pallas as pl
from jax.experimental.pallas import tpu as pltpu
from jax.sharding import PartitionSpec as P

F32 = jnp.float32
BF16 = jnp.bfloat16
MESH = pl.DeviceIdType.MESH


OFFSETS = (0, -1, 1, 2)
SIDE = (1, 2)

WHOLE = {(0, 0): 0, (0, 1): 1, (0, 2): 2, (1, 1): 3, (2, 2): 4, (3, 1): 5}
WAY = (1, 0, 1)
TABLES = ((0, 1), (0, 2), (1, 0), (1, 1), (2, 0), (2, 2), (3, 0), (3, 1))


def kernel(side, cap, ids_hbm, gat_hbm, tok_hbm, wg_hbm, wu_hbm, wd_hbm, sg_hbm, su_hbm, sd_hbm, acc, last,
           ids_ref, gat_ref, w_g, w_u, w_d, tok, info, xg, stage, raw, relay, gsplit, part, half, fin,
           own_sem, load_sem, tok_r, inf_r, x_r, raw_r, rel_r, half_r, fin_r, wr_r,
           tok_s, near_s, far_s, inf_s, f_s, rel_s, half_s, fin_s, wr_s):
    tok_count, model_dim = tok_hbm.shape
    top_count = ids_hbm.shape[0]
    local_count, _, ff = wg_hbm.shape
    chip_experts = 2 * local_count
    expert_count = local_count * side * side * 2
    block = chip_experts * cap
    piece = tok_count // 2
    chunks = 3
    width = model_dim // chunks

    me = lax.axis_index("ep")
    c = me % 2
    chip = me // 2
    cx, cy = chip % side, chip // side
    u = (1 - c) * cx + c * cy
    v = (1 - c) * cy + c * cx

    def chip_at(uu, vv):
        uu, vv = (uu + side) % side, (vv + side) % side
        return (1 - c) * (vv * side + uu) + c * (uu * side + vv)

    def dev_at(uu, vv):
        return chip_at(uu, vv) * 2 + c

    u_dev = (dev_at(u + 1, v), dev_at(u - 1, v))
    v_dev = (dev_at(u, v + 1), dev_at(u, v - 1))
    u_chip = (chip_at(u + 1, v), chip_at(u - 1, v))
    v_chip = (chip_at(u, v + 1), chip_at(u, v - 1))
    partner = chip * 2 + (1 - c)

    def send(src, dst, ssem, rsem, dev):
        copy = pltpu.make_async_remote_copy(src_ref=src, dst_ref=dst, send_sem=ssem, recv_sem=rsem,
                                            device_id={"ep": dev}, device_id_type=MESH)
        copy.start()
        return copy

    def filled(dst, sem):
        pltpu.make_async_copy(dst, dst, sem).wait()

    def rows_of(p):
        return pl.ds(p * piece, piece)

    barrier = pltpu.get_barrier_semaphore()
    for dev in u_dev + v_dev + (partner,):
        pl.semaphore_signal(barrier, inc=1, device_id={"ep": dev}, device_id_type=MESH)

    routes = [pltpu.make_async_copy(src, dst, own_sem.at[i + 1])
              for i, (src, dst) in enumerate(((ids_hbm, ids_ref), (gat_hbm, gat_ref)))]
    for copy in routes:
        copy.start()
    own = pltpu.make_async_copy(tok_hbm, tok.at[0], own_sem.at[0])
    own.start()
    def tok_wait(g, k, p):
        filled(tok.at[k, rows_of(p)], tok_r.at[2 * k + p - 2])

    def block_wait(g, k):
        filled(tok.at[WHOLE[g, k]], tok_r.at[WHOLE[g, k] + 1])

    def send_u_own(order):
        for d in range(2):
            p = (d + order) % 2
            send(tok.at[0, rows_of(p)], tok.at[SIDE[d], rows_of(p)], tok_s, tok_r.at[2 * SIDE[d] + p - 2], u_dev[d])

    def whole_v(k, p):
        d = WAY[k]
        at = WHOLE[SIDE[d], k]
        send(tok.at[k, rows_of(p)], tok.at[at, rows_of(p)], tok_s, tok_r.at[at + 1], v_dev[d])

    slot_rows = lax.broadcasted_iota(jnp.int32, (block, tok_count), 0) + c * (local_count * cap)
    turned = jnp.where(slot_rows >= block, slot_rows - block, slot_rows)
    n_step = 512 if model_dim % 512 == 0 else model_dim

    def row_codes(chip_idx):
        return (turned + chip_idx * block).astype(F32)

    def pick(g, k, chip_idx, dst, first, es=(0, chip_experts)):
        codes = row_codes(chip_idx)[es[0] * cap:es[1] * cap]
        hit = jnp.zeros(codes.shape, F32)
        for j in range(top_count):
            hit = hit + (info[table_at(g, k, j), :] == codes).astype(F32)
        hit = hit.astype(BF16)
        for n in range(0, model_dim, n_step):
            x = jnp.dot(hit, tok[WHOLE[g, k], :, n:n + n_step], preferred_element_type=F32).astype(BF16)
            for e in range(*es):
                dst[e, first:first + cap, n:n + n_step] = x[(e - es[0]) * cap:(e - es[0] + 1) * cap]

    def group_rows(k):
        return pl.ds(k * cap, cap)

    def send_picked(g, k, chip_idx, at, ssem, to_g, to_k, dev):
        pick(g, k, chip_idx, stage.at[at], 0)
        return send(stage.at[at], xg.at[to_g, :, group_rows(to_k)], ssem, x_r.at[to_g], dev)

    def near_v(k):
        d = 1 - WAY[k]
        return send_picked(0, k, v_chip[d], (0, 2, 3)[k], far_s if k == 2 else near_s.at[k], SIDE[d], k, v_dev[d])

    def table_at(g, k, j, n=1):
        first = 16 * (4 * g + k) + j
        return slice(first, first + n)

    def table_ref(g, k, n):
        return info.at[pl.ds(16 * (4 * g + k), n)]

    def send_info(at, to, n, dev):
        send(table_ref(*at, n), table_ref(*to, n), inf_s, inf_r.at[TABLES.index(to)], dev)

    def inf_wait(g, k):
        filled(table_ref(g, k, 16 if k == 0 else 8), inf_r.at[TABLES.index((g, k))])

    own.wait()
    pl.semaphore_wait(barrier, 5)
    send_u_own(0)

    for copy in routes:
        copy.wait()
    expert = lax.broadcasted_iota(jnp.int32, (expert_count, tok_count), 0)
    hots = []
    chosen = jnp.zeros((expert_count, tok_count), F32)
    for j in range(top_count):
        hot = (ids_ref[j:j + 1, :] == expert).astype(F32)
        hots.append(hot)
        chosen = chosen + hot
    above = (lax.broadcasted_iota(jnp.int32, (tok_count, tok_count), 0)
             < lax.broadcasted_iota(jnp.int32, (tok_count, tok_count), 1)).astype(F32).astype(BF16)
    slot = jnp.dot(chosen.astype(BF16), above, preferred_element_type=F32)
    info[0:16] = jnp.zeros((16, tok_count), F32)
    for j in range(top_count):
        info[j:j + 1, :] = ids_ref[j:j + 1, :].astype(F32) * cap + jnp.sum(hots[j] * slot, axis=0, keepdims=True)
        info[8 + j:9 + j, :] = gat_ref[j:j + 1, :]

    for d in range(2):
        send_info((0, 0), (0, SIDE[d]), 8, u_dev[d])
        send_info((0, 0), (SIDE[d], 0), 16, v_dev[d])
    send_u_own(1)

    shared_loads = []
    for i in range(local_count):
        cols = pl.ds(i * ff, ff)
        for j, (src, dst) in enumerate(((sg_hbm.at[:, cols], w_g), (su_hbm.at[:, cols], w_u), (sd_hbm.at[cols], w_d))):
            copy = pltpu.make_async_copy(src, dst.at[i], load_sem.at[i, j])
            copy.start()
            shared_loads.append(copy)

    near_0 = near_v(0)
    near_down = send_picked(0, 0, v_chip[1], 4, near_s.at[3], SIDE[1], 0, v_dev[1])

    for i in range(local_count):
        for j, (src, dst) in enumerate(((wg_hbm, w_g), (wu_hbm, w_u), (wd_hbm, w_d))):
            send(src.at[i], dst.at[local_count + i], wr_s.at[j], wr_r.at[j], partner)

    def silu_mul(g, up):
        return (jax.nn.silu(g) * up).astype(BF16)

    def shared_part(i):
        for copy in shared_loads[3 * i:3 * i + 3]:
            copy.wait()
        x = tok[0]
        h = silu_mul(jnp.dot(x, w_g[i], preferred_element_type=F32), jnp.dot(x, w_u[i], preferred_element_type=F32))
        for n in range(0, model_dim, n_step):
            y = jnp.dot(h, w_d[i, :, n:n + n_step], preferred_element_type=F32)
            if i > 0:
                y = y + acc[:, n:n + n_step]
            if i == local_count - 1:
                y = y.astype(BF16).astype(F32) + x[:, n:n + n_step].astype(F32)
            acc[:, n:n + n_step] = y

    own_loads = []

    def load_own(i):
        for j, (src, dst) in enumerate(((wg_hbm, w_g), (wu_hbm, w_u), (wd_hbm, w_d))):
            copy = pltpu.make_async_copy(src.at[i], dst.at[i], load_sem.at[i, j])
            copy.start()
            own_loads.append(copy)

    for i in range(local_count):
        shared_part(i)
        load_own(i)

    def e_half(d):
        return pl.ds(d * local_count, local_count)

    inf_wait(0, 1)
    send_info((0, 1), (1, 1), 8, v_dev[0])
    inf_wait(0, 2)
    send_info((0, 2), (2, 2), 8, v_dev[1])
    for k, p in ((1, 0), (2, 1), (1, 1), (2, 0)):
        tok_wait(0, k, p)
        whole_v(k, p)
    for d in range(2):
        first, count = ((0, chip_experts // 4), (chip_experts // 4, chip_experts - chip_experts // 4))[d]
        es = pl.ds(first, count)
        pick(0, SIDE[d], u_chip[d], stage.at[1], 0, (first, first + count))
        send(stage.at[1, es], xg.at[0, es, group_rows(3)], near_s.at[2], x_r.at[0], u_dev[d])
    near_1 = near_v(1)
    near_v(2)
    inf_wait(2, 0)
    send_info((2, 0), (3, 0), 16, v_dev[1])
    block_wait(1, 1)
    send(tok.at[WHOLE[1, 1]], tok.at[WHOLE[3, 1]], tok_s, tok_r.at[WHOLE[3, 1] + 1], v_dev[0])
    inf_wait(1, 1)
    send_info((1, 1), (3, 1), 8, v_dev[0])
    send_picked(1, 1, u_chip[0], 5, far_s, 1, 3, u_dev[0])

    def experts(g):
        def one(e, carry):
            x = xg[g, e]
            h = silu_mul(jnp.dot(x, w_g[e], preferred_element_type=F32), jnp.dot(x, w_u[e], preferred_element_type=F32))
            for n in range(0, model_dim, n_step):
                y = jnp.dot(h, w_d[e, :, n:n + n_step], preferred_element_type=F32).astype(BF16)
                raw[g, 0, e, :, n:n + n_step] = y[0:cap]
                xg[g, e, cap:4 * cap, n:n + n_step] = y[cap:4 * cap]
            return carry

        lax.fori_loop(0, chip_experts, one, 0)

    def own_pick(g, ks):
        for k in ks:
            pick(g, k, chip, xg.at[g], k * cap)

    def x_wait(g, ks):
        filled(xg.at[g, pl.ds(0, len(ks) * chip_experts // 4)], x_r.at[g])

    def col_chunk(f):
        return slice(None) if f is None else pl.ds(f * width, width)

    def send_rows(g, f=None):
        at = col_chunk(f)
        i = f or 0
        for d in range(2):
            send(xg.at[g, e_half(d), group_rows(3), at], relay.at[g, d, :, :, at], f_s, rel_r.at[g + i], u_dev[d])
        for d in range(2):
            send(xg.at[g, :, group_rows(2 - d), at], raw.at[g, SIDE[d], :, :, at], f_s, raw_r.at[g + i], u_dev[d])

    def pass_rows(g, f=None):
        at = col_chunk(f)
        i = f or 0
        filled(relay.at[g, :, :, :, at], rel_r.at[g + i])
        for d in range(2):
            send(relay.at[g, d, :, :, at], raw.at[g, 3, e_half(d), :, at], rel_s, raw_r.at[g + i], u_dev[d])

    def raw_wait(g, f=None):
        at = col_chunk(f)
        i = f or 0
        filled(raw.at[g, pl.ds(1, 3), :, :, at], raw_r.at[g + i])

    def gates_of(g):
        for m in range(4):
            codes = row_codes(chip_at(u + OFFSETS[m], v))
            gate = jnp.zeros((block, tok_count), F32)
            for j in range(top_count):
                gate = gate + jnp.where(info[table_at(g, 0, j), :] == codes, info[table_at(g, 0, 8 + j), :], 0.0)
            gate = gate.T
            for s in range(3):
                part_s = gate.astype(BF16)
                gsplit[s * tok_count:(s + 1) * tok_count, m * block:(m + 1) * block] = part_s
                gate = gate - part_s.astype(F32)

    step = 256 if width % 256 == 0 else width

    def gated(g, f=None):
        first, count = (0, model_dim // step) if f is None else (f * (width // step), width // step)

        def cols(n, carry):
            at = pl.ds(pl.multiple_of(n * step, 128), step)
            rows = raw[g, :, :, :, at].reshape(4 * block, step)
            y = jnp.dot(gsplit[...], rows, preferred_element_type=F32)
            y = y[0:tok_count] + y[tok_count:2 * tok_count] + y[2 * tok_count:3 * tok_count]
            if g == 0:
                acc[:, at] = acc[:, at] + y
            else:
                part[g - 1, :, at] = y
            return carry

        lax.fori_loop(first, first + count, cols, 0)

    def send_early(g, d):
        send(part.at[g - 1, rows_of(1 - d)], fin.at[d], fin_s, fin_r.at[0], v_dev[d])

    def send_last(g, d, f):
        at = col_chunk(f)
        send(part.at[g - 1, rows_of(d), at], last.at[rows_of(d), at], fin_s, fin_r.at[1], v_dev[d])

    own_pick(0, (0, 1, 2))
    for copy in own_loads:
        copy.wait()
    for j, dst in enumerate((w_g, w_u, w_d)):
        filled(dst.at[pl.ds(local_count, local_count)], wr_r.at[j])
    x_wait(0, (3,))
    experts(0)
    block_wait(2, 2)
    inf_wait(2, 2)
    near_0.wait_send()
    send_picked(2, 2, v_chip[1], 0, far_s, 3, 2, v_dev[1])
    filled(stage.at[1], near_s.at[2])
    send_picked(2, 2, u_chip[1], 1, far_s, 2, 3, u_dev[1])
    send_rows(0)
    own_pick(1, (1,))
    x_wait(1, (0, 2, 3))
    experts(1)
    block_wait(3, 1)
    inf_wait(3, 1)
    near_1.wait_send()
    send_picked(3, 1, u_chip[0], 2, far_s, 3, 3, u_dev[0])
    near_down.wait_send()
    send_picked(3, 1, u_chip[1], 4, far_s, 3, 0, u_dev[1])
    pass_rows(0)
    send_rows(1)
    own_pick(2, (2,))
    own_pick(3, (1,))
    pass_rows(1)
    x_wait(2, (0, 1, 3))
    experts(2)
    send_rows(2)
    raw_wait(0)
    gates_of(0)
    gated(0)
    x_wait(3, (0, 2, 3))
    experts(3)
    pass_rows(2)
    for f in range(chunks):
        send_rows(3, f)
    raw_wait(1)
    inf_wait(1, 0)
    gates_of(1)
    gated(1)
    inf_wait(3, 0)
    raw_wait(2)
    gates_of(2)
    pass_rows(3, 0)
    gated(2)
    send_early(1, 1)
    send_early(2, 0)
    for f in range(1, chunks):
        pass_rows(3, f)
    gates_of(3)
    for f in range(chunks):
        raw_wait(3, f)
        gated(3, f)
        for d in range(2):
            send(part.at[2, rows_of(d), col_chunk(f)], half.at[d, :, col_chunk(f)], half_s, half_r.at[f], v_dev[d])
    for f in range(chunks):
        at = slice(f * width, (f + 1) * width)
        filled(half.at[:, :, col_chunk(f)], half_r.at[f])
        for d in range(2):
            g = 2 - d
            rows = slice(d * piece, (d + 1) * piece)
            part[g - 1, rows, at] = part[g - 1, rows, at] + half[d, :, at]
            send_last(g, d, f)

    filled(fin, fin_r.at[0])
    for d in range(2):
        rows = slice((1 - d) * piece, (2 - d) * piece)
        acc[rows] = acc[rows] + fin[d]

    filled(tok.at[pl.ds(0, 5)], tok_s)
    filled(stage, far_s)
    filled(info.at[pl.ds(0, 5 * 8 + 3 * 16)], inf_s)
    for j, dst in enumerate((w_g, w_u, w_d)):
        filled(dst.at[pl.ds(0, local_count)], wr_s.at[j])
    filled(raw.at[pl.ds(0, 3)], f_s)
    filled(relay, rel_s)
    filled(half, half_s)
    filled(part.at[pl.ds(0, 2)], fin_s)
    filled(last, fin_r.at[1])


def solution(mesh):
    group_size = mesh.shape["ep"]
    side = math.isqrt(group_size // 2)

    def moe_step(tokens, expert_ids, gate_vals, w_gate, w_up, w_down, shared_gate, shared_up, shared_down):
        tok_count, model_dim = tokens.shape
        top_count = expert_ids.shape[1]
        local_count, _, ff = w_gate.shape
        expert_count = local_count * group_size
        spread = max(group_size, expert_count // 2)
        cap = (tok_count * top_count + spread - 1) // spread
        block = 2 * local_count * cap
        piece = tok_count // 2
        dma = pltpu.SemaphoreType.DMA
        hbm = pl.BlockSpec(memory_space=pl.ANY)
        scratch = [
            pltpu.VMEM((top_count, tok_count), jnp.int32),
            pltpu.VMEM((top_count, tok_count), F32),
            pltpu.VMEM((2 * local_count, model_dim, ff), BF16),
            pltpu.VMEM((2 * local_count, model_dim, ff), BF16),
            pltpu.VMEM((2 * local_count, ff, model_dim), BF16),
            pltpu.VMEM((len(WHOLE), tok_count, model_dim), BF16),
            pltpu.VMEM((16 * 16, tok_count), F32),
            pltpu.VMEM((4, 2 * local_count, 4 * cap, model_dim), BF16),
            pltpu.VMEM((6, 2 * local_count, cap, model_dim), BF16),
            pltpu.VMEM((4, 4, 2 * local_count, cap, model_dim), BF16),
            pltpu.VMEM((4, 2, local_count, cap, model_dim), BF16),
            pltpu.VMEM((3 * tok_count, 4 * block), BF16),
            pltpu.VMEM((3, tok_count, model_dim), F32),
            pltpu.VMEM((2, piece, model_dim), F32),
            pltpu.VMEM((2, piece, model_dim), F32),
            dma((3,)), dma((local_count, 3)), dma((len(WHOLE) + 1,)), dma((len(TABLES),)), dma((4,)), dma((6,)), dma((6,)),
            dma((3,)), dma((2,)), dma((3,)),
            dma(()), dma((4,)), dma(()), dma(()), dma(()), dma(()), dma(()), dma(()), dma((3,)),
        ]
        total = pltpu.VMEM(tokens.shape, F32)
        base, last = pl.pallas_call(
            functools.partial(kernel, side, cap),
            out_shape=(total, total),
            in_specs=[hbm] * 9,
            out_specs=(pl.BlockSpec(memory_space=pltpu.VMEM),) * 2,
            scratch_shapes=scratch,
            compiler_params=pltpu.CompilerParams(collective_id=0, has_side_effects=True, vmem_limit_bytes=63 * 1024 * 1024 - 3200 * 1024),
        )(expert_ids.T, gate_vals.T, tokens, w_gate, w_up, w_down, shared_gate, shared_up, shared_down)
        return (base + last).astype(tokens.dtype)

    row_spec = P(("dp", "ep"), None)
    expert_spec = P("ep", None, None)
    whole_spec = P(None, None)
    return jax.shard_map(moe_step, mesh=mesh, in_specs=(row_spec, row_spec, row_spec, expert_spec, expert_spec, expert_spec, whole_spec, whole_spec, whole_spec), out_specs=row_spec, check_vma=False)
```
